256 devices in a mesh: gx: 8 (over y_hi, x), gy: 8 (over z), gz: 4 (over y_lo, core).
Axes of the slice: x: 4, y: 4 (y_hi: 2, y_lo: 2; y = y_hi * 2 + y_lo), z: 8, core: 2. Of those that a mesh axis runs over, the one named last changes fastest.
Arguments:
- tokens: bfloat16 [4096, 49, 512], P(('gx', 'gy', 'gz')), may hold values from -6 to 6
- cotangent: bfloat16 [4096, 49, 512], P(('gx', 'gy', 'gz')), may hold values from -6 to 6
- regions: int32 [4096, 49], P(('gx', 'gy', 'gz')), may hold values from 0 to 3
- rel_index: int32 [49, 49], replicated, may hold values from 0 to 168
- w_qkv: bfloat16 [512, 1536], replicated, may hold values from -0.25 to 0.25
- w_proj: bfloat16 [512, 512], replicated, may hold values from -0.25 to 0.25
- bias_table: float32 [169, 16], replicated, may hold values from -4 to 4
- mom_qkv: float32 [786432], P(('gx', 'gy', 'gz')), may hold values from -0.06 to 0.06
- mom_proj: float32 [262144], P(('gx', 'gy', 'gz')), may hold values from -0.06 to 0.06
- mom_table: float32 [169, 16], replicated, may hold values from -0.06 to 0.06
Outputs:
- new_mom_qkv: float32 [786432], P(('gx', 'gy', 'gz'))
- new_mom_proj: float32 [262144], P(('gx', 'gy', 'gz'))
- new_mom_table: float32 [169, 16], replicated
The draws below stay inside these ranges and needn't reach their ends.
All inputs are finite; a program needn't handle non-finite values.
Results may differ from the reference program's by a relative error of at most 0.015.
Values sent between devices are 32-bit elements; how exact they have to be, the bound alone decides.
No kernel may reach another device: no remote copies, remote signals or barrier semaphores. Data moves between devices by JAX's collectives and lax.ppermute only.
A program may use at most 128 MiB of HBM per device.

```python
import jax
import jax.numpy as jnp
from jax import lax

D = 512
HEADS = 16
WIN_TOK = 49
TABLE = 169
WIN_DEV = 16
WINDOWS = 4096
N_GX = 8
N_GY = 8
N_GZ = 4


def touch_ends(drawn, own_key, smallest, largest):
    dims = drawn.shape
    index_at = [jax.random.randint(jax.random.fold_in(own_key, axis), (), 0, dims[axis]) for axis in range(len(dims))]
    drawn = drawn.at[tuple(index_at)].set(smallest)
    longest = dims.index(max(dims))
    index_at[longest] = (index_at[longest] + 1) % dims[longest]
    return drawn.at[tuple(index_at)].set(largest)


def block_levels(key, shape, cuts, low, largest):
    def one(dim, shards_of):
        steps = jax.random.uniform(jax.random.fold_in(jax.random.fold_in(key, 6), dim), (shards_of,), jnp.float32, low / len(cuts), largest / len(cuts))
        return jnp.repeat(jnp.exp(steps), shape[dim] // shards_of).reshape((-1,) + (1,) * (len(shape) - dim - 1))

    loudness = one(*cuts[0])
    for cut in cuts[1:]:
        loudness = loudness * one(*cut)
    return loudness


def noise(stream_key, extent, deviation, reach, cuts=(), held_as=jnp.bfloat16):
    drawn = deviation * jax.random.normal(stream_key, extent, jnp.float32)
    if cuts:
        drawn = drawn * block_levels(stream_key, extent, cuts, -0.22, 0.18)
    return jnp.clip(drawn, -reach, reach).astype(held_as)


def setup_inputs(seed: int = 0) -> dict:
    key_list = jax.random.split(jax.random.key(seed), 11)
    return {
        "tokens": noise(key_list[0], (WINDOWS, WIN_TOK, D), 1.0, 6.0, ((0, 256),)),
        "cotangent": noise(key_list[1], (WINDOWS, WIN_TOK, D), 1.0, 6.0, ((0, 256),)),
        "regions": touch_ends(jax.random.randint(key_list[2], (WINDOWS, WIN_TOK), 0, 4), jax.random.fold_in(key_list[2], 1), 0, 3).astype(jnp.int32),
        "rel_index": touch_ends(jax.random.randint(key_list[3], (WIN_TOK, WIN_TOK), 0, 169), jax.random.fold_in(key_list[3], 1), 0, 168).astype(jnp.int32),
        "w_qkv": noise(key_list[4], (D, 3 * D), D ** -0.5, 0.25),
        "w_proj": noise(key_list[5], (D, D), D ** -0.5, 0.25),
        "bias_table": noise(key_list[6], (TABLE, HEADS), 1.0, 4.0, (), jnp.float32),
        "mom_qkv": noise(key_list[7], (3 * D * D,), 0.01, 0.06, ((0, 256),), jnp.float32),
        "mom_proj": noise(key_list[8], (D * D,), 0.01, 0.06, ((0, 256),), jnp.float32),
        "mom_table": noise(key_list[9], (TABLE, HEADS), 0.01, 0.06, (), jnp.float32),
    }


def attend_core(qkv, table, regions, rel_index, heads):
    win, count, width = qkv.shape
    dim = width // 3
    parts = qkv.reshape(win, count, 3, heads, dim // heads).astype(jnp.float32)
    bias = jnp.transpose(table[rel_index], (2, 0, 1))
    scores = jnp.einsum('wihc,wjhc->whij', parts[:, :, 0], parts[:, :, 1]) * (dim // heads) ** (-0.5)
    masked = jnp.where(regions[:, :, None] == regions[:, None, :], 0.0, -100.0).astype(jnp.float32)
    scores = scores + bias[None] + masked[:, None]
    probs = jax.nn.softmax(scores, axis=-1).astype(jnp.bfloat16)
    attended = jnp.einsum('whij,wjhc->wihc', probs.astype(jnp.float32), parts[:, :, 2])
    return attended.astype(jnp.bfloat16).reshape(win, count, dim)

def local_grads(tokens, cotangent, regions, rel_index, w_qkv, w_proj, bias_table, heads):
    win, count, dim = tokens.shape
    flat = tokens.reshape(win * count, dim)
    qkv = jnp.dot(flat, w_qkv, preferred_element_type=jnp.float32).astype(jnp.bfloat16).reshape(win, count, 3 * dim)

    def forward(values, table):
        return attend_core(values, table, regions, rel_index, heads)
    attended, pullback = jax.vjp(forward, qkv, bias_table)
    flat_dy = cotangent.reshape(win * count, dim)
    grad_proj = jnp.dot(attended.reshape(win * count, dim).astype(jnp.float32).T, flat_dy.astype(jnp.float32))
    d_attended = jnp.dot(flat_dy, w_proj.T, preferred_element_type=jnp.float32).astype(jnp.bfloat16)
    d_qkv, grad_table = pullback(d_attended.reshape(win, count, dim))
    grad_qkv = jnp.dot(flat.astype(jnp.float32).T, d_qkv.reshape(win * count, 3 * dim).astype(jnp.float32))
    return (grad_qkv, grad_proj, grad_table)

def reference(tokens, cotangent, regions, rel_index, w_qkv, w_proj, bias_table, mom_qkv, mom_proj, mom_table):
    groups = N_GX * N_GY * N_GZ
    heads = bias_table.shape[1]
    tok_groups = tokens.reshape(groups, WIN_DEV, WIN_TOK, D)
    cot_groups = cotangent.reshape(groups, WIN_DEV, WIN_TOK, D)
    reg_groups = regions.reshape(groups, WIN_DEV, WIN_TOK)

    def step(carry, items):
        g_qkv, g_proj, g_table = local_grads(items[0], items[1], items[2], rel_index, w_qkv, w_proj, bias_table, heads)
        return ((carry[0] + g_qkv, carry[1] + g_proj, carry[2] + g_table), None)
    start = (jnp.zeros(w_qkv.shape, jnp.float32), jnp.zeros(w_proj.shape, jnp.float32), jnp.zeros(bias_table.shape, jnp.float32))
    sums, unused = lax.scan(step, start, (tok_groups, cot_groups, reg_groups))
    scale = 1.0 / (WIN_DEV * groups)
    return (0.9 * mom_qkv + sums[0].reshape(-1) * scale, 0.9 * mom_proj + sums[1].reshape(-1) * scale, 0.9 * mom_table + sums[2] * scale)
```

```python
import jax
import jax.numpy as jnp
from jax import lax
from jax.experimental import pallas as pl
from jax.experimental.pallas import tpu as pltpu
from jax.sharding import PartitionSpec as P

AXES = ("gx", "gy", "gz")
WIN = 16
TOK = 49
PAD = 64
D = 512
HEADS = 16
HD = 32
ENT = 169
EPAD = 176
ROWS = TOK * WIN
PROWS = PAD * WIN
F32 = jnp.float32
BF16 = jnp.bfloat16
NT = (((1,), (1,)), ((), ()))
NN = (((1,), (0,)), ((), ()))


def dot(a, b, dims=NN):
    return lax.dot_general(a, b, dims, preferred_element_type=F32)


def decode(flat):
    gx, gy, gz = flat // 32, (flat // 4) % 8, flat % 4
    return gx % 4, (gx // 4) * 2 + gz // 2, gy, gz % 2


def encode(x, y, z, c):
    x, y, z = x % 4, y % 4, z % 8
    return ((y // 2) * 4 + x) * 32 + z * 4 + (y % 2) * 2 + c


def shift(value, dx=0, dy=0, dz=0, dc=0):
    pairs = []
    for d in range(256):
        x, y, z, c = decode(d)
        pairs.append((d, encode(x + dx, y + dy, z + dz, c ^ dc)))
    return lax.ppermute(value, AXES, pairs)


def row_order(pos, second):
    x, y, z, c = pos
    r = lax.broadcasted_iota(jnp.int32, (D, 128), 0)
    e = r & 1
    rz = (r >> 1) & 7
    lo = (r >> 4) & 3
    hi = (r >> 6) & 3
    rc = (r >> 8) & 1
    rx, ry = (lo, hi) if second else (hi, lo)
    xt = (x + rx) & 3
    yt = (y + ry) & 3
    zt = (z + rz) & 7
    ct = (c + rc) & 1
    orig = ((((yt >> 1) * 4 + xt) * 32 + zt * 4 + (yt & 1) * 2 + ct) << 1) + e
    col = lax.broadcasted_iota(jnp.int32, (D, 128), 1)
    parts = [jnp.where(orig == col + 128 * k, 1.0, 0.0) for k in range(4)]
    return jnp.concatenate(parts, axis=1).astype(BF16)


def local_kernel(
    tok, cot, reg, rel, wqkv, wproj, tab, keep, send, qkv_s, da_s, att_s, dqkv_s, bias_s, mask_s, acc_s, sq_s, t1_s, t2_s
):
    gx, gy, gz = lax.axis_index("gx"), lax.axis_index("gy"), lax.axis_index("gz")
    pos = (gx & 3, ((gx >> 2) << 1) + (gz >> 1), gy, gz & 1)
    scale = HD**-0.5

    for n in range(6):
        two = dot(tok[...], wqkv[:, 256 * n : 256 * n + 256])
        qkv_s[2 * n, 0:ROWS] = two[:, 0:128]
        qkv_s[2 * n + 1, 0:ROWS] = two[:, 128:256]
    for n in range(2):
        two = dot(cot[...], wproj[256 * n : 256 * n + 256], NT)
        da_s[2 * n, 0:ROWS] = two[:, 0:128]
        da_s[2 * n + 1, 0:ROWS] = two[:, 128:256]
    for n in range(12):
        qkv_s[n, ROWS:PROWS] = jnp.zeros((PROWS - ROWS, 128), F32)
    for n in range(4):
        da_s[n, ROWS:PROWS] = jnp.zeros((PROWS - ROWS, 128), F32)

    sq_s[...] = jnp.zeros((128, 128), F32)
    sq_s[0:TOK, 0:TOK] = rel[...].astype(F32)
    sq_s[PAD : PAD + TOK, 0:TOK] = rel[...].astype(F32)
    relt = jnp.transpose(sq_s[...])[0:PAD].astype(jnp.int32)
    lane = lax.broadcasted_iota(jnp.int32, (PAD, 128), 1)
    sub = lax.broadcasted_iota(jnp.int32, (PAD, 128), 0)
    live = ((lane & 63) < TOK) & (sub < TOK)
    relt = jnp.where(live, relt, -1)
    safe = jnp.where(live, relt, 0)
    low_i = jnp.where(safe < 128, safe, 0)
    high_i = jnp.where(safe < 128, 0, safe - 128)
    is_low = safe < 128
    first = lane < 64
    for hp in range(HEADS // 2):
        looked = []
        for par in range(2):
            h = 2 * hp + par
            low = jnp.broadcast_to(tab[h : h + 1, 0:128], (8, 128))
            high = jnp.concatenate([tab[h : h + 1, 128:ENT], jnp.zeros((1, 256 - ENT), F32)], axis=1)
            high = jnp.broadcast_to(high, (8, 128))
            rows = []
            for b in range(PAD // 8):
                s = slice(8 * b, 8 * b + 8)
                a0 = jnp.take_along_axis(low, low_i[s], axis=1, mode="promise_in_bounds")
                a1 = jnp.take_along_axis(high, high_i[s], axis=1, mode="promise_in_bounds")
                rows.append(jnp.where(is_low[s], a0, a1))
            looked.append(jnp.concatenate(rows, axis=0))
        both = jnp.where(first, looked[0], looked[1])
        bias_s[hp * PAD : (hp + 1) * PAD] = jnp.where(sub < TOK, both, -1e30)

    sq_s[...] = jnp.zeros((128, 128), F32)
    sq_s[0:WIN, 0:TOK] = reg[...].astype(F32)
    base = sq_s[...]
    cols = jnp.transpose(base)
    for w in range(WIN):
        line = jnp.concatenate([base[w : w + 1, 0:64], base[w : w + 1, 0:64]], axis=1)
        mask_s[w * PAD : (w + 1) * PAD] = jnp.where(cols[0:PAD, w : w + 1] == line, 0.0, -100.0)

    acc_s[...] = jnp.zeros(acc_s.shape, F32)
    chan = lax.broadcasted_iota(jnp.int32, (PAD, 128), 1) // HD

    def spread(v):
        return jnp.concatenate([jnp.where(chan == h, v, 0.0) for h in range(4)], axis=0).astype(BF16)

    def fold(full):
        total = jnp.where(chan == 0, full[0:PAD], 0.0)
        for h in range(1, 4):
            total = jnp.where(chan == h, full[h * PAD : (h + 1) * PAD], total)
        return total

    def window(w, carry):
        here = pl.ds(w, PAD, stride=WIN)
        m1 = mask_s[pl.ds(pl.multiple_of(w * PAD, PAD), PAD), :]
        mask = jnp.concatenate([m1, m1], axis=1)
        for g in range(4):
            q = qkv_s[g, here, :]
            k = qkv_s[4 + g, here, :].astype(BF16)
            v = qkv_s[8 + g, here, :].astype(BF16)
            qd = spread(q)
            dd = spread(da_s[g, here, :])
            bias = jnp.concatenate(
                [bias_s[2 * g * PAD : (2 * g + 1) * PAD], bias_s[(2 * g + 1) * PAD : (2 * g + 2) * PAD]], axis=1
            )
            s = dot(k, qd, NT) * scale + bias + mask
            p = jnp.exp(s - jnp.max(s, axis=0, keepdims=True))
            p = p * (1.0 / jnp.sum(p, axis=0, keepdims=True))
            pb = p.astype(BF16)
            dp = dot(v, dd, NT).astype(BF16).astype(F32)
            ds = p * (dp - jnp.sum(dp * p, axis=0, keepdims=True))
            acc_s[2 * g * PAD : (2 * g + 1) * PAD] += ds[:, 0:128]
            acc_s[(2 * g + 1) * PAD : (2 * g + 2) * PAD] += ds[:, 128:256]
            dsb = (ds * scale).astype(BF16)
            dqkv_s[8 + g, here, :] = dot(pb, dd)
            dqkv_s[4 + g, here, :] = dot(dsb, qd)
            att_s[g, here, :] = fold(dot(jnp.transpose(pb), v))
            dqkv_s[g, here, :] = fold(dot(jnp.transpose(dsb), k))
        return carry

    lax.fori_loop(0, WIN, window, 0)

    ent = lax.broadcasted_iota(jnp.int32, (EPAD, 128), 0)
    sums = jnp.zeros((2 * EPAD, 16), F32)
    for j in range(TOK):
        part = acc_s[pl.ds(j, 8, stride=PAD), :]
        top = part.astype(BF16).astype(F32)
        rhs = jnp.concatenate([top, part - top], axis=0).astype(BF16)
        row = relt[j : j + 1]
        lo = jnp.where(lane[0:1] < 64, row, -1)
        hi = jnp.where(lane[0:1] < 64, -1, row)
        hot = jnp.concatenate([jnp.where(ent == lo, 1.0, 0.0), jnp.where(ent == hi, 1.0, 0.0)], axis=0)
        sums = sums + dot(hot.astype(BF16), rhs, NT)
    sums = jnp.concatenate([sums, jnp.zeros((2 * EPAD, 112), F32)], axis=1)
    sums = jnp.concatenate([sums, jnp.zeros((384 - 2 * EPAD, 128), F32)], axis=0)
    flat = jnp.concatenate([jnp.transpose(sums[128 * k : 128 * k + 128])[0:16] for k in range(3)], axis=1)
    table = jnp.concatenate([flat[0:8] + flat[8:16], jnp.zeros((8, 2048 - 384), F32)], axis=1)
    keep[256:264] = table
    send[256:264] = table

    order1 = row_order(pos, False)
    order2 = row_order(pos, True)
    t1_s[...] = dot(order1, tok[...], NT).astype(BF16)
    t2_s[...] = dot(order2, tok[...], NT).astype(BF16)

    def pair(ref, n):
        return jnp.concatenate([ref[n, 0:ROWS].astype(BF16), ref[n + 1, 0:ROWS].astype(BF16)], axis=1)

    for n in range(6):
        left = t1_s if n < 4 else t2_s
        grad = dot(left[...], pair(dqkv_s, 2 * n))
        cols = slice(256 * n, 256 * n + 256)
        keep[0:256, cols] = grad[0:256]
        send[0:256, cols] = grad[256:512]
    att = jnp.concatenate([pair(att_s, 0), pair(att_s, 2)], axis=1)
    t1_s[...] = dot(order2, att, NT).astype(BF16)
    for n in range(2):
        grad = dot(t1_s[...], cot[:, 256 * n : 256 * n + 256])
        cols = slice(1536 + 256 * n, 1792 + 256 * n)
        keep[0:256, cols] = grad[0:256]
        send[0:256, cols] = grad[256:512]


def sum_a(keep, got, *outs):
    one, two = outs[0:4], outs[4:8]
    for k in range(4):
        rows = slice(64 * k, 64 * k + 64)
        one[k][0:64] = keep[rows, 0:1024] + got[rows, 0:1024]
        one[k][64:72] = keep[256:264, 0:1024] + got[256:264, 0:1024]
        two[k][...] = keep[rows, 1024:2048] + got[rows, 1024:2048]


def four(refs, rows):
    return (refs[0][rows] + refs[2][rows]) + (refs[1][rows] + refs[3][rows])


def sum_b(*refs):
    a, b, one, two = refs[0:4], refs[4:8], refs[8:12], refs[12:16]
    table = four(a, slice(64, 72))
    for k in range(4):
        rows = slice(16 * k, 16 * k + 16)
        one[k][0:16] = four(a, rows)
        one[k][16:24] = table
        two[k][...] = four(b, rows)


def sum_c(*refs):
    a, b, outs = refs[0:4], refs[4:8], refs[8:12]
    table = four(a, slice(16, 24))
    one = four(a, slice(0, 16))
    two = four(b, slice(0, 16))
    for k in range(4):
        outs[k][0:4] = one[4 * k : 4 * k + 4]
        outs[k][4:8] = two[4 * k : 4 * k + 4]
        outs[k][8:16] = table


def sum_d(*refs):
    a, outs = refs[0:4], refs[4:6]
    body = four(a, slice(0, 8))
    table = four(a, slice(8, 16))
    for k in range(2):
        outs[k][0:2] = body[2 * k : 2 * k + 2]
        outs[k][2:4] = body[4 + 2 * k : 6 + 2 * k]
        outs[k][4:8] = jnp.zeros((4, 1024), F32)
        outs[k][8:16] = table


def finish(own, got, mq, mp, mt, oq, op, ot):
    scale = 1.0 / 4096
    total = (own[...] + got[...]) * scale
    for e in range(2):
        for c in range(12):
            row, at = (e, c) if c < 8 else (2 + e, c - 8)
            r = slice(12 * e + c, 12 * e + c + 1)
            oq[r] = 0.9 * mq[r] + total[row : row + 1, 128 * at : 128 * at + 128]
        for c in range(4):
            r = slice(4 * e + c, 4 * e + c + 1)
            op[r] = 0.9 * mp[r] + total[2 + e : 3 + e, 512 + 128 * c : 640 + 128 * c]
    for h in range(HEADS):
        at = (h % 2) * EPAD
        ot[h : h + 1] = 0.9 * mt[h : h + 1] + total[8 + h // 2 : 9 + h // 2, at : at + ENT]


def shapes(*dims):
    return tuple(jax.ShapeDtypeStruct(d, F32) for d in dims)


def local_grads(tok, cot, regions, rel_index, w_qkv, w_proj, table, interpret=False):
    return pl.pallas_call(
        local_kernel,
        out_shape=shapes((264, 2048), (264, 2048)),
        scratch_shapes=[
            pltpu.VMEM((12, PROWS, 128), F32),
            pltpu.VMEM((4, PROWS, 128), F32),
            pltpu.VMEM((4, PROWS, 128), F32),
            pltpu.VMEM((12, PROWS, 128), F32),
            pltpu.VMEM((8 * PAD, 128), F32),
            pltpu.VMEM((WIN * PAD, 128), F32),
            pltpu.VMEM((8 * PAD, 128), F32),
            pltpu.VMEM((128, 128), F32),
            pltpu.VMEM((D, ROWS), BF16),
            pltpu.VMEM((D, ROWS), BF16),
        ],
        name="local_grads",
        interpret=interpret,
    )(tok, cot, regions, rel_index, w_qkv, w_proj, table)


def body(
    tokens, cotangent, regions, rel_index, w_qkv, w_proj, bias_table, mom_qkv, mom_proj, mom_table
):
    tok = jnp.transpose(tokens, (1, 0, 2)).reshape(ROWS, D)
    cot = jnp.transpose(cotangent, (1, 0, 2)).reshape(ROWS, D)
    keep, send = local_grads(tok, cot, regions, rel_index, w_qkv, w_proj, bias_table.T)
    got = shift(send, dc=1)
    m = pl.pallas_call(sum_a, out_shape=shapes(*[(72, 1024)] * 4, *[(64, 1024)] * 4), name="sum_a")(keep, got)
    r = [m[0]] + [shift(m[k], dx=k) for k in (1, 2, 3)] + [m[4]] + [shift(m[4 + k], dy=k) for k in (1, 2, 3)]
    m = pl.pallas_call(sum_b, out_shape=shapes(*[(24, 1024)] * 4, *[(16, 1024)] * 4), name="sum_b")(*r)
    r = [m[0]] + [shift(m[k], dy=k) for k in (1, 2, 3)] + [m[4]] + [shift(m[4 + k], dx=k) for k in (1, 2, 3)]
    m = pl.pallas_call(sum_c, out_shape=shapes(*[(16, 1024)] * 4), name="sum_c")(*r)
    r = [m[0]] + [shift(m[k], dz=2 * k) for k in (1, 2, 3)]
    m = pl.pallas_call(sum_d, out_shape=shapes(*[(16, 1024)] * 2), name="sum_d")(*r)
    got = shift(m[1], dz=1)
    new_q, new_p, new_t = pl.pallas_call(
        finish, out_shape=shapes((24, 128), (8, 128), (HEADS, ENT)), name="finish"
    )(m[0], got, mom_qkv.reshape(24, 128), mom_proj.reshape(8, 128), mom_table.T)
    return new_q.reshape(-1), new_p.reshape(-1), new_t.T


def solution(mesh):
    return jax.shard_map(
        body,
        mesh=mesh,
        in_specs=(
            P(AXES, None, None),
            P(AXES, None, None),
            P(AXES, None),
            P(),
            P(),
            P(),
            P(),
            P(AXES),
            P(AXES),
            P(),
        ),
        out_specs=(P(AXES), P(AXES), P()),
        check_vma=False,
    )
```

```python
import jax
import jax.numpy as jnp
from jax import lax
from jax.experimental import pallas as pl
from jax.experimental.pallas import tpu as pltpu
from jax.sharding import PartitionSpec as P

AXES = ("gx", "gy", "gz")
WIN = 16
TOK = 49
PAD = 64
D = 512
HEADS = 16
HD = 32
ENT = 169
EPAD = 176
ROWS = TOK * WIN
PROWS = PAD * WIN
F32 = jnp.float32
BF16 = jnp.bfloat16
NT = (((1,), (1,)), ((), ()))
NN = (((1,), (0,)), ((), ()))


def dot(a, b, dims=NN):
    return lax.dot_general(a, b, dims, preferred_element_type=F32)


def decode(flat):
    gx, gy, gz = flat // 32, (flat // 4) % 8, flat % 4
    return gx % 4, (gx // 4) * 2 + gz // 2, gy, gz % 2


def encode(x, y, z, c):
    x, y, z = x % 4, y % 4, z % 8
    return ((y // 2) * 4 + x) * 32 + z * 4 + (y % 2) * 2 + c


def shift(value, dx=0, dy=0, dz=0, dc=0):
    pairs = []
    for d in range(256):
        x, y, z, c = decode(d)
        pairs.append((d, encode(x + dx, y + dy, z + dz, c ^ dc)))
    return lax.ppermute(value, AXES, pairs)


def planes():
    return [[encode(x, y, z, c) for y in range(4) for x in range(4)] for z in range(8) for c in range(2)]


def row_order(core):
    r = lax.broadcasted_iota(jnp.int32, (D, 128), 0)
    e = r & 1
    z = (r >> 1) & 7
    x = (r >> 4) & 3
    y = (r >> 6) & 3
    c = ((r >> 8) + core) & 1
    orig = ((((y >> 1) * 4 + x) * 32 + z * 4 + (y & 1) * 2 + c) << 1) + e
    col = lax.broadcasted_iota(jnp.int32, (D, 128), 1)
    parts = [jnp.where(orig == col + 128 * k, 1.0, 0.0) for k in range(4)]
    return jnp.concatenate(parts, axis=1).astype(BF16)


def local_kernel(
    tok, cot, reg, rel, wqkv, wproj, tab, keep, send, qkv_s, da_s, att_s, dqkv_s, bias_s, mask_s, acc_s, sq_s, t_s
):
    scale = HD**-0.5

    for n in range(6):
        two = dot(tok[...], wqkv[:, 256 * n : 256 * n + 256])
        qkv_s[2 * n, 0:ROWS] = two[:, 0:128]
        qkv_s[2 * n + 1, 0:ROWS] = two[:, 128:256]
    for n in range(2):
        two = dot(cot[...], wproj[256 * n : 256 * n + 256], NT)
        da_s[2 * n, 0:ROWS] = two[:, 0:128]
        da_s[2 * n + 1, 0:ROWS] = two[:, 128:256]
    for n in range(12):
        qkv_s[n, ROWS:PROWS] = jnp.zeros((PROWS - ROWS, 128), F32)
    for n in range(4):
        da_s[n, ROWS:PROWS] = jnp.zeros((PROWS - ROWS, 128), F32)

    sq_s[...] = jnp.zeros((128, 128), F32)
    sq_s[0:TOK, 0:TOK] = rel[...].astype(F32)
    sq_s[PAD : PAD + TOK, 0:TOK] = rel[...].astype(F32)
    relt = jnp.transpose(sq_s[...])[0:PAD].astype(jnp.int32)
    lane = lax.broadcasted_iota(jnp.int32, (PAD, 128), 1)
    sub = lax.broadcasted_iota(jnp.int32, (PAD, 128), 0)
    live = ((lane & 63) < TOK) & (sub < TOK)
    relt = jnp.where(live, relt, -1)
    safe = jnp.where(live, relt, 0)
    low_i = jnp.where(safe < 128, safe, 0)
    high_i = jnp.where(safe < 128, 0, safe - 128)
    is_low = safe < 128
    first = lane < 64
    for hp in range(HEADS // 2):
        looked = []
        for par in range(2):
            h = 2 * hp + par
            low = jnp.broadcast_to(tab[h : h + 1, 0:128], (8, 128))
            high = jnp.concatenate([tab[h : h + 1, 128:ENT], jnp.zeros((1, 256 - ENT), F32)], axis=1)
            high = jnp.broadcast_to(high, (8, 128))
            rows = []
            for b in range(PAD // 8):
                s = slice(8 * b, 8 * b + 8)
                a0 = jnp.take_along_axis(low, low_i[s], axis=1, mode="promise_in_bounds")
                a1 = jnp.take_along_axis(high, high_i[s], axis=1, mode="promise_in_bounds")
                rows.append(jnp.where(is_low[s], a0, a1))
            looked.append(jnp.concatenate(rows, axis=0))
        both = jnp.where(first, looked[0], looked[1])
        bias_s[hp * PAD : (hp + 1) * PAD] = jnp.where(sub < TOK, both, -1e30)

    sq_s[...] = jnp.zeros((128, 128), F32)
    sq_s[0:WIN, 0:TOK] = reg[...].astype(F32)
    base = sq_s[...]
    cols = jnp.transpose(base)
    for w in range(WIN):
        line = jnp.concatenate([base[w : w + 1, 0:64], base[w : w + 1, 0:64]], axis=1)
        mask_s[w * PAD : (w + 1) * PAD] = jnp.where(cols[0:PAD, w : w + 1] == line, 0.0, -100.0)

    acc_s[...] = jnp.zeros(acc_s.shape, F32)
    chan = lax.broadcasted_iota(jnp.int32, (PAD, 128), 1) // HD

    def spread(v):
        return jnp.concatenate([jnp.where(chan == h, v, 0.0) for h in range(4)], axis=0).astype(BF16)

    def fold(full):
        total = jnp.where(chan == 0, full[0:PAD], 0.0)
        for h in range(1, 4):
            total = jnp.where(chan == h, full[h * PAD : (h + 1) * PAD], total)
        return total

    def window(w, carry):
        here = pl.ds(w, PAD, stride=WIN)
        m1 = mask_s[pl.ds(pl.multiple_of(w * PAD, PAD), PAD), :]
        mask = jnp.concatenate([m1, m1], axis=1)
        for g in range(4):
            q = qkv_s[g, here, :]
            k = qkv_s[4 + g, here, :].astype(BF16)
            v = qkv_s[8 + g, here, :].astype(BF16)
            qd = spread(q)
            dd = spread(da_s[g, here, :])
            bias = jnp.concatenate(
                [bias_s[2 * g * PAD : (2 * g + 1) * PAD], bias_s[(2 * g + 1) * PAD : (2 * g + 2) * PAD]], axis=1
            )
            s = dot(k, qd, NT) * scale + bias + mask
            p = jnp.exp(s - jnp.max(s, axis=0, keepdims=True))
            p = p * (1.0 / jnp.sum(p, axis=0, keepdims=True))
            pb = p.astype(BF16)
            dp = dot(v, dd, NT).astype(BF16).astype(F32)
            ds = p * (dp - jnp.sum(dp * p, axis=0, keepdims=True))
            acc_s[2 * g * PAD : (2 * g + 1) * PAD] += ds[:, 0:128]
            acc_s[(2 * g + 1) * PAD : (2 * g + 2) * PAD] += ds[:, 128:256]
            dsb = (ds * scale).astype(BF16)
            dqkv_s[8 + g, here, :] = dot(pb, dd)
            dqkv_s[4 + g, here, :] = dot(dsb, qd)
            att_s[g, here, :] = fold(dot(jnp.transpose(pb), v))
            dqkv_s[g, here, :] = fold(dot(jnp.transpose(dsb), k))
        return carry

    lax.fori_loop(0, WIN, window, 0)

    ent = lax.broadcasted_iota(jnp.int32, (EPAD, 128), 0)
    sums = jnp.zeros((2 * EPAD, 16), F32)
    for j in range(TOK):
        part = acc_s[pl.ds(j, 8, stride=PAD), :]
        top = part.astype(BF16).astype(F32)
        rhs = jnp.concatenate([top, part - top], axis=0).astype(BF16)
        row = relt[j : j + 1]
        lo = jnp.where(lane[0:1] < 64, row, -1)
        hi = jnp.where(lane[0:1] < 64, -1, row)
        hot = jnp.concatenate([jnp.where(ent == lo, 1.0, 0.0), jnp.where(ent == hi, 1.0, 0.0)], axis=0)
        sums = sums + dot(hot.astype(BF16), rhs, NT)
    sums = jnp.concatenate([sums, jnp.zeros((2 * EPAD, 112), F32)], axis=1)
    sums = jnp.concatenate([sums, jnp.zeros((384 - 2 * EPAD, 128), F32)], axis=0)
    flat = jnp.concatenate([jnp.transpose(sums[128 * k : 128 * k + 128])[0:16] for k in range(3)], axis=1)
    table = jnp.concatenate([flat[0:8] + flat[8:16], jnp.zeros((8, 128), F32)], axis=1)
    keep[1024:1032] = table
    send[1024:1032] = table

    order = row_order(lax.axis_index("gz") & 1)

    def put(grad, n):
        cols = slice(256 * (n % 2), 256 * (n % 2) + 256)
        for k in range(16):
            rows = slice(64 * k + 16 * (n // 2), 64 * k + 16 * (n // 2) + 16)
            keep[rows, cols] = grad[16 * k : 16 * k + 16]
            send[rows, cols] = grad[256 + 16 * k : 272 + 16 * k]

    def pair(ref, n):
        return jnp.concatenate([ref[n, 0:ROWS].astype(BF16), ref[n + 1, 0:ROWS].astype(BF16)], axis=1)

    t_s[...] = dot(order, tok[...], NT).astype(BF16)
    for n in range(6):
        put(dot(t_s[...], pair(dqkv_s, 2 * n)), n)
    att = jnp.concatenate([pair(att_s, 0), pair(att_s, 2)], axis=1)
    t_s[...] = dot(order, att, NT).astype(BF16)
    for n in range(2):
        put(dot(t_s[...], cot[:, 256 * n : 256 * n + 256]), 6 + n)


def sum_core(keep, got, keep_table, got_table, out):
    table = keep_table[...] + got_table[...]
    for k in range(4):
        rows = slice(64 * k, 64 * k + 64)
        out[k, 0:64] = keep[rows] + got[rows]
        out[k, 64:72] = table


def sum_plane(got, out, acc):
    def total(rows):
        part = got[0, rows]
        for k in range(1, 4):
            part = part + got[k, rows]
        return part

    step = pl.program_id(0)

    @pl.when(step == 0)
    def _():
        acc[...] = total(slice(0, 72))

    @pl.when(step > 0)
    def _():
        acc[...] += total(slice(0, 72))

    @pl.when(step == 3)
    def _():
        table = acc[64:72]
        for z in range(8):
            for b in range(4):
                out[z, 2 * b : 2 * b + 2] = acc[16 * b + 2 * z : 16 * b + 2 * z + 2]
            out[z, 8:16] = table


def finish(got, mq, mp, mt, oq, op, ot):
    total = got[0]
    for k in range(1, 8):
        total = total + got[k]
    total = total * (1.0 / 4096)
    for e in range(2):
        for c in range(12):
            row, at = 2 * (c // 4) + e, 128 * (c % 4)
            r = slice(12 * e + c, 12 * e + c + 1)
            oq[r] = 0.9 * mq[r] + total[row : row + 1, at : at + 128]
        for c in range(4):
            r = slice(4 * e + c, 4 * e + c + 1)
            op[r] = 0.9 * mp[r] + total[6 + e : 7 + e, 128 * c : 128 * c + 128]
    for h in range(HEADS):
        at = (h % 2) * EPAD
        ot[h : h + 1] = 0.9 * mt[h : h + 1] + total[8 + h // 2 : 9 + h // 2, at : at + ENT]


def shapes(*dims):
    return tuple(jax.ShapeDtypeStruct(d, F32) for d in dims)


def local_grads(tok, cot, regions, rel_index, w_qkv, w_proj, table, interpret=False):
    return pl.pallas_call(
        local_kernel,
        out_shape=shapes((1032, 512), (1032, 512)),
        scratch_shapes=[
            pltpu.VMEM((12, PROWS, 128), F32),
            pltpu.VMEM((4, PROWS, 128), F32),
            pltpu.VMEM((4, PROWS, 128), F32),
            pltpu.VMEM((12, PROWS, 128), F32),
            pltpu.VMEM((8 * PAD, 128), F32),
            pltpu.VMEM((WIN * PAD, 128), F32),
            pltpu.VMEM((8 * PAD, 128), F32),
            pltpu.VMEM((128, 128), F32),
            pltpu.VMEM((D, ROWS), BF16),
        ],
        name="local_grads",
        interpret=interpret,
    )(tok, cot, regions, rel_index, w_qkv, w_proj, table)


def body(
    tokens, cotangent, regions, rel_index, w_qkv, w_proj, bias_table, mom_qkv, mom_proj, mom_table
):
    tok = jnp.transpose(tokens, (1, 0, 2)).reshape(ROWS, D)
    cot = jnp.transpose(cotangent, (1, 0, 2)).reshape(ROWS, D)
    keep, send = local_grads(tok, cot, regions, rel_index, w_qkv, w_proj, bias_table.T)
    got = shift(send, dc=1)
    wide = pl.BlockSpec((256, 512), lambda i: (i, 0))
    last = pl.BlockSpec((8, 512), lambda i: (128, 0))
    part = pl.BlockSpec((4, 72, 512), lambda i: (i, 0, 0))
    plane = pl.pallas_call(
        sum_core,
        grid=(4,),
        in_specs=[wide, wide, last, last],
        out_specs=part,
        out_shape=jax.ShapeDtypeStruct((16, 72, 512), F32),
        name="sum_core",
    )(keep, got, keep, got)
    plane = lax.all_to_all(plane, AXES, 0, 0, axis_index_groups=planes(), tiled=True)
    line = pl.pallas_call(
        sum_plane,
        grid=(4,),
        in_specs=[part],
        out_specs=pl.BlockSpec((8, 16, 512), lambda i: (0, 0, 0)),
        out_shape=jax.ShapeDtypeStruct((8, 16, 512), F32),
        scratch_shapes=[pltpu.VMEM((72, 512), F32)],
        name="sum_plane",
    )(plane)
    line = lax.all_to_all(line, "gy", 0, 0, tiled=True)
    new_q, new_p, new_t = pl.pallas_call(
        finish, out_shape=shapes((24, 128), (8, 128), (HEADS, ENT)), name="finish"
    )(line, mom_qkv.reshape(24, 128), mom_proj.reshape(8, 128), mom_table.T)
    return new_q.reshape(-1), new_p.reshape(-1), new_t.T


def solution(mesh):
    return jax.shard_map(
        body,
        mesh=mesh,
        in_specs=(
            P(AXES, None, None),
            P(AXES, None, None),
            P(AXES, None),
            P(),
            P(),
            P(),
            P(),
            P(AXES),
            P(AXES),
            P(),
        ),
        out_specs=(P(AXES), P(AXES), P()),
        check_vma=False,
    )
```

```python
import jax
import jax.numpy as jnp
from jax import lax
from jax.experimental import pallas as pl
from jax.experimental.pallas import tpu as pltpu
from jax.sharding import PartitionSpec as P

AXES = ("gx", "gy", "gz")
WIN = 16
TOK = 49
PAD = 64
D = 512
HEADS = 16
HD = 32
ENT = 169
EPAD = 176
ROWS = TOK * WIN
PROWS = PAD * WIN
F32 = jnp.float32
BF16 = jnp.bfloat16
NT = (((1,), (1,)), ((), ()))
NN = (((1,), (0,)), ((), ()))


def dot(a, b, dims=NN):
    return lax.dot_general(a, b, dims, preferred_element_type=F32)


def decode(flat):
    gx, gy, gz = flat // 32, (flat // 4) % 8, flat % 4
    return gx % 4, (gx // 4) * 2 + gz // 2, gy, gz % 2


def encode(x, y, z, c):
    x, y, z = x % 4, y % 4, z % 8
    return ((y // 2) * 4 + x) * 32 + z * 4 + (y % 2) * 2 + c


def shift(value, dx=0, dy=0, dz=0, dc=0):
    pairs = []
    for d in range(256):
        x, y, z, c = decode(d)
        pairs.append((d, encode(x + dx, y + dy, z + dz, c ^ dc)))
    return lax.ppermute(value, AXES, pairs)


def planes():
    return [[encode(x, y, z, c) for y in range(4) for x in range(4)] for z in range(8) for c in range(2)]


def row_order(core):
    r = lax.broadcasted_iota(jnp.int32, (D, 128), 0)
    e = r & 1
    z = (r >> 1) & 7
    x = (r >> 4) & 3
    y = (r >> 6) & 3
    c = ((r >> 8) + core) & 1
    orig = ((((y >> 1) * 4 + x) * 32 + z * 4 + (y & 1) * 2 + c) << 1) + e
    col = lax.broadcasted_iota(jnp.int32, (D, 128), 1)
    parts = [jnp.where(orig == col + 128 * k, 1.0, 0.0) for k in range(4)]
    return jnp.concatenate(parts, axis=1).astype(BF16)


def local_kernel(
    tok, cot, reg, rel, wqkv, wproj, tab, keep, send, qkv_s, da_s, att_s, dqkv_s, bias_s, mask_s, acc_s, sq_s, t_s
):
    scale = HD**-0.5

    for n in range(6):
        two = dot(tok[...], wqkv[:, 256 * n : 256 * n + 256])
        qkv_s[2 * n, 0:ROWS] = two[:, 0:128]
        qkv_s[2 * n + 1, 0:ROWS] = two[:, 128:256]
    for n in range(2):
        two = dot(cot[...], wproj[256 * n : 256 * n + 256], NT)
        da_s[2 * n, 0:ROWS] = two[:, 0:128]
        da_s[2 * n + 1, 0:ROWS] = two[:, 128:256]
    for n in range(12):
        qkv_s[n, ROWS:PROWS] = jnp.zeros((PROWS - ROWS, 128), F32)
    for n in range(4):
        da_s[n, ROWS:PROWS] = jnp.zeros((PROWS - ROWS, 128), F32)

    sq_s[...] = jnp.zeros((128, 128), F32)
    sq_s[0:TOK, 0:TOK] = rel[...].astype(F32)
    sq_s[PAD : PAD + TOK, 0:TOK] = rel[...].astype(F32)
    relt = jnp.transpose(sq_s[...])[0:PAD].astype(jnp.int32)
    lane = lax.broadcasted_iota(jnp.int32, (PAD, 128), 1)
    sub = lax.broadcasted_iota(jnp.int32, (PAD, 128), 0)
    live = ((lane & 63) < TOK) & (sub < TOK)
    relt = jnp.where(live, relt, -1)
    safe = jnp.where(live, relt, 0)
    low_i = jnp.where(safe < 128, safe, 0)
    high_i = jnp.where(safe < 128, 0, safe - 128)
    is_low = safe < 128
    first = lane < 64
    for hp in range(HEADS // 2):
        looked = []
        for par in range(2):
            h = 2 * hp + par
            low = jnp.broadcast_to(tab[h : h + 1, 0:128], (8, 128))
            high = jnp.concatenate([tab[h : h + 1, 128:ENT], jnp.zeros((1, 256 - ENT), F32)], axis=1)
            high = jnp.broadcast_to(high, (8, 128))
            rows = []
            for b in range(PAD // 8):
                s = slice(8 * b, 8 * b + 8)
                a0 = jnp.take_along_axis(low, low_i[s], axis=1, mode="promise_in_bounds")
                a1 = jnp.take_along_axis(high, high_i[s], axis=1, mode="promise_in_bounds")
                rows.append(jnp.where(is_low[s], a0, a1))
            looked.append(jnp.concatenate(rows, axis=0))
        both = jnp.where(first, looked[0], looked[1])
        bias_s[hp * PAD : (hp + 1) * PAD] = jnp.where(sub < TOK, both, -1e30)

    sq_s[...] = jnp.zeros((128, 128), F32)
    sq_s[0:WIN, 0:TOK] = reg[...].astype(F32)
    base = sq_s[...]
    cols = jnp.transpose(base)
    for w in range(WIN):
        line = jnp.concatenate([base[w : w + 1, 0:64], base[w : w + 1, 0:64]], axis=1)
        mask_s[w * PAD : (w + 1) * PAD] = jnp.where(cols[0:PAD, w : w + 1] == line, 0.0, -100.0)

    acc_s[...] = jnp.zeros(acc_s.shape, F32)
    chan = lax.broadcasted_iota(jnp.int32, (PAD, 128), 1) // HD

    def spread(v):
        return jnp.concatenate([jnp.where(chan == h, v, 0.0) for h in range(4)], axis=0).astype(BF16)

    def fold(full):
        total = jnp.where(chan == 0, full[0:PAD], 0.0)
        for h in range(1, 4):
            total = jnp.where(chan == h, full[h * PAD : (h + 1) * PAD], total)
        return total

    def window(w, carry):
        here = pl.ds(w, PAD, stride=WIN)
        m1 = mask_s[pl.ds(pl.multiple_of(w * PAD, PAD), PAD), :]
        mask = jnp.concatenate([m1, m1], axis=1)
        for g in range(4):
            q = qkv_s[g, here, :]
            k = qkv_s[4 + g, here, :].astype(BF16)
            v = qkv_s[8 + g, here, :].astype(BF16)
            qd = spread(q)
            dd = spread(da_s[g, here, :])
            bias = jnp.concatenate(
                [bias_s[2 * g * PAD : (2 * g + 1) * PAD], bias_s[(2 * g + 1) * PAD : (2 * g + 2) * PAD]], axis=1
            )
            s = dot(k, qd, NT) * scale + bias + mask
            p = jnp.exp(s - jnp.max(s, axis=0, keepdims=True))
            p = p * (1.0 / jnp.sum(p, axis=0, keepdims=True))
            pb = p.astype(BF16)
            dp = dot(v, dd, NT).astype(BF16).astype(F32)
            ds = p * (dp - jnp.sum(dp * p, axis=0, keepdims=True))
            acc_s[2 * g * PAD : (2 * g + 1) * PAD] += ds[:, 0:128]
            acc_s[(2 * g + 1) * PAD : (2 * g + 2) * PAD] += ds[:, 128:256]
            dsb = (ds * scale).astype(BF16)
            dqkv_s[8 + g, here, :] = dot(pb, dd)
            dqkv_s[4 + g, here, :] = dot(dsb, qd)
            att_s[g, here, :] = fold(dot(jnp.transpose(pb), v))
            dqkv_s[g, here, :] = fold(dot(jnp.transpose(dsb), k))
        return carry

    lax.fori_loop(0, WIN, window, 0)

    ent = lax.broadcasted_iota(jnp.int32, (EPAD, 128), 0)
    sums = jnp.zeros((2 * EPAD, 16), F32)
    for j in range(TOK):
        part = acc_s[pl.ds(j, 8, stride=PAD), :]
        top = part.astype(BF16).astype(F32)
        rhs = jnp.concatenate([top, part - top], axis=0).astype(BF16)
        row = relt[j : j + 1]
        lo = jnp.where(lane[0:1] < 64, row, -1)
        hi = jnp.where(lane[0:1] < 64, -1, row)
        hot = jnp.concatenate([jnp.where(ent == lo, 1.0, 0.0), jnp.where(ent == hi, 1.0, 0.0)], axis=0)
        sums = sums + dot(hot.astype(BF16), rhs, NT)
    sums = jnp.concatenate([sums, jnp.zeros((2 * EPAD, 112), F32)], axis=1)
    sums = jnp.concatenate([sums, jnp.zeros((384 - 2 * EPAD, 128), F32)], axis=0)
    flat = jnp.concatenate([jnp.transpose(sums[128 * k : 128 * k + 128])[0:16] for k in range(3)], axis=1)
    table = jnp.concatenate([flat[0:8] + flat[8:16], jnp.zeros((8, 128), F32)], axis=1)
    keep[1024:1032] = table
    send[1024:1032] = table

    order = row_order(lax.axis_index("gz") & 1)

    def put(grad, n):
        cols = slice(256 * (n % 2), 256 * (n % 2) + 256)
        for k in range(16):
            rows = slice(64 * k + 16 * (n // 2), 64 * k + 16 * (n // 2) + 16)
            keep[rows, cols] = grad[16 * k : 16 * k + 16]
            send[rows, cols] = grad[256 + 16 * k : 272 + 16 * k]

    def pair(ref, n):
        return jnp.concatenate([ref[n, 0:ROWS].astype(BF16), ref[n + 1, 0:ROWS].astype(BF16)], axis=1)

    t_s[...] = dot(order, tok[...], NT).astype(BF16)
    for n in range(6):
        put(dot(t_s[...], pair(dqkv_s, 2 * n)), n)
    att = jnp.concatenate([pair(att_s, 0), pair(att_s, 2)], axis=1)
    t_s[...] = dot(order, att, NT).astype(BF16)
    for n in range(2):
        put(dot(t_s[...], cot[:, 256 * n : 256 * n + 256]), 6 + n)


def sum_core(keep, got, keep_table, got_table, out):
    table = keep_table[...] + got_table[...]
    for k in range(4):
        rows = slice(64 * k, 64 * k + 64)
        out[k, 0:64] = keep[rows] + got[rows]
        out[k, 64:72] = table


def sum_plane(got, out, acc):
    def total(rows):
        part = got[0, rows]
        for k in range(1, 4):
            part = part + got[k, rows]
        return part

    step = pl.program_id(0)

    @pl.when(step == 0)
    def _():
        acc[...] = total(slice(0, 72))

    @pl.when(step > 0)
    def _():
        acc[...] += total(slice(0, 72))

    @pl.when(step == 3)
    def _():
        table = acc[64:72]
        for z in range(8):
            for b in range(4):
                out[z, 2 * b : 2 * b + 2] = acc[16 * b + 2 * z : 16 * b + 2 * z + 2]
            out[z, 8:16] = table


def finish(got, mq, mp, mt, oq, op, ot):
    total = got[0]
    for k in range(1, 8):
        total = total + got[k]
    total = total * (1.0 / 4096)
    for e in range(2):
        for c in range(12):
            row, at = 2 * (c // 4) + e, 128 * (c % 4)
            r = slice(12 * e + c, 12 * e + c + 1)
            oq[r] = 0.9 * mq[r] + total[row : row + 1, at : at + 128]
        for c in range(4):
            r = slice(4 * e + c, 4 * e + c + 1)
            op[r] = 0.9 * mp[r] + total[6 + e : 7 + e, 128 * c : 128 * c + 128]
    for h in range(HEADS):
        at = (h % 2) * EPAD
        ot[h : h + 1] = 0.9 * mt[h : h + 1] + total[8 + h // 2 : 9 + h // 2, at : at + ENT]


def shapes(*dims):
    return tuple(jax.ShapeDtypeStruct(d, F32) for d in dims)


def local_grads(tok, cot, regions, rel_index, w_qkv, w_proj, table, interpret=False):
    return pl.pallas_call(
        local_kernel,
        out_shape=shapes((1032, 512), (1032, 512)),
        scratch_shapes=[
            pltpu.VMEM((12, PROWS, 128), F32),
            pltpu.VMEM((4, PROWS, 128), F32),
            pltpu.VMEM((4, PROWS, 128), F32),
            pltpu.VMEM((12, PROWS, 128), F32),
            pltpu.VMEM((8 * PAD, 128), F32),
            pltpu.VMEM((WIN * PAD, 128), F32),
            pltpu.VMEM((8 * PAD, 128), F32),
            pltpu.VMEM((128, 128), F32),
            pltpu.VMEM((D, ROWS), BF16),
        ],
        name="local_grads",
        compiler_params=pltpu.CompilerParams(vmem_limit_bytes=40 << 20),
        interpret=interpret,
    )(tok, cot, regions, rel_index, w_qkv, w_proj, table)


def body(
    tokens, cotangent, regions, rel_index, w_qkv, w_proj, bias_table, mom_qkv, mom_proj, mom_table
):
    tok = jnp.transpose(tokens, (1, 0, 2)).reshape(ROWS, D)
    cot = jnp.transpose(cotangent, (1, 0, 2)).reshape(ROWS, D)
    keep, send = local_grads(tok, cot, regions, rel_index, w_qkv, w_proj, bias_table.T)
    got = shift(send, dc=1)
    wide = pl.BlockSpec((256, 512), lambda i: (i, 0))
    last = pl.BlockSpec((8, 512), lambda i: (128, 0))
    part = pl.BlockSpec((4, 72, 512), lambda i: (i, 0, 0))
    plane = pl.pallas_call(
        sum_core,
        grid=(4,),
        in_specs=[wide, wide, last, last],
        out_specs=part,
        out_shape=jax.ShapeDtypeStruct((16, 72, 512), F32),
        name="sum_core",
        compiler_params=pltpu.CompilerParams(vmem_limit_bytes=12 << 20),
    )(keep, got, keep, got)
    plane = lax.all_to_all(plane, AXES, 0, 0, axis_index_groups=planes(), tiled=True)
    line = pl.pallas_call(
        sum_plane,
        grid=(4,),
        in_specs=[part],
        out_specs=pl.BlockSpec((8, 16, 512), lambda i: (0, 0, 0)),
        out_shape=jax.ShapeDtypeStruct((8, 16, 512), F32),
        scratch_shapes=[pltpu.VMEM((72, 512), F32)],
        name="sum_plane",
        compiler_params=pltpu.CompilerParams(vmem_limit_bytes=12 << 20),
    )(plane)
    line = lax.all_to_all(line, "gy", 0, 0, tiled=True)
    new_q, new_p, new_t = pl.pallas_call(
        finish,
        out_shape=shapes((24, 128), (8, 128), (HEADS, ENT)),
        name="finish",
        compiler_params=pltpu.CompilerParams(vmem_limit_bytes=4 << 20),
    )(line, mom_qkv.reshape(24, 128), mom_proj.reshape(8, 128), mom_table.T)
    return new_q.reshape(-1), new_p.reshape(-1), new_t.T


def solution(mesh):
    return jax.shard_map(
        body,
        mesh=mesh,
        in_specs=(
            P(AXES, None, None),
            P(AXES, None, None),
            P(AXES, None),
            P(),
            P(),
            P(),
            P(),
            P(AXES),
            P(AXES),
            P(),
        ),
        out_specs=(P(AXES), P(AXES), P()),
        check_vma=False,
    )
```

```python
import jax
import jax.numpy as jnp
from jax import lax
from jax.experimental import pallas as pl
from jax.experimental.pallas import tpu as pltpu
from jax.sharding import PartitionSpec as P

AXES = ("gx", "gy", "gz")
WIN = 16
TOK = 49
PAD = 64
D = 512
HEADS = 16
HD = 32
ENT = 169
EPAD = 176
UNROLL = 4
AHEAD = 1
ROWS = TOK * WIN
PROWS = PAD * WIN
F32 = jnp.float32
BF16 = jnp.bfloat16
NT = (((1,), (1,)), ((), ()))
NN = (((1,), (0,)), ((), ()))


def dot(a, b, dims=NN):
    return lax.dot_general(a, b, dims, preferred_element_type=F32)


def decode(flat):
    gx, gy, gz = flat // 32, (flat // 4) % 8, flat % 4
    return gx % 4, (gx // 4) * 2 + gz // 2, gy, gz % 2


def encode(x, y, z, c):
    x, y, z = x % 4, y % 4, z % 8
    return ((y // 2) * 4 + x) * 32 + z * 4 + (y % 2) * 2 + c


def shift(value, dx=0, dy=0, dz=0, dc=0):
    pairs = []
    for d in range(256):
        x, y, z, c = decode(d)
        pairs.append((d, encode(x + dx, y + dy, z + dz, c ^ dc)))
    return lax.ppermute(value, AXES, pairs)


def planes():
    return [[encode(x, y, z, c) for y in range(4) for x in range(4)] for z in range(8) for c in range(2)]


def row_order(core):
    r = lax.broadcasted_iota(jnp.int32, (D, 128), 0)
    e = r & 1
    z = (r >> 1) & 7
    x = (r >> 4) & 3
    y = (r >> 6) & 3
    c = ((r >> 8) + core) & 1
    orig = ((((y >> 1) * 4 + x) * 32 + z * 4 + (y & 1) * 2 + c) << 1) + e
    col = lax.broadcasted_iota(jnp.int32, (D, 128), 1)
    parts = [jnp.where(orig == col + 128 * k, 1.0, 0.0) for k in range(4)]
    return jnp.concatenate(parts, axis=1).astype(BF16)


def local_kernel(
    tok_h, cot_h, reg_h, rel_h, wqkv_h, wproj_h, tab_h, keep, send,
    tok, cot, reg, rel, wqkv, wproj, tab, sems, pick_s, tokw, cotw, qkv_s, da_s, att_s, dqkv_s, bias_s, mask_s, acc_s, sq_s, t_s,
):
    moves = [
        pltpu.make_async_copy(src, dst, sems.at[n])
        for n, (src, dst) in enumerate(
            zip((rel_h, reg_h, tab_h, tok_h, wqkv_h, cot_h, wproj_h), (rel, reg, tab, tok, wqkv, cot, wproj))
        )
    ]
    for move in moves:
        move.start()
    factor = 1.4426950408889634
    scale = HD**-0.5

    line = lax.broadcasted_iota(jnp.int32, (256, 128), 0)
    lanes = lax.broadcasted_iota(jnp.int32, (256, 128), 1)
    for b in range(4):
        t = line & 63
        source = jnp.where(t < TOK, t * WIN + (line >> 6) + 4 * b, -1)
        for k in range(7):
            n = min(128, ROWS - 128 * k)
            hot = jnp.where(source == lanes + 128 * k, 1.0, 0.0).astype(BF16)
            pick_s[256 * b : 256 * b + 256, 128 * k : 128 * k + n] = hot[:, 0:n]

    for move in moves[0:3]:
        move.wait()

    sq_s[...] = jnp.zeros((128, 128), F32)
    sq_s[0:TOK, 0:TOK] = rel[...].astype(F32)
    sq_s[PAD : PAD + TOK, 0:TOK] = rel[...].astype(F32)
    relt = jnp.transpose(sq_s[...])[0:PAD].astype(jnp.int32)
    lane = lax.broadcasted_iota(jnp.int32, (PAD, 128), 1)
    sub = lax.broadcasted_iota(jnp.int32, (PAD, 128), 0)
    live = ((lane & 63) < TOK) & (sub < TOK)
    relt = jnp.where(live, relt, -1)
    safe = jnp.where(live, relt, 0)
    low_i = jnp.where(safe < 128, safe, 0)
    high_i = jnp.where(safe < 128, 0, safe - 128)
    is_low = safe < 128
    first = lane < 64
    for hp in range(HEADS // 2):
        looked = []
        for par in range(2):
            h = 2 * hp + par
            low = jnp.broadcast_to(tab[h : h + 1, 0:128], (8, 128))
            high = jnp.concatenate([tab[h : h + 1, 128:ENT], jnp.zeros((1, 256 - ENT), F32)], axis=1)
            high = jnp.broadcast_to(high, (8, 128))
            rows = []
            for b in range(PAD // 8):
                s = slice(8 * b, 8 * b + 8)
                a0 = jnp.take_along_axis(low, low_i[s], axis=1, mode="promise_in_bounds")
                a1 = jnp.take_along_axis(high, high_i[s], axis=1, mode="promise_in_bounds")
                rows.append(jnp.where(is_low[s], a0, a1))
            looked.append(jnp.concatenate(rows, axis=0))
        both = jnp.where(first, looked[0], looked[1])
        bias_s[hp * PAD : (hp + 1) * PAD] = jnp.where(sub < TOK, both * factor, -1e30)

    sq_s[...] = jnp.zeros((128, 128), F32)
    sq_s[0:WIN, 0:TOK] = reg[...].astype(F32)
    base = sq_s[...]
    cols = jnp.transpose(base)
    for w in range(WIN):
        row = jnp.concatenate([base[w : w + 1, 0:64], base[w : w + 1, 0:64]], axis=1)
        mask_s[w * PAD : (w + 1) * PAD] = jnp.where(cols[0:PAD, w : w + 1] == row, 0.0, -100.0 * factor)

    acc_s[...] = jnp.zeros(acc_s.shape, F32)

    moves[3].wait()
    for b in range(4):
        rows = slice(256 * b, 256 * b + 256)
        tokw[rows] = dot(pick_s[rows], tok[...]).astype(BF16)
    moves[4].wait()
    for n in range(6):
        cols = slice(256 * n, 256 * n + 256)
        qkv_s[:, cols] = dot(tokw[...], wqkv[:, cols]).astype(BF16)
    moves[5].wait()
    for b in range(4):
        rows = slice(256 * b, 256 * b + 256)
        cotw[rows] = dot(pick_s[rows], cot[...]).astype(BF16)
    moves[6].wait()
    for n in range(2):
        cols = slice(256 * n, 256 * n + 256)
        da_s[:, cols] = dot(cotw[...], wproj[cols], NT).astype(BF16)

    chan = lax.broadcasted_iota(jnp.int32, (PAD, 128), 1) // HD
    none = jnp.zeros((PAD, 128), BF16)

    def spread(v):
        return jnp.concatenate([jnp.where(chan == h, v, none) for h in range(4)], axis=0)

    def fold(full):
        total = full[0:PAD]
        for h in range(1, 4):
            total = jnp.where(chan == h, full[h * PAD : (h + 1) * PAD], total)
        return total.astype(BF16)

    def scores(rows, mask, g):
        cq = slice(g * 128, g * 128 + 128)
        k = qkv_s[rows, D + g * 128 : D + g * 128 + 128]
        v = qkv_s[rows, 2 * D + g * 128 : 2 * D + g * 128 + 128]
        qd = spread(qkv_s[rows, cq])
        dd = spread(da_s[rows, cq])
        return dict(rows=rows, mask=mask, g=g, k=k, v=v, qd=qd, dd=dd, s=dot(k, qd, NT), dp=dot(v, dd, NT))

    def softmax(it):
        g, mask = it["g"], it["mask"]
        bias = jnp.concatenate(
            [bias_s[2 * g * PAD : (2 * g + 1) * PAD] + mask, bias_s[(2 * g + 1) * PAD : (2 * g + 2) * PAD] + mask], axis=1
        )
        s = it["s"] * (scale * factor) + bias
        p = jnp.exp2(s - jnp.max(s, axis=0, keepdims=True))
        p = p * (1.0 / jnp.sum(p, axis=0, keepdims=True))
        dp = it["dp"].astype(BF16).astype(F32)
        ds = p * (dp - jnp.sum(dp * p, axis=0, keepdims=True))
        it["pb"] = p.astype(BF16)
        it["dsb"] = (ds * scale).astype(BF16)
        it["pt"] = jnp.transpose(it["pb"])
        it["dst"] = jnp.transpose(it["dsb"])
        return ds

    def results(it):
        rows, g = it["rows"], it["g"]
        cq = slice(g * 128, g * 128 + 128)
        dqkv_s[rows, 2 * D + g * 128 : 2 * D + g * 128 + 128] = dot(it["pb"], it["dd"]).astype(BF16)
        att_s[rows, cq] = fold(dot(it["pt"], it["v"]))
        dqkv_s[rows, D + g * 128 : D + g * 128 + 128] = dot(it["dsb"], it["qd"]).astype(BF16)
        dqkv_s[rows, cq] = fold(dot(it["dst"], it["k"]))

    def windows(step, carry):
        chains = []
        for g in range(4):
            for i in range(UNROLL):
                rows = pl.ds(pl.multiple_of((step * UNROLL + i) * PAD, PAD), PAD)
                chains.append((rows, i, g))
        masks = [mask_s[pl.ds(pl.multiple_of((step * UNROLL + i) * PAD, PAD), PAD), :] for i in range(UNROLL)]
        sums = [None] * 4
        items = []
        for c in range(len(chains) + 1 + AHEAD):
            if c < len(chains):
                rows, i, g = chains[c]
                items.append(scores(rows, masks[i], g))
            if 0 <= c - AHEAD < len(chains):
                it = items[c - AHEAD]
                ds = softmax(it)
                g = it["g"]
                sums[g] = ds if sums[g] is None else sums[g] + ds
                if c - AHEAD == UNROLL * g + UNROLL - 1:
                    acc_s[2 * g * PAD : (2 * g + 1) * PAD] += sums[g][:, 0:128]
                    acc_s[(2 * g + 1) * PAD : (2 * g + 2) * PAD] += sums[g][:, 128:256]
            if c - AHEAD - 1 >= 0:
                results(items[c - AHEAD - 1])
        return carry

    lax.fori_loop(0, WIN // UNROLL, windows, 0)

    ent = lax.broadcasted_iota(jnp.int32, (EPAD, 128), 0)
    sums = jnp.zeros((2 * EPAD, 16), F32)
    for j7 in range(7):
        hots, parts = [], []
        for j in range(7 * j7, 7 * j7 + 7):
            part = acc_s[pl.ds(j, 8, stride=PAD), :]
            top = part.astype(BF16).astype(F32)
            parts.append(jnp.concatenate([top, part - top], axis=0).astype(BF16))
            row = relt[j : j + 1]
            lo = jnp.where(lane[0:1] < 64, row, -1)
            hi = jnp.where(lane[0:1] < 64, -1, row)
            hot = jnp.concatenate([jnp.where(ent == lo, 1.0, 0.0), jnp.where(ent == hi, 1.0, 0.0)], axis=0)
            hots.append(hot.astype(BF16))
        sums = sums + dot(jnp.concatenate(hots, axis=1), jnp.concatenate(parts, axis=1), NT)
    sums = jnp.concatenate([sums, jnp.zeros((2 * EPAD, 112), F32)], axis=1)
    sums = jnp.concatenate([sums, jnp.zeros((384 - 2 * EPAD, 128), F32)], axis=0)
    flat = jnp.concatenate([jnp.transpose(sums[128 * k : 128 * k + 128])[0:16] for k in range(3)], axis=1)
    table = jnp.concatenate([flat[0:8] + flat[8:16], jnp.zeros((8, 128), F32)], axis=1)
    keep[1024:1032] = table
    send[1024:1032] = table

    order = row_order(lax.axis_index("gz") & 1)

    def put(grad, n):
        cols = slice(256 * (n % 2), 256 * (n % 2) + 256)
        for k in range(16):
            rows = slice(64 * k + 16 * (n // 2), 64 * k + 16 * (n // 2) + 16)
            keep[rows, cols] = grad[16 * k : 16 * k + 16]
            send[rows, cols] = grad[256 + 16 * k : 272 + 16 * k]

    t_s[...] = dot(order, tokw[...], NT).astype(BF16)
    for n in range(6):
        put(dot(t_s[...], dqkv_s[:, 256 * n : 256 * n + 256]), n)
    t_s[...] = dot(order, att_s[...], NT).astype(BF16)
    for n in range(2):
        put(dot(t_s[...], cotw[:, 256 * n : 256 * n + 256]), 6 + n)


def sum_core(keep, got, keep_table, got_table, out):
    table = keep_table[...] + got_table[...]
    for k in range(4):
        rows = slice(64 * k, 64 * k + 64)
        out[k, 0:64] = keep[rows] + got[rows]
        out[k, 64:72] = table


def sum_plane(got, out, acc):
    def total(rows):
        part = got[0, rows]
        for k in range(1, 4):
            part = part + got[k, rows]
        return part

    step = pl.program_id(0)

    @pl.when(step == 0)
    def _():
        acc[...] = total(slice(0, 72))

    @pl.when(step > 0)
    def _():
        acc[...] += total(slice(0, 72))

    @pl.when(step == 3)
    def _():
        table = acc[64:72]
        for z in range(8):
            for b in range(4):
                out[z, 2 * b : 2 * b + 2] = acc[16 * b + 2 * z : 16 * b + 2 * z + 2]
            out[z, 8:16] = table


def finish(got, mq, mp, mt, oq, op, ot):
    total = got[0]
    for k in range(1, 8):
        total = total + got[k]
    total = total * (1.0 / 4096)
    for e in range(2):
        for c in range(12):
            row, at = 2 * (c // 4) + e, 128 * (c % 4)
            r = slice(12 * e + c, 12 * e + c + 1)
            oq[r] = 0.9 * mq[r] + total[row : row + 1, at : at + 128]
        for c in range(4):
            r = slice(4 * e + c, 4 * e + c + 1)
            op[r] = 0.9 * mp[r] + total[6 + e : 7 + e, 128 * c : 128 * c + 128]
    for h in range(HEADS):
        at = (h % 2) * EPAD
        ot[h : h + 1] = 0.9 * mt[h : h + 1] + total[8 + h // 2 : 9 + h // 2, at : at + ENT]


def shapes(*dims):
    return tuple(jax.ShapeDtypeStruct(d, F32) for d in dims)


def local_grads(tok, cot, regions, rel_index, w_qkv, w_proj, table, interpret=False):
    return pl.pallas_call(
        local_kernel,
        out_shape=shapes((1032, 512), (1032, 512)),
        in_specs=[pl.BlockSpec(memory_space=pltpu.HBM)] * 7,
        scratch_shapes=[
            pltpu.VMEM((ROWS, D), BF16),
            pltpu.VMEM((ROWS, D), BF16),
            pltpu.VMEM((WIN, TOK), jnp.int32),
            pltpu.VMEM((TOK, TOK), jnp.int32),
            pltpu.VMEM((D, 3 * D), BF16),
            pltpu.VMEM((D, D), BF16),
            pltpu.VMEM((HEADS, ENT), F32),
            pltpu.SemaphoreType.DMA((7,)),
            pltpu.VMEM((PROWS, ROWS), BF16),
            pltpu.VMEM((PROWS, D), BF16),
            pltpu.VMEM((PROWS, D), BF16),
            pltpu.VMEM((PROWS, 3 * D), BF16),
            pltpu.VMEM((PROWS, D), BF16),
            pltpu.VMEM((PROWS, D), BF16),
            pltpu.VMEM((PROWS, 3 * D), BF16),
            pltpu.VMEM((8 * PAD, 128), F32),
            pltpu.VMEM((WIN * PAD, 128), F32),
            pltpu.VMEM((8 * PAD, 128), F32),
            pltpu.VMEM((128, 128), F32),
            pltpu.VMEM((D, PROWS), BF16),
        ],
        name="local_grads",
        compiler_params=pltpu.CompilerParams(vmem_limit_bytes=40 << 20),
        interpret=interpret,
    )(tok, cot, regions, rel_index, w_qkv, w_proj, table)


def body(
    tokens, cotangent, regions, rel_index, w_qkv, w_proj, bias_table, mom_qkv, mom_proj, mom_table
):
    tok = jnp.transpose(tokens, (1, 0, 2)).reshape(ROWS, D)
    cot = jnp.transpose(cotangent, (1, 0, 2)).reshape(ROWS, D)
    keep, send = local_grads(tok, cot, regions, rel_index, w_qkv, w_proj, bias_table.T)
    got = shift(send, dc=1)
    wide = pl.BlockSpec((256, 512), lambda i: (i, 0))
    last = pl.BlockSpec((8, 512), lambda i: (128, 0))
    part = pl.BlockSpec((4, 72, 512), lambda i: (i, 0, 0))
    plane = pl.pallas_call(
        sum_core,
        grid=(4,),
        in_specs=[wide, wide, last, last],
        out_specs=part,
        out_shape=jax.ShapeDtypeStruct((16, 72, 512), F32),
        name="sum_core",
        compiler_params=pltpu.CompilerParams(vmem_limit_bytes=12 << 20),
    )(keep, got, keep, got)
    plane = lax.all_to_all(plane, AXES, 0, 0, axis_index_groups=planes(), tiled=True)
    line = pl.pallas_call(
        sum_plane,
        grid=(4,),
        in_specs=[part],
        out_specs=pl.BlockSpec((8, 16, 512), lambda i: (0, 0, 0)),
        out_shape=jax.ShapeDtypeStruct((8, 16, 512), F32),
        scratch_shapes=[pltpu.VMEM((72, 512), F32)],
        name="sum_plane",
        compiler_params=pltpu.CompilerParams(vmem_limit_bytes=12 << 20),
    )(plane)
    line = lax.all_to_all(line, "gy", 0, 0, tiled=True)
    new_q, new_p, new_t = pl.pallas_call(
        finish,
        out_shape=shapes((24, 128), (8, 128), (HEADS, ENT)),
        name="finish",
        compiler_params=pltpu.CompilerParams(vmem_limit_bytes=4 << 20),
    )(line, mom_qkv.reshape(24, 128), mom_proj.reshape(8, 128), mom_table.T)
    return new_q.reshape(-1), new_p.reshape(-1), new_t.T


def solution(mesh):
    return jax.shard_map(
        body,
        mesh=mesh,
        in_specs=(
            P(AXES, None, None),
            P(AXES, None, None),
            P(AXES, None),
            P(),
            P(),
            P(),
            P(),
            P(AXES),
            P(AXES),
            P(),
        ),
        out_specs=(P(AXES), P(AXES), P()),
        check_vma=False,
    )
```

```python
import jax
import jax.numpy as jnp
from jax import lax
from jax.experimental import pallas as pl
from jax.experimental.pallas import tpu as pltpu
from jax.sharding import PartitionSpec as P

AXES = ("gx", "gy", "gz")
WIN = 16
TOK = 49
PAD = 64
D = 512
HEADS = 16
HD = 32
ENT = 169
EPAD = 176
UNROLL = 4
AHEAD = 1
ROWS = TOK * WIN
PROWS = PAD * WIN
F32 = jnp.float32
BF16 = jnp.bfloat16
NT = (((1,), (1,)), ((), ()))
NN = (((1,), (0,)), ((), ()))


def dot(a, b, dims=NN):
    return lax.dot_general(a, b, dims, preferred_element_type=F32)


def decode(flat):
    gx, gy, gz = flat // 32, (flat // 4) % 8, flat % 4
    return gx % 4, (gx // 4) * 2 + gz // 2, gy, gz % 2


def encode(x, y, z, c):
    x, y, z = x % 4, y % 4, z % 8
    return ((y // 2) * 4 + x) * 32 + z * 4 + (y % 2) * 2 + c


def shift(value, dx=0, dy=0, dz=0, dc=0):
    pairs = []
    for d in range(256):
        x, y, z, c = decode(d)
        pairs.append((d, encode(x + dx, y + dy, z + dz, c ^ dc)))
    return lax.ppermute(value, AXES, pairs)


def planes():
    return [[encode(x, y, z, c) for y in range(4) for x in range(4)] for z in range(8) for c in range(2)]


def row_order(core):
    r = lax.broadcasted_iota(jnp.int32, (D, 128), 0)
    e = r & 1
    z = (r >> 1) & 7
    x = (r >> 4) & 3
    y = (r >> 6) & 3
    c = ((r >> 8) + core) & 1
    orig = ((((y >> 1) * 4 + x) * 32 + z * 4 + (y & 1) * 2 + c) << 1) + e
    col = lax.broadcasted_iota(jnp.int32, (D, 128), 1)
    parts = [jnp.where(orig == col + 128 * k, 1.0, 0.0) for k in range(4)]
    return jnp.concatenate(parts, axis=1).astype(BF16)


def local_kernel(
    tok_h, cot_h, reg_h, rel_h, wqkv_h, wproj_h, tab_h, keep, send,
    tok, cot, reg, rel, wqkv, wproj, tab, sems, pick_s, tokw, cotw, qkv_s, da_s, att_s, dqkv_s, bias_s, mask_s, acc_s, sq_s, t_s,
):
    moves = [
        pltpu.make_async_copy(src, dst, sems.at[n])
        for n, (src, dst) in enumerate(
            zip((rel_h, reg_h, tab_h, tok_h, wqkv_h, cot_h, wproj_h), (rel, reg, tab, tok, wqkv, cot, wproj))
        )
    ]
    for move in moves:
        move.start()
    factor = 1.4426950408889634
    scale = HD**-0.5

    line = lax.broadcasted_iota(jnp.int32, (256, 128), 0)
    lanes = lax.broadcasted_iota(jnp.int32, (256, 128), 1)
    for b in range(4):
        t = line & 63
        source = jnp.where(t < TOK, t * WIN + (line >> 6) + 4 * b, -1)
        for k in range(7):
            n = min(128, ROWS - 128 * k)
            hot = jnp.where(source == lanes + 128 * k, 1.0, 0.0).astype(BF16)
            pick_s[256 * b : 256 * b + 256, 128 * k : 128 * k + n] = hot[:, 0:n]

    for move in moves[0:3]:
        move.wait()

    sq_s[...] = jnp.zeros((128, 128), F32)
    sq_s[0:TOK, 0:TOK] = rel[...].astype(F32)
    sq_s[PAD : PAD + TOK, 0:TOK] = rel[...].astype(F32)
    relt = jnp.transpose(sq_s[...])[0:PAD].astype(jnp.int32)
    lane = lax.broadcasted_iota(jnp.int32, (PAD, 128), 1)
    sub = lax.broadcasted_iota(jnp.int32, (PAD, 128), 0)
    live = ((lane & 63) < TOK) & (sub < TOK)
    relt = jnp.where(live, relt, -1)
    safe = jnp.where(live, relt, 0)
    low_i = jnp.where(safe < 128, safe, 0)
    high_i = jnp.where(safe < 128, 0, safe - 128)
    is_low = safe < 128
    first = lane < 64
    for hp in range(HEADS // 2):
        looked = []
        for par in range(2):
            h = 2 * hp + par
            low = jnp.broadcast_to(tab[h : h + 1, 0:128], (8, 128))
            high = jnp.concatenate([tab[h : h + 1, 128:ENT], jnp.zeros((1, 256 - ENT), F32)], axis=1)
            high = jnp.broadcast_to(high, (8, 128))
            rows = []
            for b in range(PAD // 8):
                s = slice(8 * b, 8 * b + 8)
                a0 = jnp.take_along_axis(low, low_i[s], axis=1, mode="promise_in_bounds")
                a1 = jnp.take_along_axis(high, high_i[s], axis=1, mode="promise_in_bounds")
                rows.append(jnp.where(is_low[s], a0, a1))
            looked.append(jnp.concatenate(rows, axis=0))
        both = jnp.where(first, looked[0], looked[1])
        bias_s[hp * PAD : (hp + 1) * PAD] = jnp.where(sub < TOK, both * factor, -1e30)

    sq_s[...] = jnp.zeros((128, 128), F32)
    sq_s[0:WIN, 0:TOK] = reg[...].astype(F32)
    base = sq_s[...]
    cols = jnp.transpose(base)
    for w in range(WIN):
        row = jnp.concatenate([base[w : w + 1, 0:64], base[w : w + 1, 0:64]], axis=1)
        mask_s[w * PAD : (w + 1) * PAD] = jnp.where(cols[0:PAD, w : w + 1] == row, 0.0, -100.0 * factor)

    acc_s[...] = jnp.zeros(acc_s.shape, F32)

    moves[3].wait()
    for b in range(4):
        rows = slice(256 * b, 256 * b + 256)
        tokw[rows] = dot(pick_s[rows], tok[...]).astype(BF16)
    moves[4].wait()
    for n in range(6):
        cols = slice(256 * n, 256 * n + 256)
        qkv_s[:, cols] = dot(tokw[...], wqkv[:, cols]).astype(BF16)
    moves[5].wait()
    for b in range(4):
        rows = slice(256 * b, 256 * b + 256)
        cotw[rows] = dot(pick_s[rows], cot[...]).astype(BF16)
    moves[6].wait()
    for n in range(2):
        cols = slice(256 * n, 256 * n + 256)
        da_s[:, cols] = dot(cotw[...], wproj[cols], NT).astype(BF16)

    chan = lax.broadcasted_iota(jnp.int32, (PAD, 128), 1) // HD
    none = jnp.zeros((PAD, 128), BF16)

    def spread(v):
        return jnp.concatenate([jnp.where(chan == h, v, none) for h in range(4)], axis=0)

    def fold(full):
        total = full[0:PAD]
        for h in range(1, 4):
            total = jnp.where(chan == h, full[h * PAD : (h + 1) * PAD], total)
        return total.astype(BF16)

    def scores(rows, mask, g):
        cq = slice(g * 128, g * 128 + 128)
        k = qkv_s[rows, D + g * 128 : D + g * 128 + 128]
        v = qkv_s[rows, 2 * D + g * 128 : 2 * D + g * 128 + 128]
        qd = spread(qkv_s[rows, cq])
        dd = spread(da_s[rows, cq])
        return dict(rows=rows, mask=mask, g=g, k=k, v=v, qd=qd, dd=dd, s=dot(k, qd, NT), dp=dot(v, dd, NT))

    def softmax(it):
        g, mask = it["g"], it["mask"]
        bias = jnp.concatenate(
            [bias_s[2 * g * PAD : (2 * g + 1) * PAD] + mask, bias_s[(2 * g + 1) * PAD : (2 * g + 2) * PAD] + mask], axis=1
        )
        s = it["s"] * (scale * factor) + bias
        p = jnp.exp2(s - jnp.max(s, axis=0, keepdims=True))
        p = p * (1.0 / jnp.sum(p, axis=0, keepdims=True))
        dp = it["dp"].astype(BF16).astype(F32)
        ds = p * (dp - jnp.sum(dp * p, axis=0, keepdims=True))
        it["pb"] = p.astype(BF16)
        it["dsb"] = (ds * scale).astype(BF16)
        it["pt"] = jnp.transpose(it["pb"])
        it["dst"] = jnp.transpose(it["dsb"])
        return ds

    def results(it):
        rows, g = it["rows"], it["g"]
        cq = slice(g * 128, g * 128 + 128)
        dqkv_s[rows, 2 * D + g * 128 : 2 * D + g * 128 + 128] = dot(it["pb"], it["dd"]).astype(BF16)
        att_s[rows, cq] = fold(dot(it["pt"], it["v"]))
        dqkv_s[rows, D + g * 128 : D + g * 128 + 128] = dot(it["dsb"], it["qd"]).astype(BF16)
        dqkv_s[rows, cq] = fold(dot(it["dst"], it["k"]))

    def windows(step, carry):
        chains = []
        for g in range(4):
            for i in range(UNROLL):
                rows = pl.ds(pl.multiple_of((step * UNROLL + i) * PAD, PAD), PAD)
                chains.append((rows, i, g))
        masks = [mask_s[pl.ds(pl.multiple_of((step * UNROLL + i) * PAD, PAD), PAD), :] for i in range(UNROLL)]
        sums = [None] * 4
        items = []
        for c in range(len(chains) + 1 + AHEAD):
            if c < len(chains):
                rows, i, g = chains[c]
                items.append(scores(rows, masks[i], g))
            if 0 <= c - AHEAD < len(chains):
                it = items[c - AHEAD]
                ds = softmax(it)
                g = it["g"]
                sums[g] = ds if sums[g] is None else sums[g] + ds
                if c - AHEAD == UNROLL * g + UNROLL - 1:
                    acc_s[2 * g * PAD : (2 * g + 1) * PAD] += sums[g][:, 0:128]
                    acc_s[(2 * g + 1) * PAD : (2 * g + 2) * PAD] += sums[g][:, 128:256]
            if c - AHEAD - 1 >= 0:
                results(items[c - AHEAD - 1])
        return carry

    lax.fori_loop(0, WIN // UNROLL, windows, 0)

    ent = lax.broadcasted_iota(jnp.int32, (EPAD, 128), 0)
    sums = jnp.zeros((2 * EPAD, 16), F32)
    for j7 in range(7):
        hots, parts = [], []
        for j in range(7 * j7, 7 * j7 + 7):
            part = acc_s[pl.ds(j, 8, stride=PAD), :]
            top = part.astype(BF16).astype(F32)
            parts.append(jnp.concatenate([top, part - top], axis=0).astype(BF16))
            row = relt[j : j + 1]
            lo = jnp.where(lane[0:1] < 64, row, -1)
            hi = jnp.where(lane[0:1] < 64, -1, row)
            hot = jnp.concatenate([jnp.where(ent == lo, 1.0, 0.0), jnp.where(ent == hi, 1.0, 0.0)], axis=0)
            hots.append(hot.astype(BF16))
        sums = sums + dot(jnp.concatenate(hots, axis=1), jnp.concatenate(parts, axis=1), NT)
    sums = jnp.concatenate([sums, jnp.zeros((2 * EPAD, 112), F32)], axis=1)
    sums = jnp.concatenate([sums, jnp.zeros((384 - 2 * EPAD, 128), F32)], axis=0)
    flat = jnp.concatenate([jnp.transpose(sums[128 * k : 128 * k + 128])[0:16] for k in range(3)], axis=1)
    table = jnp.concatenate([flat[0:8] + flat[8:16], jnp.zeros((8, 128), F32)], axis=1)
    keep[1024:1032] = table
    send[1024:1032] = table

    order = row_order(lax.axis_index("gz") & 1)

    def put(grad, n):
        cols = slice(256 * (n % 2), 256 * (n % 2) + 256)
        for k in range(16):
            rows = slice(64 * k + 16 * (n // 2), 64 * k + 16 * (n // 2) + 16)
            keep[rows, cols] = grad[16 * k : 16 * k + 16]
            send[rows, cols] = grad[256 + 16 * k : 272 + 16 * k]

    t_s[...] = dot(order, tokw[...], NT).astype(BF16)
    for n in range(6):
        put(dot(t_s[...], dqkv_s[:, 256 * n : 256 * n + 256]), n)
    t_s[...] = dot(order, att_s[...], NT).astype(BF16)
    for n in range(2):
        put(dot(t_s[...], cotw[:, 256 * n : 256 * n + 256]), 6 + n)


def sum_core(keep, got, keep_table, got_table, out):
    table = keep_table[...] + got_table[...]
    for k in range(4):
        rows = slice(64 * k, 64 * k + 64)
        out[k, 0:64] = keep[rows] + got[rows]
        out[k, 64:72] = table


def sum_plane(got, out, acc):
    def total(rows):
        part = got[0, rows]
        for k in range(1, 4):
            part = part + got[k, rows]
        return part

    step = pl.program_id(0)

    @pl.when(step == 0)
    def _():
        acc[...] = total(slice(0, 72))

    @pl.when(step > 0)
    def _():
        acc[...] += total(slice(0, 72))

    @pl.when(step == 3)
    def _():
        table = acc[64:72]
        for z in range(8):
            for b in range(4):
                out[z, 2 * b : 2 * b + 2] = acc[16 * b + 2 * z : 16 * b + 2 * z + 2]
            out[z, 8:16] = table


def finish(got, mq, mp, mt, oq, op, ot):
    total = got[0]
    for k in range(1, 8):
        total = total + got[k]
    total = total * (1.0 / 4096)
    for e in range(2):
        for c in range(12):
            row, at = 2 * (c // 4) + e, 128 * (c % 4)
            r = slice(12 * e + c, 12 * e + c + 1)
            oq[r] = 0.9 * mq[r] + total[row : row + 1, at : at + 128]
        for c in range(4):
            r = slice(4 * e + c, 4 * e + c + 1)
            op[r] = 0.9 * mp[r] + total[6 + e : 7 + e, 128 * c : 128 * c + 128]
    for h in range(HEADS):
        at = (h % 2) * EPAD
        ot[h : h + 1] = 0.9 * mt[h : h + 1] + total[8 + h // 2 : 9 + h // 2, at : at + ENT]


def shapes(*dims):
    return tuple(jax.ShapeDtypeStruct(d, F32) for d in dims)


def local_grads(tok, cot, regions, rel_index, w_qkv, w_proj, table, interpret=False):
    return pl.pallas_call(
        local_kernel,
        out_shape=shapes((1032, 512), (1032, 512)),
        in_specs=[pl.BlockSpec(memory_space=pltpu.HBM)] * 7,
        scratch_shapes=[
            pltpu.VMEM((ROWS, D), BF16),
            pltpu.VMEM((ROWS, D), BF16),
            pltpu.VMEM((WIN, TOK), jnp.int32),
            pltpu.VMEM((TOK, TOK), jnp.int32),
            pltpu.VMEM((D, 3 * D), BF16),
            pltpu.VMEM((D, D), BF16),
            pltpu.VMEM((HEADS, ENT), F32),
            pltpu.SemaphoreType.DMA((7,)),
            pltpu.VMEM((PROWS, ROWS), BF16),
            pltpu.VMEM((PROWS, D), BF16),
            pltpu.VMEM((PROWS, D), BF16),
            pltpu.VMEM((PROWS, 3 * D), BF16),
            pltpu.VMEM((PROWS, D), BF16),
            pltpu.VMEM((PROWS, D), BF16),
            pltpu.VMEM((PROWS, 3 * D), BF16),
            pltpu.VMEM((8 * PAD, 128), F32),
            pltpu.VMEM((WIN * PAD, 128), F32),
            pltpu.VMEM((8 * PAD, 128), F32),
            pltpu.VMEM((128, 128), F32),
            pltpu.VMEM((D, PROWS), BF16),
        ],
        name="local_grads",
        compiler_params=pltpu.CompilerParams(vmem_limit_bytes=40 << 20),
        interpret=interpret,
    )(*(pltpu.with_memory_space_constraint(v, pltpu.HBM) for v in (tok, cot, regions, rel_index, w_qkv, w_proj, table)))


def body(
    tokens, cotangent, regions, rel_index, w_qkv, w_proj, bias_table, mom_qkv, mom_proj, mom_table
):
    tok = jnp.transpose(tokens, (1, 0, 2)).reshape(ROWS, D)
    cot = jnp.transpose(cotangent, (1, 0, 2)).reshape(ROWS, D)
    keep, send = local_grads(tok, cot, regions, rel_index, w_qkv, w_proj, bias_table.T)
    got = shift(send, dc=1)
    wide = pl.BlockSpec((256, 512), lambda i: (i, 0))
    last = pl.BlockSpec((8, 512), lambda i: (128, 0))
    part = pl.BlockSpec((4, 72, 512), lambda i: (i, 0, 0))
    plane = pl.pallas_call(
        sum_core,
        grid=(4,),
        in_specs=[wide, wide, last, last],
        out_specs=part,
        out_shape=jax.ShapeDtypeStruct((16, 72, 512), F32),
        name="sum_core",
        compiler_params=pltpu.CompilerParams(vmem_limit_bytes=12 << 20),
    )(keep, got, keep, got)
    plane = lax.all_to_all(plane, AXES, 0, 0, axis_index_groups=planes(), tiled=True)
    line = pl.pallas_call(
        sum_plane,
        grid=(4,),
        in_specs=[part],
        out_specs=pl.BlockSpec((8, 16, 512), lambda i: (0, 0, 0)),
        out_shape=jax.ShapeDtypeStruct((8, 16, 512), F32),
        scratch_shapes=[pltpu.VMEM((72, 512), F32)],
        name="sum_plane",
        compiler_params=pltpu.CompilerParams(vmem_limit_bytes=12 << 20),
    )(plane)
    line = lax.all_to_all(line, "gy", 0, 0, tiled=True)
    new_q, new_p, new_t = pl.pallas_call(
        finish,
        out_shape=shapes((24, 128), (8, 128), (HEADS, ENT)),
        name="finish",
        compiler_params=pltpu.CompilerParams(vmem_limit_bytes=4 << 20),
    )(line, mom_qkv.reshape(24, 128), mom_proj.reshape(8, 128), mom_table.T)
    return new_q.reshape(-1), new_p.reshape(-1), new_t.T


def solution(mesh):
    return jax.shard_map(
        body,
        mesh=mesh,
        in_specs=(
            P(AXES, None, None),
            P(AXES, None, None),
            P(AXES, None),
            P(),
            P(),
            P(),
            P(),
            P(AXES),
            P(AXES),
            P(),
        ),
        out_specs=(P(AXES), P(AXES), P()),
        check_vma=False,
    )
```

```python
import jax
import jax.numpy as jnp
from jax import lax
from jax.experimental import pallas as pl
from jax.experimental.pallas import tpu as pltpu
from jax.sharding import PartitionSpec as P


AXES = ("gx", "gy", "gz")
WIN = 16
TOK = 49
PAD = 64
D = 512
HEADS = 16
HD = 32
ENT = 169
EPAD = 176
UNROLL = 4
AHEAD = 1
LOG2E = 1.4426950408889634
SCALE = HD**-0.5
ROWS = TOK * WIN
PROWS = PAD * WIN
F32 = jnp.float32
BF16 = jnp.bfloat16
NT = (((1,), (1,)), ((), ()))
NN = (((1,), (0,)), ((), ()))


def dot(a, b, dims=NN):
    return lax.dot_general(a, b, dims, preferred_element_type=F32)


def decode(flat):
    gx, gy, gz = flat // 32, (flat // 4) % 8, flat % 4
    return gx % 4, (gx // 4) * 2 + gz // 2, gy, gz % 2


def encode(x, y, z, c):
    x, y, z = x % 4, y % 4, z % 8
    return ((y // 2) * 4 + x) * 32 + z * 4 + (y % 2) * 2 + c


def shift(value, dx=0, dy=0, dz=0, dc=0):
    pairs = []
    for d in range(256):
        x, y, z, c = decode(d)
        pairs.append((d, encode(x + dx, y + dy, z + dz, c ^ dc)))
    return lax.ppermute(value, AXES, pairs)


def planes():
    return [[encode(x, y, z, c) for y in range(4) for x in range(4)] for z in range(8) for c in range(2)]


def row_order(core):
    r = lax.broadcasted_iota(jnp.int32, (D, 128), 0)
    e = r & 1
    z = (r >> 1) & 7
    x = (r >> 4) & 3
    y = (r >> 6) & 3
    c = ((r >> 8) + core) & 1
    orig = ((((y >> 1) * 4 + x) * 32 + z * 4 + (y & 1) * 2 + c) << 1) + e
    col = lax.broadcasted_iota(jnp.int32, (D, 128), 1)
    parts = [jnp.where(orig == col + 128 * k, 1.0, 0.0) for k in range(4)]
    return jnp.concatenate(parts, axis=1).astype(BF16)


def put(grad, block, count, keep, send):
    for half in range(2):
        cols = slice(128 * half, 128 * half + 128)
        for k in range(16):
            at = 16 * count * k + 16 * (block + half)
            keep[at : at + 16] = grad[16 * k : 16 * k + 16, cols]
            send[at : at + 16] = grad[256 + 16 * k : 272 + 16 * k, cols]


def attention(part, qkv_s, da_s, dqkv_s, att_s, bias_s, mask_s, acc_s):
    base = 4 * PAD * part
    into = acc_s.shape[0] - 4 * PAD
    acc_s[into : into + 4 * PAD] = jnp.zeros((4 * PAD, 128), F32)
    chan = lax.broadcasted_iota(jnp.int32, (PAD, 128), 1) // HD
    none = jnp.zeros((PAD, 128), BF16)

    def spread(v):
        return jnp.concatenate([jnp.where(chan == h, v, none) for h in range(4)], axis=0)

    def fold(full):
        total = full[0:PAD]
        for h in range(1, 4):
            total = jnp.where(chan == h, full[h * PAD : (h + 1) * PAD], total)
        return total.astype(BF16)

    def scores(rows, mask, g):
        cq = slice(g * 128, g * 128 + 128)
        k = qkv_s[rows, 256 + g * 128 : 384 + g * 128]
        v = qkv_s[rows, 512 + g * 128 : 640 + g * 128]
        qd = spread(qkv_s[rows, cq])
        dd = spread(da_s[rows, cq])
        return dict(rows=rows, mask=mask, g=g, k=k, v=v, qd=qd, dd=dd, s=dot(k, qd, NT), dp=dot(v, dd, NT))

    def softmax(it):
        g, mask = it["g"], it["mask"]
        bias = jnp.concatenate(
            [bias_s[base + 2 * g * PAD : base + (2 * g + 1) * PAD] + mask,
             bias_s[base + (2 * g + 1) * PAD : base + (2 * g + 2) * PAD] + mask], axis=1,
        )
        s = it["s"] * (SCALE * LOG2E) + bias
        p = jnp.exp2(s - jnp.max(s, axis=0, keepdims=True))
        p = p * (1.0 / jnp.sum(p, axis=0, keepdims=True))
        dp = it["dp"].astype(BF16).astype(F32)
        ds = p * (dp - jnp.sum(dp * p, axis=0, keepdims=True))
        it["pb"] = p.astype(BF16)
        it["dsb"] = (ds * SCALE).astype(BF16)
        it["pt"] = jnp.transpose(it["pb"])
        it["dst"] = jnp.transpose(it["dsb"])
        return ds

    def results(it):
        rows, g = it["rows"], it["g"]
        cq = slice(g * 128, g * 128 + 128)
        dqkv_s[rows, 512 + g * 128 : 640 + g * 128] = dot(it["pb"], it["dd"]).astype(BF16)
        att_s[rows, cq] = fold(dot(it["pt"], it["v"]))
        dqkv_s[rows, 256 + g * 128 : 384 + g * 128] = dot(it["dsb"], it["qd"]).astype(BF16)
        dqkv_s[rows, cq] = fold(dot(it["dst"], it["k"]))

    def windows(step, carry):
        chains = []
        for g in range(2):
            for i in range(UNROLL):
                rows = pl.ds(pl.multiple_of((step * UNROLL + i) * PAD, PAD), PAD)
                chains.append((rows, i, g))
        masks = [mask_s[pl.ds(pl.multiple_of((step * UNROLL + i) * PAD, PAD), PAD), :] for i in range(UNROLL)]
        sums = [None] * 2
        items = []
        for c in range(len(chains) + 1 + AHEAD):
            if c < len(chains):
                rows, i, g = chains[c]
                items.append(scores(rows, masks[i], g))
            if 0 <= c - AHEAD < len(chains):
                it = items[c - AHEAD]
                ds = softmax(it)
                g = it["g"]
                sums[g] = ds if sums[g] is None else sums[g] + ds
                if c - AHEAD == UNROLL * g + UNROLL - 1:
                    acc_s[into + 2 * g * PAD : into + (2 * g + 1) * PAD] += sums[g][:, 0:128]
                    acc_s[into + (2 * g + 1) * PAD : into + (2 * g + 2) * PAD] += sums[g][:, 128:256]
            if c - AHEAD - 1 >= 0:
                results(items[c - AHEAD - 1])
        return carry

    lax.fori_loop(0, WIN // UNROLL, windows, 0)


def first_kernel(
    tok_h, cot_h, reg_h, rel_h, wqkv_h, wproj_h, tab_h,
    keep, send, *rest,
):
    outs, (tok, cot, reg, rel, wqkv, wproj, tab, sems, pick_s, qkv_s, da_s, dqkv_s, sq_s), kept, out_sems = (
        rest[0:8], rest[8:21], rest[21:29], rest[29]
    )
    tokw, cotw, t_s, att_s, bias_s, mask_s, acc_s, relt_s = kept
    puts = [pltpu.make_async_copy(src, dst, out_sems.at[n]) for n, (src, dst) in enumerate(zip(kept, outs))]
    moves = [
        pltpu.make_async_copy(src, dst, sems.at[n])
        for n, (src, dst) in enumerate(
            zip((rel_h, reg_h, tab_h, tok_h, wqkv_h, cot_h, wproj_h), (rel, reg, tab, tok, wqkv, cot, wproj))
        )
    ]
    for move in moves:
        move.start()

    line = lax.broadcasted_iota(jnp.int32, (256, 128), 0)
    lanes = lax.broadcasted_iota(jnp.int32, (256, 128), 1)
    for b in range(4):
        t = line & 63
        source = jnp.where(t < TOK, t * WIN + (line >> 6) + 4 * b, -1)
        for k in range(7):
            n = min(128, ROWS - 128 * k)
            hot = jnp.where(source == lanes + 128 * k, 1.0, 0.0).astype(BF16)
            pick_s[256 * b : 256 * b + 256, 128 * k : 128 * k + n] = hot[:, 0:n]

    for move in moves[0:3]:
        move.wait()

    sq_s[...] = jnp.zeros((128, 128), F32)
    sq_s[0:TOK, 0:TOK] = rel[...].astype(F32)
    sq_s[PAD : PAD + TOK, 0:TOK] = rel[...].astype(F32)
    relt = jnp.transpose(sq_s[...])[0:PAD].astype(jnp.int32)
    lane = lax.broadcasted_iota(jnp.int32, (PAD, 128), 1)
    sub = lax.broadcasted_iota(jnp.int32, (PAD, 128), 0)
    live = ((lane & 63) < TOK) & (sub < TOK)
    relt_s[...] = jnp.where(live, relt, -1)
    safe = jnp.where(live, relt, 0)
    low_i = jnp.where(safe < 128, safe, 0)
    high_i = jnp.where(safe < 128, 0, safe - 128)
    is_low = safe < 128
    first = lane < 64
    for hp in range(HEADS // 2):
        looked = []
        for par in range(2):
            h = 2 * hp + par
            low = jnp.broadcast_to(tab[h : h + 1, 0:128], (8, 128))
            high = jnp.concatenate([tab[h : h + 1, 128:ENT], jnp.zeros((1, 256 - ENT), F32)], axis=1)
            high = jnp.broadcast_to(high, (8, 128))
            rows = []
            for b in range(PAD // 8):
                s = slice(8 * b, 8 * b + 8)
                a0 = jnp.take_along_axis(low, low_i[s], axis=1, mode="promise_in_bounds")
                a1 = jnp.take_along_axis(high, high_i[s], axis=1, mode="promise_in_bounds")
                rows.append(jnp.where(is_low[s], a0, a1))
            looked.append(jnp.concatenate(rows, axis=0))
        both = jnp.where(first, looked[0], looked[1])
        bias_s[hp * PAD : (hp + 1) * PAD] = jnp.where(sub < TOK, both * LOG2E, -1e30)

    sq_s[...] = jnp.zeros((128, 128), F32)
    sq_s[0:WIN, 0:TOK] = reg[...].astype(F32)
    base = sq_s[...]
    cols = jnp.transpose(base)
    for w in range(WIN):
        row = jnp.concatenate([base[w : w + 1, 0:64], base[w : w + 1, 0:64]], axis=1)
        mask_s[w * PAD : (w + 1) * PAD] = jnp.where(cols[0:PAD, w : w + 1] == row, 0.0, -100.0 * LOG2E)
    for n in (4, 5, 7):
        puts[n].start()

    moves[3].wait()
    for b in range(4):
        rows = slice(256 * b, 256 * b + 256)
        tokw[rows] = dot(pick_s[rows], tok[...]).astype(BF16)
    puts[0].start()
    moves[5].wait()
    for b in range(4):
        rows = slice(256 * b, 256 * b + 256)
        cotw[rows] = dot(pick_s[rows], cot[...]).astype(BF16)
    puts[1].start()
    moves[4].wait()
    moves[6].wait()
    for n in range(3):
        at = D * n
        qkv_s[:, 256 * n : 256 * n + 256] = dot(tokw[...], wqkv[:, at : at + 256]).astype(BF16)
    da_s[...] = dot(cotw[...], wproj[0:256], NT).astype(BF16)
    order = row_order(lax.axis_index("gz") & 1)
    t_s[...] = dot(order, tokw[...], NT).astype(BF16)
    puts[2].start()
    attention(0, qkv_s, da_s, dqkv_s, att_s, bias_s, mask_s, acc_s)
    puts[3].start()
    puts[6].start()
    for n in range(3):
        put(dot(t_s[...], dqkv_s[:, 256 * n : 256 * n + 256]), 2 * n, 6, keep, send)
    for move in puts:
        move.wait()


def second_kernel(*refs):
    given, (keep, send, qkv_s, da_s, att_s, dqkv_s, acc_s, u_s), (sems, *held) = refs[0:10], refs[10:18], refs[18:]
    tokw, cotw, t_s, att_first, bias_s, mask_s, acc_first, relt_s, wqkv, wproj = held
    moves = []
    for n, (src, dst) in enumerate(zip(given[0:8], held)):
        moves.append(pltpu.make_async_copy(src, dst, sems.at[n]))
    for n in range(3):
        src = given[8].at[:, D * n + 256 : D * n + 512]
        moves.append(pltpu.make_async_copy(src, wqkv.at[n], sems.at[8 + n]))
    moves.append(pltpu.make_async_copy(given[9].at[256:512], wproj, sems.at[11]))
    for n in (0, 8, 9, 10, 1, 11, 4, 5, 2, 3, 6, 7):
        moves[n].start()
    moves[0].wait()
    for n in range(3):
        moves[8 + n].wait()
        qkv_s[:, 256 * n : 256 * n + 256] = dot(tokw[...], wqkv[n]).astype(BF16)
    moves[1].wait()
    moves[11].wait()
    da_s[...] = dot(cotw[...], wproj[...], NT).astype(BF16)
    for n in range(2, 8):
        moves[n].wait()
    attention(1, qkv_s, da_s, dqkv_s, att_s, bias_s, mask_s, acc_s)
    acc_s[0 : 4 * PAD] = acc_first[...]
    lane = lax.broadcasted_iota(jnp.int32, (1, 128), 1)

    ent = lax.broadcasted_iota(jnp.int32, (EPAD, 128), 0)
    sums = jnp.zeros((2 * EPAD, 16), F32)
    for j7 in range(7):
        hots, parts = [], []
        for j in range(7 * j7, 7 * j7 + 7):
            part = acc_s[pl.ds(j, 8, stride=PAD), :]
            top = part.astype(BF16).astype(F32)
            parts.append(jnp.concatenate([top, part - top], axis=0).astype(BF16))
            row = relt_s[j : j + 1]
            lo = jnp.where(lane < 64, row, -1)
            hi = jnp.where(lane < 64, -1, row)
            hot = jnp.concatenate([jnp.where(ent == lo, 1.0, 0.0), jnp.where(ent == hi, 1.0, 0.0)], axis=0)
            hots.append(hot.astype(BF16))
        sums = sums + dot(jnp.concatenate(hots, axis=1), jnp.concatenate(parts, axis=1), NT)
    sums = jnp.concatenate([sums, jnp.zeros((2 * EPAD, 112), F32)], axis=1)
    sums = jnp.concatenate([sums, jnp.zeros((384 - 2 * EPAD, 128), F32)], axis=0)
    flat = jnp.concatenate([jnp.transpose(sums[128 * k : 128 * k + 128])[0:16] for k in range(3)], axis=1)
    table = flat[0:8] + flat[8:16]
    for k in range(3):
        keep[2560 + 8 * k : 2568 + 8 * k] = table[:, 128 * k : 128 * k + 128]
        send[2560 + 8 * k : 2568 + 8 * k] = table[:, 128 * k : 128 * k + 128]

    for n in range(3):
        put(dot(t_s[...], dqkv_s[:, 256 * n : 256 * n + 256]), 2 * n, 10, keep, send)
    order = row_order(lax.axis_index("gz") & 1)
    u_s[...] = dot(order, jnp.concatenate([att_first[...], att_s[...]], axis=1), NT).astype(BF16)
    for n in range(2):
        put(dot(u_s[...], cotw[:, 256 * n : 256 * n + 256]), 6 + 2 * n, 10, keep, send)


def sum_first(keep, got, out):
    for k in range(16):
        rows = slice(96 * k, 96 * k + 96)
        out[k] = keep[rows] + got[rows]


def sum_second(keep, got, out):
    table = keep[2560:2584] + got[2560:2584]
    for k in range(16):
        rows = slice(160 * k, 160 * k + 160)
        out[k, 0:160] = keep[rows] + got[rows]
        out[k, 160:184] = table


def sum_plane(one, two, out):
    def total(ref, rows):
        part = ref[0, rows]
        for k in range(1, 16):
            part = part + ref[k, rows]
        return part

    for b in range(16):
        ref, at = (one, 16 * b) if b < 6 else (two, 16 * b - 96)
        part = total(ref, slice(at, at + 16))
        for z in range(8):
            out[z, 2 * b : 2 * b + 2] = part[2 * z : 2 * z + 2]
    table = total(two, slice(160, 184))
    for z in range(8):
        out[z, 32:56] = table


def finish(got, mq, mp, mt, oq, op, ot):
    total = got[0]
    for k in range(1, 8):
        total = total + got[k]
    total = total * (1.0 / 4096)
    for e in range(2):
        for c in range(12):
            kind, g = c // 4, c % 4
            row = 2 * (2 * kind + g % 2 + 6 * (g // 2)) + e
            r = slice(12 * e + c, 12 * e + c + 1)
            oq[r] = 0.9 * mq[r] + total[row : row + 1]
        for c in range(4):
            row = 2 * (12 + c) + e
            r = slice(4 * e + c, 4 * e + c + 1)
            op[r] = 0.9 * mp[r] + total[row : row + 1]
    table = jnp.concatenate([total[32:40], total[40:48], total[48:56]], axis=1)
    for h in range(HEADS):
        at = (h % 2) * EPAD
        ot[h : h + 1] = 0.9 * mt[h : h + 1] + table[h // 2 : h // 2 + 1, at : at + ENT]


def shapes(*dims):
    return tuple(jax.ShapeDtypeStruct(d, F32) for d in dims)


HANDED = (
    ((PROWS, D), BF16),
    ((PROWS, D), BF16),
    ((D, PROWS), BF16),
    ((PROWS, 256), BF16),
    ((8 * PAD, 128), F32),
    ((WIN * PAD, 128), F32),
    ((4 * PAD, 128), F32),
    ((PAD, 128), jnp.int32),
)


def local_grads(tok, cot, regions, rel_index, w_qkv, w_proj, table, interpret=False):
    args = (tok, cot, regions, rel_index, w_qkv, w_proj, table)
    if not interpret:
        args = tuple(pltpu.with_memory_space_constraint(v, pltpu.HBM) for v in args)
    space = jax.ShapeDtypeStruct if interpret else pltpu.HBM
    keep, send, *rest = pl.pallas_call(
        first_kernel,
        out_shape=shapes((1536, 128), (1536, 128)) + tuple(space(*v) for v in HANDED),
        in_specs=[pl.BlockSpec(memory_space=pltpu.HBM)] * 7,
        out_specs=[pl.BlockSpec(memory_space=pltpu.VMEM)] * 2 + [pl.BlockSpec(memory_space=pltpu.HBM)] * 8,
        scratch_shapes=[
            pltpu.VMEM((ROWS, D), BF16),
            pltpu.VMEM((ROWS, D), BF16),
            pltpu.VMEM((WIN, TOK), jnp.int32),
            pltpu.VMEM((TOK, TOK), jnp.int32),
            pltpu.VMEM((D, 3 * D), BF16),
            pltpu.VMEM((D, D), BF16),
            pltpu.VMEM((HEADS, ENT), F32),
            pltpu.SemaphoreType.DMA((7,)),
            pltpu.VMEM((PROWS, ROWS), BF16),
            pltpu.VMEM((PROWS, 768), BF16),
            pltpu.VMEM((PROWS, 256), BF16),
            pltpu.VMEM((PROWS, 768), BF16),
            pltpu.VMEM((128, 128), F32),
            *(pltpu.VMEM(*v) for v in HANDED),
            pltpu.SemaphoreType.DMA((8,)),
        ],
        name="first_grads",
        compiler_params=pltpu.CompilerParams(vmem_limit_bytes=32 << 20),
        cost_estimate=pl.CostEstimate(flops=10 * 10**9, bytes_accessed=4 << 20, transcendentals=0),
        interpret=interpret,
    )(*args)
    return keep, send, rest


def more_grads(rest, w_qkv, w_proj, interpret=False):
    args = (*rest, w_qkv, w_proj)
    if not interpret:
        args = tuple(pltpu.with_memory_space_constraint(v, pltpu.HBM) for v in args)
    return pl.pallas_call(
        second_kernel,
        out_shape=shapes((2584, 128), (2584, 128)),
        in_specs=[pl.BlockSpec(memory_space=pltpu.HBM)] * 10,
        scratch_shapes=[
            pltpu.VMEM((PROWS, 768), BF16),
            pltpu.VMEM((PROWS, 256), BF16),
            pltpu.VMEM((PROWS, 256), BF16),
            pltpu.VMEM((PROWS, 768), BF16),
            pltpu.VMEM((8 * PAD, 128), F32),
            pltpu.VMEM((D, PROWS), BF16),
            pltpu.SemaphoreType.DMA((12,)),
            *(pltpu.VMEM(*v) for v in HANDED),
            pltpu.VMEM((3, D, 256), BF16),
            pltpu.VMEM((256, D), BF16),
        ],
        name="second_grads",
        compiler_params=pltpu.CompilerParams(vmem_limit_bytes=32 << 20),
        cost_estimate=pl.CostEstimate(flops=10 * 10**9, bytes_accessed=4 << 20, transcendentals=0),
        interpret=interpret,
    )(*args)


def small(kernel, out_shape, *args):
    return pl.pallas_call(
        kernel, out_shape=out_shape, compiler_params=pltpu.CompilerParams(vmem_limit_bytes=3 << 20)
    )(*args)


def exchange(part):
    return lax.all_to_all(part, AXES, 0, 0, axis_index_groups=planes(), tiled=True)


def body(
    tokens, cotangent, regions, rel_index, w_qkv, w_proj, bias_table, mom_qkv, mom_proj, mom_table
):
    tok = jnp.transpose(tokens, (1, 0, 2)).reshape(ROWS, D)
    cot = jnp.transpose(cotangent, (1, 0, 2)).reshape(ROWS, D)
    keep, send, rest = local_grads(tok, cot, regions, rel_index, w_qkv, w_proj, bias_table.T)
    one = small(sum_first, jax.ShapeDtypeStruct((16, 96, 128), F32), keep, shift(send, dc=1))
    one, rest = lax.optimization_barrier((one, tuple(rest)))
    one = exchange(one)
    keep, send = more_grads(rest, w_qkv, w_proj)
    two = small(sum_second, jax.ShapeDtypeStruct((16, 184, 128), F32), keep, shift(send, dc=1))
    two = exchange(two)
    line = small(sum_plane, jax.ShapeDtypeStruct((8, 56, 128), F32), one, two)
    line = lax.all_to_all(line, "gy", 0, 0, tiled=True)
    new_q, new_p, new_t = small(
        finish,
        shapes((24, 128), (8, 128), (HEADS, ENT)),
        line,
        mom_qkv.reshape(24, 128),
        mom_proj.reshape(8, 128),
        mom_table.T,
    )
    return new_q.reshape(-1), new_p.reshape(-1), new_t.T


def solution(mesh):
    return jax.shard_map(
        body,
        mesh=mesh,
        in_specs=(
            P(AXES, None, None),
            P(AXES, None, None),
            P(AXES, None),
            P(),
            P(),
            P(),
            P(),
            P(AXES),
            P(AXES),
            P(),
        ),
        out_specs=(P(AXES), P(AXES), P()),
        check_vma=False,
    )
```

```python
import jax
import jax.numpy as jnp
from jax import lax
from jax.experimental import pallas as pl
from jax.experimental.pallas import tpu as pltpu
from jax.sharding import PartitionSpec as P

AXES = ("gx", "gy", "gz")
WIN = 16
TOK = 49
PAD = 64
D = 512
HEADS = 16
HD = 32
ENT = 169
EPAD = 176
UNROLL = 4
AHEAD = 2
ROWS = TOK * WIN
PROWS = PAD * WIN
F32 = jnp.float32
BF16 = jnp.bfloat16
NT = (((1,), (1,)), ((), ()))
NN = (((1,), (0,)), ((), ()))


def dot(a, b, dims=NN):
    return lax.dot_general(a, b, dims, preferred_element_type=F32)


def decode(flat):
    gx, gy, gz = flat // 32, (flat // 4) % 8, flat % 4
    return gx % 4, (gx // 4) * 2 + gz // 2, gy, gz % 2


def encode(x, y, z, c):
    x, y, z = x % 4, y % 4, z % 8
    return ((y // 2) * 4 + x) * 32 + z * 4 + (y % 2) * 2 + c


def shift(value, dx=0, dy=0, dz=0, dc=0):
    pairs = []
    for d in range(256):
        x, y, z, c = decode(d)
        pairs.append((d, encode(x + dx, y + dy, z + dz, c ^ dc)))
    return lax.ppermute(value, AXES, pairs)


def planes():
    return [[encode(x, y, z, c) for y in range(4) for x in range(4)] for z in range(8) for c in range(2)]


def reorder(core, src, dst):
    r = lax.broadcasted_iota(jnp.int32, (128, 128), 0)
    col = lax.broadcasted_iota(jnp.int32, (128, 128), 1)
    e = r & 1
    z = (r >> 1) & 7
    x = (r >> 4) & 3
    y0 = (r >> 6) & 1
    for rc in range(2):
        c = (rc + core) & 1
        orig = ((x * 32 + z * 4 + y0 * 2 + c) << 1) + e
        hot = jnp.concatenate([jnp.where(orig == col + 128 * k, 1.0, 0.0) for k in range(2)], axis=1).astype(BF16)
        for y1 in range(2):
            at = 256 * rc + 128 * y1
            dst[at : at + 128] = dot(hot, src[:, 256 * y1 : 256 * y1 + 256], NT).astype(BF16)


def local_kernel(
    tok_h, cot_h, reg_h, rel_h, wqkv_h, wproj_h, tab_h, keep, send,
    tok, cot, reg, rel, wqkv, wproj, tab, sems, tokw, cotw, qkv_s, da_s, att_s, dqkv_s, bias_s, mask_s, acc_s, sq_s, t_s,
):
    moves = [
        pltpu.make_async_copy(src, dst, sems.at[n])
        for n, (src, dst) in enumerate(
            zip((tok_h, rel_h, reg_h, tab_h, wqkv_h, cot_h, wproj_h), (tok, rel, reg, tab, wqkv, cot, wproj))
        )
    ]
    for move in moves:
        move.start()
    factor = 1.4426950408889634
    scale = HD**-0.5

    line = lax.broadcasted_iota(jnp.int32, (256, 128), 0)
    lanes = lax.broadcasted_iota(jnp.int32, (256, 128), 1)
    source = (line & 15) * WIN + (line >> 4)
    pick = jnp.concatenate([jnp.where(source == lanes + 128 * k, 1.0, 0.0) for k in range(2)], axis=1).astype(BF16)
    alone = jnp.where(((line & 15) == 0) & ((line >> 4) == lanes), 1.0, 0.0).astype(BF16)[:, 0:WIN]

    def regroup(src, dst):
        for b in range(4):
            if b < 3:
                moved = dot(pick, src[256 * b : 256 * b + 256]).astype(BF16)
            else:
                moved = dot(alone, src[768:784]).astype(BF16)
            for w in range(WIN):
                dst[w * PAD + 16 * b : w * PAD + 16 * b + 16] = moved[16 * w : 16 * w + 16]

    for move in moves[0:4]:
        move.wait()
    regroup(tok, tokw)

    sq_s[...] = jnp.zeros((128, 128), F32)
    sq_s[0:TOK, 0:TOK] = rel[...].astype(F32)
    sq_s[PAD : PAD + TOK, 0:TOK] = rel[...].astype(F32)
    relt = jnp.transpose(sq_s[...])[0:PAD].astype(jnp.int32)
    lane = lax.broadcasted_iota(jnp.int32, (PAD, 128), 1)
    sub = lax.broadcasted_iota(jnp.int32, (PAD, 128), 0)
    live = ((lane & 63) < TOK) & (sub < TOK)
    relt = jnp.where(live, relt, -1)
    safe = jnp.where(live, relt, 0)
    low_i = jnp.where(safe < 128, safe, 0)
    high_i = jnp.where(safe < 128, 0, safe - 128)
    is_low = safe < 128
    first = lane < 64
    for hp in range(HEADS // 2):
        looked = []
        for par in range(2):
            h = 2 * hp + par
            low = jnp.broadcast_to(tab[h : h + 1, 0:128], (8, 128))
            high = jnp.concatenate([tab[h : h + 1, 128:ENT], jnp.zeros((1, 256 - ENT), F32)], axis=1)
            high = jnp.broadcast_to(high, (8, 128))
            rows = []
            for b in range(PAD // 8):
                s = slice(8 * b, 8 * b + 8)
                a0 = jnp.take_along_axis(low, low_i[s], axis=1, mode="promise_in_bounds")
                a1 = jnp.take_along_axis(high, high_i[s], axis=1, mode="promise_in_bounds")
                rows.append(jnp.where(is_low[s], a0, a1))
            looked.append(jnp.concatenate(rows, axis=0))
        both = jnp.where(first, looked[0], looked[1])
        bias_s[hp * PAD : (hp + 1) * PAD] = jnp.where(sub < TOK, both * factor, -1e30)

    sq_s[...] = jnp.zeros((128, 128), F32)
    sq_s[0:WIN, 0:TOK] = reg[...].astype(F32)
    base = sq_s[...]
    cols = jnp.transpose(base)
    for w in range(WIN):
        row = jnp.concatenate([base[w : w + 1, 0:64], base[w : w + 1, 0:64]], axis=1)
        mask_s[w * PAD : (w + 1) * PAD] = jnp.where(cols[0:PAD, w : w + 1] == row, 0.0, -100.0 * factor)

    acc_s[...] = jnp.zeros(acc_s.shape, F32)

    for move in moves[4:7]:
        move.wait()
    regroup(cot, cotw)
    for n in range(6):
        cols = slice(256 * n, 256 * n + 256)
        qkv_s[:, cols] = dot(tokw[...], wqkv[:, cols]).astype(BF16)
    for n in range(2):
        cols = slice(256 * n, 256 * n + 256)
        da_s[:, cols] = dot(cotw[...], wproj[cols], NT).astype(BF16)

    chan = lax.broadcasted_iota(jnp.int32, (PAD, 128), 1) // HD
    none = jnp.zeros((PAD, 128), BF16)

    def spread(v):
        return jnp.concatenate([jnp.where(chan == h, v, none) for h in range(4)], axis=0)

    def fold(full):
        total = full[0:PAD]
        for h in range(1, 4):
            total = jnp.where(chan == h, full[h * PAD : (h + 1) * PAD], total)
        return total.astype(BF16)

    def scores(rows, mask, g):
        cq = slice(g * 128, g * 128 + 128)
        k = qkv_s[rows, D + g * 128 : D + g * 128 + 128]
        v = qkv_s[rows, 2 * D + g * 128 : 2 * D + g * 128 + 128]
        qd = spread(qkv_s[rows, cq])
        dd = spread(da_s[rows, cq])
        return dict(rows=rows, mask=mask, g=g, k=k, v=v, qd=qd, dd=dd, s=dot(k, qd, NT), dp=dot(v, dd, NT))

    def softmax(it):
        g, mask = it["g"], it["mask"]
        bias = jnp.concatenate(
            [bias_s[2 * g * PAD : (2 * g + 1) * PAD] + mask, bias_s[(2 * g + 1) * PAD : (2 * g + 2) * PAD] + mask], axis=1
        )
        s = it["s"] * (scale * factor) + bias
        p = jnp.exp2(s - jnp.max(s, axis=0, keepdims=True))
        p = p * (1.0 / jnp.sum(p, axis=0, keepdims=True))
        dp = it["dp"].astype(BF16).astype(F32)
        ds = p * (dp - jnp.sum(dp * p, axis=0, keepdims=True))
        it["pb"] = p.astype(BF16)
        it["dsb"] = (ds * scale).astype(BF16)
        it["pt"] = jnp.transpose(it["pb"])
        it["dst"] = jnp.transpose(it["dsb"])
        return ds

    def results(it):
        rows, g = it["rows"], it["g"]
        cq = slice(g * 128, g * 128 + 128)
        dqkv_s[rows, 2 * D + g * 128 : 2 * D + g * 128 + 128] = dot(it["pb"], it["dd"]).astype(BF16)
        att_s[rows, cq] = fold(dot(it["pt"], it["v"]))
        dqkv_s[rows, D + g * 128 : D + g * 128 + 128] = dot(it["dsb"], it["qd"]).astype(BF16)
        dqkv_s[rows, cq] = fold(dot(it["dst"], it["k"]))

    def windows(step, carry):
        chains = []
        for g in range(4):
            for i in range(UNROLL):
                rows = pl.ds(pl.multiple_of((step * UNROLL + i) * PAD, PAD), PAD)
                chains.append((rows, i, g))
        masks = [mask_s[pl.ds(pl.multiple_of((step * UNROLL + i) * PAD, PAD), PAD), :] for i in range(UNROLL)]
        sums = [None] * 4
        items = []
        for c in range(len(chains) + 1 + AHEAD):
            if c < len(chains):
                rows, i, g = chains[c]
                items.append(scores(rows, masks[i], g))
            if 0 <= c - AHEAD < len(chains):
                it = items[c - AHEAD]
                ds = softmax(it)
                g = it["g"]
                sums[g] = ds if sums[g] is None else sums[g] + ds
                if c - AHEAD == UNROLL * g + UNROLL - 1:
                    acc_s[2 * g * PAD : (2 * g + 1) * PAD] += sums[g][:, 0:128]
                    acc_s[(2 * g + 1) * PAD : (2 * g + 2) * PAD] += sums[g][:, 128:256]
            if c - AHEAD - 1 >= 0:
                results(items[c - AHEAD - 1])
        return carry

    lax.fori_loop(0, WIN // UNROLL, windows, 0)

    ent = lax.broadcasted_iota(jnp.int32, (EPAD, 128), 0)
    sums = jnp.zeros((EPAD, 32), F32)
    left = lax.broadcasted_iota(jnp.int32, (8, 128), 1) < 64
    for j7 in range(7):
        hots, parts = [], []
        for j in range(7 * j7, 7 * j7 + 7):
            part = acc_s[pl.ds(j, 8, stride=PAD), :]
            top = part.astype(BF16).astype(F32)
            rest = part - top
            split = [jnp.where(left, top, 0.0), jnp.where(left, rest, 0.0), jnp.where(left, 0.0, top), jnp.where(left, 0.0, rest)]
            parts.append(jnp.concatenate(split, axis=0).astype(BF16))
            hots.append(jnp.where(ent == relt[j : j + 1], 1.0, 0.0).astype(BF16))
        sums = sums + dot(jnp.concatenate(hots, axis=1), jnp.concatenate(parts, axis=1), NT)
    sums = jnp.concatenate([sums, jnp.zeros((EPAD, 96), F32)], axis=1)
    sums = jnp.concatenate([sums, pltpu.roll(sums, 112, 1), jnp.zeros((384 - 2 * EPAD, 128), F32)], axis=0)
    flat = jnp.concatenate([jnp.transpose(sums[128 * k : 128 * k + 128])[0:16] for k in range(3)], axis=1)
    table = flat[0:8] + flat[8:16]
    for k in range(3):
        keep[4096 + 8 * k : 4104 + 8 * k] = table[:, 128 * k : 128 * k + 128]
        send[4096 + 8 * k : 4104 + 8 * k] = table[:, 128 * k : 128 * k + 128]

    core = lax.axis_index("gz") & 1

    def put(grad, block):
        for half in range(2):
            cols = slice(128 * half, 128 * half + 128)
            for k in range(16):
                at = 256 * k + 16 * (block + half)
                keep[at : at + 16] = grad[16 * k : 16 * k + 16, cols]
                send[at : at + 16] = grad[256 + 16 * k : 272 + 16 * k, cols]

    reorder(core, tokw, t_s)
    for n in range(6):
        put(dot(t_s[...], dqkv_s[:, 256 * n : 256 * n + 256]), 2 * n)
    reorder(core, att_s, t_s)
    for n in range(2):
        put(dot(t_s[...], cotw[:, 256 * n : 256 * n + 256]), 12 + 2 * n)


def sum_core(keep, got, out):
    table = keep[4096:4120] + got[4096:4120]
    for k in range(16):
        rows = slice(256 * k, 256 * k + 256)
        out[k, 0:256] = keep[rows] + got[rows]
        out[k, 256:280] = table


def sum_plane(got, out):
    def total(rows):
        part = got[0, rows]
        for k in range(1, 16):
            part = part + got[k, rows]
        return part

    for b in range(16):
        part = total(slice(16 * b, 16 * b + 16))
        for z in range(8):
            out[z, 2 * b : 2 * b + 2] = part[2 * z : 2 * z + 2]
    table = total(slice(256, 280))
    for z in range(8):
        out[z, 32:56] = table


def finish(got, mq, mp, mt, oq, op, ot):
    total = got[0]
    for k in range(1, 8):
        total = total + got[k]
    total = total * (1.0 / 4096)
    for e in range(2):
        for c in range(12):
            row = 2 * c + e
            r = slice(12 * e + c, 12 * e + c + 1)
            oq[r] = 0.9 * mq[r] + total[row : row + 1]
        for c in range(4):
            row = 2 * (12 + c) + e
            r = slice(4 * e + c, 4 * e + c + 1)
            op[r] = 0.9 * mp[r] + total[row : row + 1]
    table = jnp.concatenate([total[32:40], total[40:48], total[48:56]], axis=1)
    for h in range(HEADS):
        at = (h % 2) * EPAD
        ot[h : h + 1] = 0.9 * mt[h : h + 1] + table[h // 2 : h // 2 + 1, at : at + ENT]


def shapes(*dims):
    return tuple(jax.ShapeDtypeStruct(d, F32) for d in dims)


def local_grads(tok, cot, regions, rel_index, w_qkv, w_proj, table, interpret=False):
    return pl.pallas_call(
        local_kernel,
        out_shape=shapes((4120, 128), (4120, 128)),
        in_specs=[pl.BlockSpec(memory_space=pltpu.HBM)] * 7,
        scratch_shapes=[
            pltpu.VMEM((ROWS, D), BF16),
            pltpu.VMEM((ROWS, D), BF16),
            pltpu.VMEM((WIN, TOK), jnp.int32),
            pltpu.VMEM((TOK, TOK), jnp.int32),
            pltpu.VMEM((D, 3 * D), BF16),
            pltpu.VMEM((D, D), BF16),
            pltpu.VMEM((HEADS, ENT), F32),
            pltpu.SemaphoreType.DMA((7,)),
            pltpu.VMEM((PROWS, D), BF16),
            pltpu.VMEM((PROWS, D), BF16),
            pltpu.VMEM((PROWS, 3 * D), BF16),
            pltpu.VMEM((PROWS, D), BF16),
            pltpu.VMEM((PROWS, D), BF16),
            pltpu.VMEM((PROWS, 3 * D), BF16),
            pltpu.VMEM((8 * PAD, 128), F32),
            pltpu.VMEM((WIN * PAD, 128), F32),
            pltpu.VMEM((8 * PAD, 128), F32),
            pltpu.VMEM((128, 128), F32),
            pltpu.VMEM((D, PROWS), BF16),
        ],
        name="local_grads",
        compiler_params=pltpu.CompilerParams(vmem_limit_bytes=40 << 20),
        interpret=interpret,
    )(*(pltpu.with_memory_space_constraint(v, pltpu.HBM) for v in (tok, cot, regions, rel_index, w_qkv, w_proj, table)))


def small(kernel, out_shape, *args):
    return pl.pallas_call(
        kernel, out_shape=out_shape, name=kernel.__name__, compiler_params=pltpu.CompilerParams(vmem_limit_bytes=3 << 20)
    )(*args)


def body(
    tokens, cotangent, regions, rel_index, w_qkv, w_proj, bias_table, mom_qkv, mom_proj, mom_table
):
    tok = jnp.transpose(tokens, (1, 0, 2)).reshape(ROWS, D)
    cot = jnp.transpose(cotangent, (1, 0, 2)).reshape(ROWS, D)
    keep, send = local_grads(tok, cot, regions, rel_index, w_qkv, w_proj, bias_table.T)
    got = shift(send, dc=1)
    plane = small(sum_core, jax.ShapeDtypeStruct((16, 280, 128), F32), keep, got)
    plane = lax.all_to_all(plane, AXES, 0, 0, axis_index_groups=planes(), tiled=True)
    line = small(sum_plane, jax.ShapeDtypeStruct((8, 56, 128), F32), plane)
    line = lax.all_to_all(line, "gy", 0, 0, tiled=True)
    new_q, new_p, new_t = small(
        finish,
        shapes((24, 128), (8, 128), (HEADS, ENT)),
        line,
        mom_qkv.reshape(24, 128),
        mom_proj.reshape(8, 128),
        mom_table.T,
    )
    return new_q.reshape(-1), new_p.reshape(-1), new_t.T


def solution(mesh):
    return jax.shard_map(
        body,
        mesh=mesh,
        in_specs=(
            P(AXES, None, None),
            P(AXES, None, None),
            P(AXES, None),
            P(),
            P(),
            P(),
            P(),
            P(AXES),
            P(AXES),
            P(),
        ),
        out_specs=(P(AXES), P(AXES), P()),
        check_vma=False,
    )
```

```python
import jax
import jax.numpy as jnp
from jax import lax
from jax.experimental import pallas as pl
from jax.experimental.pallas import tpu as pltpu
from jax.sharding import PartitionSpec as P

AXES = ("gx", "gy", "gz")
WIN = 16
TOK = 49
PAD = 64
D = 512
HEADS = 16
HD = 32
ENT = 169
EPAD = 176
UNROLL = 4
AHEAD = 2
ROWS = TOK * WIN
PROWS = PAD * WIN
F32 = jnp.float32
BF16 = jnp.bfloat16
NT = (((1,), (1,)), ((), ()))
NN = (((1,), (0,)), ((), ()))


def dot(a, b, dims=NN):
    return lax.dot_general(a, b, dims, preferred_element_type=F32)


def decode(flat):
    gx, gy, gz = flat // 32, (flat // 4) % 8, flat % 4
    return gx % 4, (gx // 4) * 2 + gz // 2, gy, gz % 2


def encode(x, y, z, c):
    x, y, z = x % 4, y % 4, z % 8
    return ((y // 2) * 4 + x) * 32 + z * 4 + (y % 2) * 2 + c


def shift(value, dx=0, dy=0, dz=0, dc=0):
    pairs = []
    for d in range(256):
        x, y, z, c = decode(d)
        pairs.append((d, encode(x + dx, y + dy, z + dz, c ^ dc)))
    return lax.ppermute(value, AXES, pairs)


def reorder(core, src, dst):
    r = lax.broadcasted_iota(jnp.int32, (128, 128), 0)
    col = lax.broadcasted_iota(jnp.int32, (128, 128), 1)
    e = r & 1
    z = (r >> 1) & 7
    x = (r >> 4) & 3
    y0 = (r >> 6) & 1
    for rc in range(2):
        c = (rc + core) & 1
        orig = ((x * 32 + z * 4 + y0 * 2 + c) << 1) + e
        hot = jnp.concatenate([jnp.where(orig == col + 128 * k, 1.0, 0.0) for k in range(2)], axis=1).astype(BF16)
        for y1 in range(2):
            at = 256 * rc + 128 * y1
            dst[at : at + 128] = dot(hot, src[:, 256 * y1 : 256 * y1 + 256], NT).astype(BF16)


def local_kernel(
    tok_h, cot_h, reg_h, rel_h, wqkv_h, wproj_h, tab_h, keep, send,
    tok, cot, reg, rel, wqkv, wproj, tab, sems, tokw, cotw, qkv_s, da_s, att_s, dqkv_s, bias_s, mask_s, acc_s, sq_s, t_s,
):
    moves = [
        pltpu.make_async_copy(src, dst, sems.at[n])
        for n, (src, dst) in enumerate(
            zip((tok_h, rel_h, reg_h, tab_h, wqkv_h, cot_h, wproj_h), (tok, rel, reg, tab, wqkv, cot, wproj))
        )
    ]
    for move in moves:
        move.start()
    factor = 1.4426950408889634
    scale = HD**-0.5

    line = lax.broadcasted_iota(jnp.int32, (256, 128), 0)
    lanes = lax.broadcasted_iota(jnp.int32, (256, 128), 1)
    source = (line & 15) * WIN + (line >> 4)
    pick = jnp.concatenate([jnp.where(source == lanes + 128 * k, 1.0, 0.0) for k in range(2)], axis=1).astype(BF16)
    alone = jnp.where(((line & 15) == 0) & ((line >> 4) == lanes), 1.0, 0.0).astype(BF16)[:, 0:WIN]

    def regroup(src, dst):
        for b in range(4):
            if b < 3:
                moved = dot(pick, src[256 * b : 256 * b + 256]).astype(BF16)
            else:
                moved = dot(alone, src[768:784]).astype(BF16)
            for w in range(WIN):
                dst[w * PAD + 16 * b : w * PAD + 16 * b + 16] = moved[16 * w : 16 * w + 16]

    for move in moves[0:4]:
        move.wait()
    regroup(tok, tokw)

    sq_s[...] = jnp.zeros((128, 128), F32)
    sq_s[0:TOK, 0:TOK] = rel[...].astype(F32)
    sq_s[PAD : PAD + TOK, 0:TOK] = rel[...].astype(F32)
    relt = jnp.transpose(sq_s[...])[0:PAD].astype(jnp.int32)
    lane = lax.broadcasted_iota(jnp.int32, (PAD, 128), 1)
    sub = lax.broadcasted_iota(jnp.int32, (PAD, 128), 0)
    live = ((lane & 63) < TOK) & (sub < TOK)
    relt = jnp.where(live, relt, -1)
    safe = jnp.where(live, relt, 0)
    low_i = jnp.where(safe < 128, safe, 0)
    high_i = jnp.where(safe < 128, 0, safe - 128)
    is_low = safe < 128
    first = lane < 64
    for hp in range(HEADS // 2):
        looked = []
        for par in range(2):
            h = 2 * hp + par
            low = jnp.broadcast_to(tab[h : h + 1, 0:128], (8, 128))
            high = jnp.concatenate([tab[h : h + 1, 128:ENT], jnp.zeros((1, 256 - ENT), F32)], axis=1)
            high = jnp.broadcast_to(high, (8, 128))
            rows = []
            for b in range(PAD // 8):
                s = slice(8 * b, 8 * b + 8)
                a0 = jnp.take_along_axis(low, low_i[s], axis=1, mode="promise_in_bounds")
                a1 = jnp.take_along_axis(high, high_i[s], axis=1, mode="promise_in_bounds")
                rows.append(jnp.where(is_low[s], a0, a1))
            looked.append(jnp.concatenate(rows, axis=0))
        both = jnp.where(first, looked[0], looked[1])
        bias_s[hp * PAD : (hp + 1) * PAD] = jnp.where(sub < TOK, both * factor, -1e30)

    sq_s[...] = jnp.zeros((128, 128), F32)
    sq_s[0:WIN, 0:TOK] = reg[...].astype(F32)
    base = sq_s[...]
    cols = jnp.transpose(base)
    for w in range(WIN):
        row = jnp.concatenate([base[w : w + 1, 0:64], base[w : w + 1, 0:64]], axis=1)
        mask_s[w * PAD : (w + 1) * PAD] = jnp.where(cols[0:PAD, w : w + 1] == row, 0.0, -100.0 * factor)

    acc_s[...] = jnp.zeros(acc_s.shape, F32)

    for move in moves[4:7]:
        move.wait()
    regroup(cot, cotw)
    for n in range(6):
        cols = slice(256 * n, 256 * n + 256)
        qkv_s[:, cols] = dot(tokw[...], wqkv[:, cols]).astype(BF16)
    for n in range(2):
        cols = slice(256 * n, 256 * n + 256)
        da_s[:, cols] = dot(cotw[...], wproj[cols], NT).astype(BF16)

    chan = lax.broadcasted_iota(jnp.int32, (PAD, 128), 1) // HD
    none = jnp.zeros((PAD, 128), BF16)

    def spread(v):
        return jnp.concatenate([jnp.where(chan == h, v, none) for h in range(4)], axis=0)

    def fold(full):
        total = full[0:PAD]
        for h in range(1, 4):
            total = jnp.where(chan == h, full[h * PAD : (h + 1) * PAD], total)
        return total.astype(BF16)

    def scores(rows, mask, g):
        cq = slice(g * 128, g * 128 + 128)
        k = qkv_s[rows, D + g * 128 : D + g * 128 + 128]
        v = qkv_s[rows, 2 * D + g * 128 : 2 * D + g * 128 + 128]
        qd = spread(qkv_s[rows, cq])
        dd = spread(da_s[rows, cq])
        return dict(rows=rows, mask=mask, g=g, k=k, v=v, qd=qd, dd=dd, s=dot(k, qd, NT), dp=dot(v, dd, NT))

    def softmax(it):
        g, mask = it["g"], it["mask"]
        bias = jnp.concatenate(
            [bias_s[2 * g * PAD : (2 * g + 1) * PAD] + mask, bias_s[(2 * g + 1) * PAD : (2 * g + 2) * PAD] + mask], axis=1
        )
        s = it["s"] * (scale * factor) + bias
        p = jnp.exp2(s - jnp.max(s, axis=0, keepdims=True))
        p = p * (1.0 / jnp.sum(p, axis=0, keepdims=True))
        dp = it["dp"].astype(BF16).astype(F32)
        ds = p * (dp - jnp.sum(dp * p, axis=0, keepdims=True))
        it["pb"] = p.astype(BF16)
        it["dsb"] = (ds * scale).astype(BF16)
        it["pt"] = jnp.transpose(it["pb"])
        it["dst"] = jnp.transpose(it["dsb"])
        return ds

    def results(it):
        rows, g = it["rows"], it["g"]
        cq = slice(g * 128, g * 128 + 128)
        dqkv_s[rows, 2 * D + g * 128 : 2 * D + g * 128 + 128] = dot(it["pb"], it["dd"]).astype(BF16)
        att_s[rows, cq] = fold(dot(it["pt"], it["v"]))
        dqkv_s[rows, D + g * 128 : D + g * 128 + 128] = dot(it["dsb"], it["qd"]).astype(BF16)
        dqkv_s[rows, cq] = fold(dot(it["dst"], it["k"]))

    def windows(step, carry):
        chains = []
        for g in range(4):
            for i in range(UNROLL):
                rows = pl.ds(pl.multiple_of((step * UNROLL + i) * PAD, PAD), PAD)
                chains.append((rows, i, g))
        masks = [mask_s[pl.ds(pl.multiple_of((step * UNROLL + i) * PAD, PAD), PAD), :] for i in range(UNROLL)]
        sums = [None] * 4
        items = []
        for c in range(len(chains) + 1 + AHEAD):
            if c < len(chains):
                rows, i, g = chains[c]
                items.append(scores(rows, masks[i], g))
            if 0 <= c - AHEAD < len(chains):
                it = items[c - AHEAD]
                ds = softmax(it)
                g = it["g"]
                sums[g] = ds if sums[g] is None else sums[g] + ds
                if c - AHEAD == UNROLL * g + UNROLL - 1:
                    acc_s[2 * g * PAD : (2 * g + 1) * PAD] += sums[g][:, 0:128]
                    acc_s[(2 * g + 1) * PAD : (2 * g + 2) * PAD] += sums[g][:, 128:256]
            if c - AHEAD - 1 >= 0:
                results(items[c - AHEAD - 1])
        return carry

    lax.fori_loop(0, WIN // UNROLL, windows, 0)

    ent = lax.broadcasted_iota(jnp.int32, (EPAD, 128), 0)
    sums = jnp.zeros((EPAD, 32), F32)
    left = lax.broadcasted_iota(jnp.int32, (8, 128), 1) < 64
    for j7 in range(7):
        hots, parts = [], []
        for j in range(7 * j7, 7 * j7 + 7):
            part = acc_s[pl.ds(j, 8, stride=PAD), :]
            top = part.astype(BF16).astype(F32)
            rest = part - top
            split = [jnp.where(left, top, 0.0), jnp.where(left, rest, 0.0), jnp.where(left, 0.0, top), jnp.where(left, 0.0, rest)]
            parts.append(jnp.concatenate(split, axis=0).astype(BF16))
            hots.append(jnp.where(ent == relt[j : j + 1], 1.0, 0.0).astype(BF16))
        sums = sums + dot(jnp.concatenate(hots, axis=1), jnp.concatenate(parts, axis=1), NT)
    sums = jnp.concatenate([sums, jnp.zeros((EPAD, 96), F32)], axis=1)
    sums = jnp.concatenate([sums, pltpu.roll(sums, 112, 1), jnp.zeros((384 - 2 * EPAD, 128), F32)], axis=0)
    flat = jnp.concatenate([jnp.transpose(sums[128 * k : 128 * k + 128])[0:16] for k in range(3)], axis=1)
    table = flat[0:8] + flat[8:16]
    for k in range(3):
        keep[4096 + 8 * k : 4104 + 8 * k] = table[:, 128 * k : 128 * k + 128]
        send[4096 + 8 * k : 4104 + 8 * k] = table[:, 128 * k : 128 * k + 128]

    core = lax.axis_index("gz") & 1

    def put(grad, block):
        for half in range(2):
            cols = slice(128 * half, 128 * half + 128)
            for k in range(16):
                at = 256 * k + 16 * (block + half)
                keep[at : at + 16] = grad[16 * k : 16 * k + 16, cols]
                send[at : at + 16] = grad[256 + 16 * k : 272 + 16 * k, cols]

    reorder(core, tokw, t_s)
    for n in range(6):
        put(dot(t_s[...], dqkv_s[:, 256 * n : 256 * n + 256]), 2 * n)
    reorder(core, att_s, t_s)
    for n in range(2):
        put(dot(t_s[...], cotw[:, 256 * n : 256 * n + 256]), 12 + 2 * n)


def place():
    gx, gz = lax.axis_index("gx"), lax.axis_index("gz")
    return gx & 3, ((gx >> 2) << 1) + (gz >> 1)


def block(index, size):
    return pl.ds(pl.multiple_of(index * size, size), size)


def sum_core(keep, got, *outs):
    one, two = outs[0:4], outs[4:8]
    x, y = place()
    table = keep[4096:4120] + got[4096:4120]
    for k in range(4):
        for other in range(4):
            rows = slice(128 * other, 128 * other + 128)
            at = block(2 * (4 * other + ((x + k) & 3)), 128)
            one[k][rows] = keep[at] + got[at]
            at = block(2 * (4 * ((y + k) & 3) + other) + 1, 128)
            two[k][rows] = keep[at] + got[at]
        one[k][512:536] = table


def four(refs, rows):
    return (refs[0][rows] + refs[2][rows]) + (refs[1][rows] + refs[3][rows])


def sum_first(*refs):
    a, b, one, two = refs[0:4], refs[4:8], refs[8:12], refs[12:16]
    x, y = place()
    table = four(a, slice(512, 536))
    for k in range(4):
        one[k][0:128] = four(a, block((y + k) & 3, 128))
        one[k][128:152] = table
        two[k][...] = four(b, block((x + k) & 3, 128))


def sum_second(*refs):
    a, b, out = refs[0:4], refs[4:8], refs[8]
    for n in range(16):
        rows = slice(16 * (n % 8), 16 * (n % 8) + 16)
        part = four(a if n < 8 else b, rows)
        for z in range(8):
            out[z, 2 * n : 2 * n + 2] = part[2 * z : 2 * z + 2]
    table = four(a, slice(128, 152))
    for z in range(8):
        out[z, 32:56] = table


def finish(got, mq, mp, mt, oq, op, ot):
    total = got[0]
    for k in range(1, 8):
        total = total + got[k]
    total = total * (1.0 / 4096)
    for e in range(2):
        for c in range(12):
            row = 2 * c + e
            r = slice(12 * e + c, 12 * e + c + 1)
            oq[r] = 0.9 * mq[r] + total[row : row + 1]
        for c in range(4):
            row = 2 * (12 + c) + e
            r = slice(4 * e + c, 4 * e + c + 1)
            op[r] = 0.9 * mp[r] + total[row : row + 1]
    table = jnp.concatenate([total[32:40], total[40:48], total[48:56]], axis=1)
    for h in range(HEADS):
        at = (h % 2) * EPAD
        ot[h : h + 1] = 0.9 * mt[h : h + 1] + table[h // 2 : h // 2 + 1, at : at + ENT]


def shapes(*dims):
    return tuple(jax.ShapeDtypeStruct(d, F32) for d in dims)


def local_grads(tok, cot, regions, rel_index, w_qkv, w_proj, table, interpret=False):
    return pl.pallas_call(
        local_kernel,
        out_shape=shapes((4120, 128), (4120, 128)),
        in_specs=[pl.BlockSpec(memory_space=pltpu.HBM)] * 7,
        scratch_shapes=[
            pltpu.VMEM((ROWS, D), BF16),
            pltpu.VMEM((ROWS, D), BF16),
            pltpu.VMEM((WIN, TOK), jnp.int32),
            pltpu.VMEM((TOK, TOK), jnp.int32),
            pltpu.VMEM((D, 3 * D), BF16),
            pltpu.VMEM((D, D), BF16),
            pltpu.VMEM((HEADS, ENT), F32),
            pltpu.SemaphoreType.DMA((7,)),
            pltpu.VMEM((PROWS, D), BF16),
            pltpu.VMEM((PROWS, D), BF16),
            pltpu.VMEM((PROWS, 3 * D), BF16),
            pltpu.VMEM((PROWS, D), BF16),
            pltpu.VMEM((PROWS, D), BF16),
            pltpu.VMEM((PROWS, 3 * D), BF16),
            pltpu.VMEM((8 * PAD, 128), F32),
            pltpu.VMEM((WIN * PAD, 128), F32),
            pltpu.VMEM((8 * PAD, 128), F32),
            pltpu.VMEM((128, 128), F32),
            pltpu.VMEM((D, PROWS), BF16),
        ],
        name="local_grads",
        compiler_params=pltpu.CompilerParams(vmem_limit_bytes=40 << 20),
        interpret=interpret,
    )(*(pltpu.with_memory_space_constraint(v, pltpu.HBM) for v in (tok, cot, regions, rel_index, w_qkv, w_proj, table)))


def small(kernel, out_shape, *args):
    return pl.pallas_call(
        kernel, out_shape=out_shape, name=kernel.__name__, compiler_params=pltpu.CompilerParams(vmem_limit_bytes=3 << 20)
    )(*args)


def spread_out(m, one, two):
    m = list(m)
    for k in (2, 1, 3):
        m[k] = shift(m[k], **{one: k})
        m[4 + k] = shift(m[4 + k], **{two: k})
    return m


def body(
    tokens, cotangent, regions, rel_index, w_qkv, w_proj, bias_table, mom_qkv, mom_proj, mom_table
):
    tok = jnp.transpose(tokens, (1, 0, 2)).reshape(ROWS, D)
    cot = jnp.transpose(cotangent, (1, 0, 2)).reshape(ROWS, D)
    keep, send = local_grads(tok, cot, regions, rel_index, w_qkv, w_proj, bias_table.T)
    got = shift(send, dc=1)
    m = small(sum_core, shapes(*[(536, 128)] * 4, *[(512, 128)] * 4), keep, got)
    m = spread_out(m, "dx", "dy")
    m = small(sum_first, shapes(*[(152, 128)] * 4, *[(128, 128)] * 4), *m)
    m = spread_out(m, "dy", "dx")
    line = small(sum_second, jax.ShapeDtypeStruct((8, 56, 128), F32), *m)
    line = lax.all_to_all(line, "gy", 0, 0, tiled=True)
    new_q, new_p, new_t = small(
        finish,
        shapes((24, 128), (8, 128), (HEADS, ENT)),
        line,
        mom_qkv.reshape(24, 128),
        mom_proj.reshape(8, 128),
        mom_table.T,
    )
    return new_q.reshape(-1), new_p.reshape(-1), new_t.T


def solution(mesh):
    return jax.shard_map(
        body,
        mesh=mesh,
        in_specs=(
            P(AXES, None, None),
            P(AXES, None, None),
            P(AXES, None),
            P(),
            P(),
            P(),
            P(),
            P(AXES),
            P(AXES),
            P(),
        ),
        out_specs=(P(AXES), P(AXES), P()),
        check_vma=False,
    )
```

```python
import jax
import jax.numpy as jnp
from jax import lax
from jax.experimental import pallas as pl
from jax.experimental.pallas import tpu as pltpu
from jax.sharding import PartitionSpec as P


AXES = ("gx", "gy", "gz")
WIN = 16
TOK = 49
PAD = 64
D = 512
HEADS = 16
HD = 32
ENT = 169
EPAD = 176
UNROLL = 8
OFFSETS = (2, 1, 3, 0)
AHEAD = 2
ROWS = TOK * WIN
PROWS = PAD * WIN
F32 = jnp.float32
BF16 = jnp.bfloat16
NT = (((1,), (1,)), ((), ()))
NN = (((1,), (0,)), ((), ()))


def dot(a, b, dims=NN):
    return lax.dot_general(a, b, dims, preferred_element_type=F32)


def decode(flat):
    gx, gy, gz = flat // 32, (flat // 4) % 8, flat % 4
    return gx % 4, (gx // 4) * 2 + gz // 2, gy, gz % 2


def encode(x, y, z, c):
    x, y, z = x % 4, y % 4, z % 8
    return ((y // 2) * 4 + x) * 32 + z * 4 + (y % 2) * 2 + c


def shift(value, dx=0, dy=0, dz=0, dc=0):
    pairs = []
    for d in range(256):
        x, y, z, c = decode(d)
        pairs.append((d, encode(x + dx, y + dy, z + dz, c ^ dc)))
    return lax.ppermute(value, AXES, pairs)


def reorder(core, src, dst):
    r = lax.broadcasted_iota(jnp.int32, (128, 128), 0)
    col = lax.broadcasted_iota(jnp.int32, (128, 128), 1)
    e = r & 1
    z = (r >> 1) & 7
    x = (r >> 4) & 3
    y0 = (r >> 6) & 1
    for rc in range(2):
        c = (rc + core) & 1
        orig = ((x * 32 + z * 4 + y0 * 2 + c) << 1) + e
        hot = jnp.concatenate([jnp.where(orig == col + 128 * k, 1.0, 0.0) for k in range(2)], axis=1).astype(BF16)
        for y1 in range(2):
            at = 256 * rc + 128 * y1
            dst[at : at + 128] = dot(hot, src[:, 256 * y1 : 256 * y1 + 256], NT).astype(BF16)


def local_kernel(
    tok_h, cot_h, reg_h, rel_h, wqkv_h, wproj_h, tab_h, keep, send,
    tok, cot, reg, rel, wqkv, wproj, tab, sems, tokw, cotw, qkv_s, da_s, att_s, dqkv_s, bias_s, mask_s, acc_s, sq_s, t_s,
):
    moves = [
        pltpu.make_async_copy(src, dst, sems.at[n])
        for n, (src, dst) in enumerate(
            zip((tok_h, rel_h, reg_h, tab_h, wqkv_h, cot_h, wproj_h), (tok, rel, reg, tab, wqkv, cot, wproj))
        )
    ]
    for move in moves:
        move.start()
    factor = 1.4426950408889634
    scale = HD**-0.5

    line = lax.broadcasted_iota(jnp.int32, (256, 128), 0)
    lanes = lax.broadcasted_iota(jnp.int32, (256, 128), 1)
    source = (line & 15) * WIN + (line >> 4)
    pick = jnp.concatenate([jnp.where(source == lanes + 128 * k, 1.0, 0.0) for k in range(2)], axis=1).astype(BF16)
    alone = jnp.where(((line & 15) == 0) & ((line >> 4) == lanes), 1.0, 0.0).astype(BF16)[:, 0:WIN]

    def regroup(src, dst):
        for b in range(4):
            if b < 3:
                moved = dot(pick, src[256 * b : 256 * b + 256]).astype(BF16)
            else:
                moved = dot(alone, src[768:784]).astype(BF16)
            for w in range(WIN):
                dst[w * PAD + 16 * b : w * PAD + 16 * b + 16] = moved[16 * w : 16 * w + 16]

    for move in moves[0:4]:
        move.wait()
    regroup(tok, tokw)

    sq_s[...] = jnp.zeros((128, 128), F32)
    sq_s[0:TOK, 0:TOK] = rel[...].astype(F32)
    sq_s[PAD : PAD + TOK, 0:TOK] = rel[...].astype(F32)
    relt = jnp.transpose(sq_s[...])[0:PAD].astype(jnp.int32)
    lane = lax.broadcasted_iota(jnp.int32, (PAD, 128), 1)
    sub = lax.broadcasted_iota(jnp.int32, (PAD, 128), 0)
    live = ((lane & 63) < TOK) & (sub < TOK)
    relt = jnp.where(live, relt, -1)
    safe = jnp.where(live, relt, 0)
    low_i = jnp.where(safe < 128, safe, 0)
    high_i = jnp.where(safe < 128, 0, safe - 128)
    is_low = safe < 128
    first = lane < 64
    for hp in range(HEADS // 2):
        looked = []
        for par in range(2):
            h = 2 * hp + par
            low = jnp.broadcast_to(tab[h : h + 1, 0:128], (8, 128))
            high = jnp.concatenate([tab[h : h + 1, 128:ENT], jnp.zeros((1, 256 - ENT), F32)], axis=1)
            high = jnp.broadcast_to(high, (8, 128))
            rows = []
            for b in range(PAD // 8):
                s = slice(8 * b, 8 * b + 8)
                a0 = jnp.take_along_axis(low, low_i[s], axis=1, mode="promise_in_bounds")
                a1 = jnp.take_along_axis(high, high_i[s], axis=1, mode="promise_in_bounds")
                rows.append(jnp.where(is_low[s], a0, a1))
            looked.append(jnp.concatenate(rows, axis=0))
        both = jnp.where(first, looked[0], looked[1])
        bias_s[hp * PAD : (hp + 1) * PAD] = jnp.where(sub < TOK, both * factor, -1e30)

    sq_s[...] = jnp.zeros((128, 128), F32)
    sq_s[0:WIN, 0:TOK] = reg[...].astype(F32)
    base = sq_s[...]
    cols = jnp.transpose(base)
    for w in range(WIN):
        row = jnp.concatenate([base[w : w + 1, 0:64], base[w : w + 1, 0:64]], axis=1)
        mask_s[w * PAD : (w + 1) * PAD] = jnp.where(cols[0:PAD, w : w + 1] == row, 0.0, -100.0 * factor)

    acc_s[...] = jnp.zeros(acc_s.shape, F32)

    for move in moves[4:7]:
        move.wait()
    regroup(cot, cotw)
    for n in range(6):
        cols = slice(256 * n, 256 * n + 256)
        qkv_s[:, cols] = dot(tokw[...], wqkv[:, cols]).astype(BF16)
    for n in range(2):
        cols = slice(256 * n, 256 * n + 256)
        da_s[:, cols] = dot(cotw[...], wproj[cols], NT).astype(BF16)

    chan = lax.broadcasted_iota(jnp.int32, (PAD, 128), 1) // HD
    none = jnp.zeros((PAD, 128), BF16)

    def spread(v):
        return jnp.concatenate([jnp.where(chan == h, v, none) for h in range(4)], axis=0)

    def fold(full):
        total = full[0:PAD]
        for h in range(1, 4):
            total = jnp.where(chan == h, full[h * PAD : (h + 1) * PAD], total)
        return total.astype(BF16)

    def scores(rows, mask, g):
        cq = slice(g * 128, g * 128 + 128)
        k = qkv_s[rows, D + g * 128 : D + g * 128 + 128]
        v = qkv_s[rows, 2 * D + g * 128 : 2 * D + g * 128 + 128]
        qd = spread(qkv_s[rows, cq])
        dd = spread(da_s[rows, cq])
        return dict(rows=rows, mask=mask, g=g, k=k, v=v, qd=qd, dd=dd, s=dot(k, qd, NT), dp=dot(v, dd, NT))

    def softmax(it):
        g, mask = it["g"], it["mask"]
        bias = jnp.concatenate(
            [bias_s[2 * g * PAD : (2 * g + 1) * PAD] + mask, bias_s[(2 * g + 1) * PAD : (2 * g + 2) * PAD] + mask], axis=1
        )
        s = it["s"] * (scale * factor) + bias
        p = jnp.exp2(s - jnp.max(s, axis=0, keepdims=True))
        p = p * (1.0 / jnp.sum(p, axis=0, keepdims=True))
        dp = it["dp"].astype(BF16).astype(F32)
        ds = p * (dp - jnp.sum(dp * p, axis=0, keepdims=True))
        it["pb"] = p.astype(BF16)
        it["dsb"] = (ds * scale).astype(BF16)
        it["pt"] = jnp.transpose(it["pb"])
        it["dst"] = jnp.transpose(it["dsb"])
        return ds

    def results(it):
        rows, g = it["rows"], it["g"]
        cq = slice(g * 128, g * 128 + 128)
        dqkv_s[rows, 2 * D + g * 128 : 2 * D + g * 128 + 128] = dot(it["pb"], it["dd"]).astype(BF16)
        att_s[rows, cq] = fold(dot(it["pt"], it["v"]))
        dqkv_s[rows, D + g * 128 : D + g * 128 + 128] = dot(it["dsb"], it["qd"]).astype(BF16)
        dqkv_s[rows, cq] = fold(dot(it["dst"], it["k"]))

    def windows(step, carry):
        chains = []
        for g in range(4):
            for i in range(UNROLL):
                rows = pl.ds(pl.multiple_of((step * UNROLL + i) * PAD, PAD), PAD)
                chains.append((rows, i, g))
        masks = [mask_s[pl.ds(pl.multiple_of((step * UNROLL + i) * PAD, PAD), PAD), :] for i in range(UNROLL)]
        sums = [None] * 4
        items = []
        for c in range(len(chains) + 1 + AHEAD):
            if c < len(chains):
                rows, i, g = chains[c]
                items.append(scores(rows, masks[i], g))
            if 0 <= c - AHEAD < len(chains):
                it = items[c - AHEAD]
                ds = softmax(it)
                g = it["g"]
                sums[g] = ds if sums[g] is None else sums[g] + ds
                if c - AHEAD == UNROLL * g + UNROLL - 1:
                    acc_s[2 * g * PAD : (2 * g + 1) * PAD] += sums[g][:, 0:128]
                    acc_s[(2 * g + 1) * PAD : (2 * g + 2) * PAD] += sums[g][:, 128:256]
            if c - AHEAD - 1 >= 0:
                results(items[c - AHEAD - 1])
        return carry

    lax.fori_loop(0, WIN // UNROLL, windows, 0)

    ent = lax.broadcasted_iota(jnp.int32, (EPAD, 128), 0)
    sums = jnp.zeros((EPAD, 32), F32)
    left = lax.broadcasted_iota(jnp.int32, (8, 128), 1) < 64
    for j7 in range(7):
        hots, parts = [], []
        for j in range(7 * j7, 7 * j7 + 7):
            part = acc_s[pl.ds(j, 8, stride=PAD), :]
            top = part.astype(BF16).astype(F32)
            rest = part - top
            split = [jnp.where(left, top, 0.0), jnp.where(left, rest, 0.0), jnp.where(left, 0.0, top), jnp.where(left, 0.0, rest)]
            parts.append(jnp.concatenate(split, axis=0).astype(BF16))
            hots.append(jnp.where(ent == relt[j : j + 1], 1.0, 0.0).astype(BF16))
        sums = sums + dot(jnp.concatenate(hots, axis=1), jnp.concatenate(parts, axis=1), NT)
    sums = jnp.concatenate([sums, jnp.zeros((EPAD, 96), F32)], axis=1)
    sums = jnp.concatenate([sums, pltpu.roll(sums, 112, 1), jnp.zeros((384 - 2 * EPAD, 128), F32)], axis=0)
    flat = jnp.concatenate([jnp.transpose(sums[128 * k : 128 * k + 128])[0:16] for k in range(3)], axis=1)
    table = flat[0:8] + flat[8:16]
    for k in range(3):
        keep[4096 + 8 * k : 4104 + 8 * k] = table[:, 128 * k : 128 * k + 128]
        send[4096 + 8 * k : 4104 + 8 * k] = table[:, 128 * k : 128 * k + 128]

    core = lax.axis_index("gz") & 1

    def put(grad, block):
        for half in range(2):
            cols = slice(128 * half, 128 * half + 128)
            for k in range(16):
                at = 256 * k + 16 * (block + half)
                keep[at : at + 16] = grad[16 * k : 16 * k + 16, cols]
                send[at : at + 16] = grad[256 + 16 * k : 272 + 16 * k, cols]

    reorder(core, tokw, t_s)
    for n in range(6):
        put(dot(t_s[...], dqkv_s[:, 256 * n : 256 * n + 256]), 2 * n)
    reorder(core, att_s, t_s)
    for n in range(2):
        put(dot(t_s[...], cotw[:, 256 * n : 256 * n + 256]), 12 + 2 * n)


def place():
    gx, gz = lax.axis_index("gx"), lax.axis_index("gz")
    return gx & 3, ((gx >> 2) << 1) + (gz >> 1)


def block(index, size):
    return pl.ds(pl.multiple_of(index * size, size), size)


def by_offset(refs):
    return [[refs[2 * OFFSETS.index(k) + half] for k in range(4)] for half in range(2)]


def sum_core(keep, got, *outs):
    one, two = by_offset(outs)
    x, y = place()
    table = keep[4096:4120] + got[4096:4120]
    for k in range(4):
        for other in range(4):
            rows = slice(128 * other, 128 * other + 128)
            at = block(2 * (4 * other + ((x + k) & 3)), 128)
            one[k][rows] = keep[at] + got[at]
            at = block(2 * (4 * ((y + k) & 3) + other) + 1, 128)
            two[k][rows] = keep[at] + got[at]
        one[k][512:536] = table


def four(refs, rows):
    return (refs[0][rows] + refs[2][rows]) + (refs[1][rows] + refs[3][rows])


def sum_first(*refs):
    (a, b), (one, two) = by_offset(refs[0:8]), by_offset(refs[8:16])
    x, y = place()
    table = four(a, slice(512, 536))
    for k in range(4):
        one[k][0:128] = four(a, block((y + k) & 3, 128))
        one[k][128:152] = table
        two[k][...] = four(b, block((x + k) & 3, 128))


def sum_second(*refs):
    (a, b), out = by_offset(refs[0:8]), refs[8]
    for n in range(16):
        rows = slice(16 * (n % 8), 16 * (n % 8) + 16)
        part = four(a if n < 8 else b, rows)
        for z in range(8):
            out[z, 2 * n : 2 * n + 2] = part[2 * z : 2 * z + 2]
    table = four(a, slice(128, 152))
    for z in range(8):
        out[z, 32:56] = table


def finish(got, mq, mp, mt, oq, op, ot):
    total = got[0]
    for k in range(1, 8):
        total = total + got[k]
    total = total * (1.0 / 4096)
    for e in range(2):
        for c in range(12):
            row = 2 * c + e
            r = slice(12 * e + c, 12 * e + c + 1)
            oq[r] = 0.9 * mq[r] + total[row : row + 1]
        for c in range(4):
            row = 2 * (12 + c) + e
            r = slice(4 * e + c, 4 * e + c + 1)
            op[r] = 0.9 * mp[r] + total[row : row + 1]
    table = jnp.concatenate([total[32:40], total[40:48], total[48:56]], axis=1)
    for h in range(HEADS):
        at = (h % 2) * EPAD
        ot[h : h + 1] = 0.9 * mt[h : h + 1] + table[h // 2 : h // 2 + 1, at : at + ENT]


def shapes(*dims):
    return tuple(jax.ShapeDtypeStruct(d, F32) for d in dims)


def local_grads(tok, cot, regions, rel_index, w_qkv, w_proj, table, interpret=False):
    return pl.pallas_call(
        local_kernel,
        out_shape=shapes((4120, 128), (4120, 128)),
        in_specs=[pl.BlockSpec(memory_space=pltpu.HBM)] * 7,
        scratch_shapes=[
            pltpu.VMEM((ROWS, D), BF16),
            pltpu.VMEM((ROWS, D), BF16),
            pltpu.VMEM((WIN, TOK), jnp.int32),
            pltpu.VMEM((TOK, TOK), jnp.int32),
            pltpu.VMEM((D, 3 * D), BF16),
            pltpu.VMEM((D, D), BF16),
            pltpu.VMEM((HEADS, ENT), F32),
            pltpu.SemaphoreType.DMA((7,)),
            pltpu.VMEM((PROWS, D), BF16),
            pltpu.VMEM((PROWS, D), BF16),
            pltpu.VMEM((PROWS, 3 * D), BF16),
            pltpu.VMEM((PROWS, D), BF16),
            pltpu.VMEM((PROWS, D), BF16),
            pltpu.VMEM((PROWS, 3 * D), BF16),
            pltpu.VMEM((8 * PAD, 128), F32),
            pltpu.VMEM((WIN * PAD, 128), F32),
            pltpu.VMEM((8 * PAD, 128), F32),
            pltpu.VMEM((128, 128), F32),
            pltpu.VMEM((D, PROWS), BF16),
        ],
        name="local_grads",
        compiler_params=pltpu.CompilerParams(vmem_limit_bytes=40 << 20),
        interpret=interpret,
    )(*(pltpu.with_memory_space_constraint(v, pltpu.HBM) for v in (tok, cot, regions, rel_index, w_qkv, w_proj, table)))


def small(kernel, out_shape, *args):
    return pl.pallas_call(
        kernel, out_shape=out_shape, compiler_params=pltpu.CompilerParams(vmem_limit_bytes=3 << 20)
    )(*args)


def spread_out(m, one, two):
    out = list(m)
    for n in range(6):
        out[n] = shift(m[n], **{(one, two)[n % 2]: OFFSETS[n // 2]})
    return out


def body(
    tokens, cotangent, regions, rel_index, w_qkv, w_proj, bias_table, mom_qkv, mom_proj, mom_table
):
    tok = jnp.transpose(tokens, (1, 0, 2)).reshape(ROWS, D)
    cot = jnp.transpose(cotangent, (1, 0, 2)).reshape(ROWS, D)
    keep, send = local_grads(tok, cot, regions, rel_index, w_qkv, w_proj, bias_table.T)
    got = shift(send, dc=1)
    m = small(sum_core, shapes(*[(536, 128), (512, 128)] * 4), keep, got)
    m = spread_out(m, "dx", "dy")
    m = small(sum_first, shapes(*[(152, 128), (128, 128)] * 4), *m)
    m = spread_out(m, "dy", "dx")
    line = small(sum_second, jax.ShapeDtypeStruct((8, 56, 128), F32), *m)
    line = lax.all_to_all(line, "gy", 0, 0, tiled=True)
    new_q, new_p, new_t = small(
        finish,
        shapes((24, 128), (8, 128), (HEADS, ENT)),
        line,
        mom_qkv.reshape(24, 128),
        mom_proj.reshape(8, 128),
        mom_table.T,
    )
    return new_q.reshape(-1), new_p.reshape(-1), new_t.T


def solution(mesh):
    return jax.shard_map(
        body,
        mesh=mesh,
        in_specs=(
            P(AXES, None, None),
            P(AXES, None, None),
            P(AXES, None),
            P(),
            P(),
            P(),
            P(),
            P(AXES),
            P(AXES),
            P(),
        ),
        out_specs=(P(AXES), P(AXES), P()),
        check_vma=False,
    )
```

```python
import jax
import jax.numpy as jnp
from jax import lax
from jax.experimental import pallas as pl
from jax.experimental.pallas import tpu as pltpu
from jax.sharding import PartitionSpec as P


AXES = ("gx", "gy", "gz")
WIN = 16
TOK = 49
PAD = 64
D = 512
HEADS = 16
HD = 32
ENT = 169
EPAD = 176
UNROLL = 8
OFFSETS = (2, 1, 3, 0)
AHEAD = 2
ROWS = TOK * WIN
PROWS = PAD * WIN
F32 = jnp.float32
BF16 = jnp.bfloat16
NT = (((1,), (1,)), ((), ()))
NN = (((1,), (0,)), ((), ()))


def dot(a, b, dims=NN):
    return lax.dot_general(a, b, dims, preferred_element_type=F32)


def decode(flat):
    gx, gy, gz = flat // 32, (flat // 4) % 8, flat % 4
    return gx % 4, (gx // 4) * 2 + gz // 2, gy, gz % 2


def encode(x, y, z, c):
    x, y, z = x % 4, y % 4, z % 8
    return ((y // 2) * 4 + x) * 32 + z * 4 + (y % 2) * 2 + c


def shift(value, dx=0, dy=0, dz=0, dc=0):
    pairs = []
    for d in range(256):
        x, y, z, c = decode(d)
        pairs.append((d, encode(x + dx, y + dy, z + dz, c ^ dc)))
    return lax.ppermute(value, AXES, pairs)


def reorder(core, src, dst):
    r = lax.broadcasted_iota(jnp.int32, (128, 128), 0)
    col = lax.broadcasted_iota(jnp.int32, (128, 128), 1)
    e = r & 1
    z = (r >> 1) & 7
    x = (r >> 4) & 3
    y0 = (r >> 6) & 1
    for rc in range(2):
        c = (rc + core) & 1
        orig = ((x * 32 + z * 4 + y0 * 2 + c) << 1) + e
        hot = jnp.concatenate([jnp.where(orig == col + 128 * k, 1.0, 0.0) for k in range(2)], axis=1).astype(BF16)
        for y1 in range(2):
            at = 256 * rc + 128 * y1
            dst[at : at + 128] = dot(hot, src[:, 256 * y1 : 256 * y1 + 256], NT).astype(BF16)


def local_kernel(
    tok_h, cot_h, reg_h, rel_h, wqkv_h, wproj_h, tab_h, keep1, keep2, send1, send2,
    tok, cot, reg, rel, wqkv, wproj, tab, sems, tokw, cotw, qkv_s, da_s, att_s, dqkv_s, bias_s, mask_s, acc_s, sq_s, t_s,
):
    moves = [
        pltpu.make_async_copy(src, dst, sems.at[n])
        for n, (src, dst) in enumerate(
            zip((rel_h, reg_h, tab_h, tok_h, wqkv_h, cot_h, wproj_h), (rel, reg, tab, tok, wqkv, cot, wproj))
        )
    ]
    for move in moves:
        move.start()
    factor = 1.4426950408889634
    scale = HD**-0.5

    line = lax.broadcasted_iota(jnp.int32, (256, 128), 0)
    lanes = lax.broadcasted_iota(jnp.int32, (256, 128), 1)
    source = (line & 15) * WIN + (line >> 4)
    pick = jnp.concatenate([jnp.where(source == lanes + 128 * k, 1.0, 0.0) for k in range(2)], axis=1).astype(BF16)
    alone = jnp.where(((line & 15) == 0) & ((line >> 4) == lanes), 1.0, 0.0).astype(BF16)[:, 0:WIN]

    def regroup(src, dst):
        for b in range(4):
            if b < 3:
                moved = dot(pick, src[256 * b : 256 * b + 256]).astype(BF16)
            else:
                moved = dot(alone, src[768:784]).astype(BF16)
            for w in range(WIN):
                dst[w * PAD + 16 * b : w * PAD + 16 * b + 16] = moved[16 * w : 16 * w + 16]

    for move in moves[0:3]:
        move.wait()

    sq_s[...] = jnp.zeros((128, 128), F32)
    sq_s[0:TOK, 0:TOK] = rel[...].astype(F32)
    sq_s[PAD : PAD + TOK, 0:TOK] = rel[...].astype(F32)
    relt = jnp.transpose(sq_s[...])[0:PAD].astype(jnp.int32)
    lane = lax.broadcasted_iota(jnp.int32, (PAD, 128), 1)
    sub = lax.broadcasted_iota(jnp.int32, (PAD, 128), 0)
    live = ((lane & 63) < TOK) & (sub < TOK)
    relt = jnp.where(live, relt, -1)
    safe = jnp.where(live, relt, 0)
    low_i = jnp.where(safe < 128, safe, 0)
    high_i = jnp.where(safe < 128, 0, safe - 128)
    is_low = safe < 128
    first = lane < 64
    for hp in range(HEADS // 2):
        looked = []
        for par in range(2):
            h = 2 * hp + par
            low = jnp.broadcast_to(tab[h : h + 1, 0:128], (8, 128))
            high = jnp.concatenate([tab[h : h + 1, 128:ENT], jnp.zeros((1, 256 - ENT), F32)], axis=1)
            high = jnp.broadcast_to(high, (8, 128))
            rows = []
            for b in range(PAD // 8):
                s = slice(8 * b, 8 * b + 8)
                a0 = jnp.take_along_axis(low, low_i[s], axis=1, mode="promise_in_bounds")
                a1 = jnp.take_along_axis(high, high_i[s], axis=1, mode="promise_in_bounds")
                rows.append(jnp.where(is_low[s], a0, a1))
            looked.append(jnp.concatenate(rows, axis=0))
        both = jnp.where(first, looked[0], looked[1])
        bias_s[hp * PAD : (hp + 1) * PAD] = jnp.where(sub < TOK, both * factor, -1e30)

    sq_s[...] = jnp.zeros((128, 128), F32)
    sq_s[0:WIN, 0:TOK] = reg[...].astype(F32)
    base = sq_s[...]
    cols = jnp.transpose(base)
    for w in range(WIN):
        row = jnp.concatenate([base[w : w + 1, 0:64], base[w : w + 1, 0:64]], axis=1)
        mask_s[w * PAD : (w + 1) * PAD] = jnp.where(cols[0:PAD, w : w + 1] == row, 0.0, -100.0 * factor)

    acc_s[...] = jnp.zeros(acc_s.shape, F32)

    for move in moves[3:7]:
        move.wait()
    regroup(tok, tokw)
    regroup(cot, cotw)
    for n in range(6):
        cols = slice(256 * n, 256 * n + 256)
        qkv_s[:, cols] = dot(tokw[...], wqkv[:, cols]).astype(BF16)
    for n in range(2):
        cols = slice(256 * n, 256 * n + 256)
        da_s[:, cols] = dot(cotw[...], wproj[cols], NT).astype(BF16)

    chan = lax.broadcasted_iota(jnp.int32, (PAD, 128), 1) // HD
    none = jnp.zeros((PAD, 128), BF16)

    def spread(v):
        return jnp.concatenate([jnp.where(chan == h, v, none) for h in range(4)], axis=0)

    def fold(full):
        total = full[0:PAD]
        for h in range(1, 4):
            total = jnp.where(chan == h, full[h * PAD : (h + 1) * PAD], total)
        return total.astype(BF16)

    def scores(rows, mask, g):
        cq = slice(g * 128, g * 128 + 128)
        k = qkv_s[rows, D + g * 128 : D + g * 128 + 128]
        v = qkv_s[rows, 2 * D + g * 128 : 2 * D + g * 128 + 128]
        qd = spread(qkv_s[rows, cq])
        dd = spread(da_s[rows, cq])
        return dict(rows=rows, mask=mask, g=g, k=k, v=v, qd=qd, dd=dd, s=dot(k, qd, NT), dp=dot(v, dd, NT))

    def softmax(it):
        g, mask = it["g"], it["mask"]
        bias = jnp.concatenate(
            [bias_s[2 * g * PAD : (2 * g + 1) * PAD] + mask, bias_s[(2 * g + 1) * PAD : (2 * g + 2) * PAD] + mask], axis=1
        )
        s = it["s"] * (scale * factor) + bias
        p = jnp.exp2(s - jnp.max(s, axis=0, keepdims=True))
        p = p * (1.0 / jnp.sum(p, axis=0, keepdims=True))
        dp = it["dp"].astype(BF16).astype(F32)
        ds = p * (dp - jnp.sum(dp * p, axis=0, keepdims=True))
        it["pb"] = p.astype(BF16)
        it["dsb"] = (ds * scale).astype(BF16)
        it["pt"] = jnp.transpose(it["pb"])
        it["dst"] = jnp.transpose(it["dsb"])
        return ds

    def results(it):
        rows, g = it["rows"], it["g"]
        cq = slice(g * 128, g * 128 + 128)
        dqkv_s[rows, 2 * D + g * 128 : 2 * D + g * 128 + 128] = dot(it["pb"], it["dd"]).astype(BF16)
        att_s[rows, cq] = fold(dot(it["pt"], it["v"]))
        dqkv_s[rows, D + g * 128 : D + g * 128 + 128] = dot(it["dsb"], it["qd"]).astype(BF16)
        dqkv_s[rows, cq] = fold(dot(it["dst"], it["k"]))

    def windows(step, carry):
        chains = []
        for g in range(4):
            for i in range(UNROLL):
                rows = pl.ds(pl.multiple_of((step * UNROLL + i) * PAD, PAD), PAD)
                chains.append((rows, i, g))
        masks = [mask_s[pl.ds(pl.multiple_of((step * UNROLL + i) * PAD, PAD), PAD), :] for i in range(UNROLL)]
        sums = [None] * 4
        items = []
        for c in range(len(chains) + 1 + AHEAD):
            if c < len(chains):
                rows, i, g = chains[c]
                items.append(scores(rows, masks[i], g))
            if 0 <= c - AHEAD < len(chains):
                it = items[c - AHEAD]
                ds = softmax(it)
                g = it["g"]
                sums[g] = ds if sums[g] is None else sums[g] + ds
                if c - AHEAD == UNROLL * g + UNROLL - 1:
                    acc_s[2 * g * PAD : (2 * g + 1) * PAD] += sums[g][:, 0:128]
                    acc_s[(2 * g + 1) * PAD : (2 * g + 2) * PAD] += sums[g][:, 128:256]
            if c - AHEAD - 1 >= 0:
                results(items[c - AHEAD - 1])
        return carry

    lax.fori_loop(0, WIN // UNROLL, windows, 0)

    ent = lax.broadcasted_iota(jnp.int32, (EPAD, 128), 0)
    sums = jnp.zeros((EPAD, 32), F32)
    left = lax.broadcasted_iota(jnp.int32, (8, 128), 1) < 64
    for j7 in range(7):
        hots, parts = [], []
        for j in range(7 * j7, 7 * j7 + 7):
            part = acc_s[pl.ds(j, 8, stride=PAD), :]
            top = part.astype(BF16).astype(F32)
            rest = part - top
            split = [jnp.where(left, top, 0.0), jnp.where(left, rest, 0.0), jnp.where(left, 0.0, top), jnp.where(left, 0.0, rest)]
            parts.append(jnp.concatenate(split, axis=0).astype(BF16))
            hots.append(jnp.where(ent == relt[j : j + 1], 1.0, 0.0).astype(BF16))
        sums = sums + dot(jnp.concatenate(hots, axis=1), jnp.concatenate(parts, axis=1), NT)
    sums = jnp.concatenate([sums, jnp.zeros((EPAD, 96), F32)], axis=1)
    sums = jnp.concatenate([sums, pltpu.roll(sums, 112, 1), jnp.zeros((384 - 2 * EPAD, 128), F32)], axis=0)
    flat = jnp.concatenate([jnp.transpose(sums[128 * k : 128 * k + 128])[0:16] for k in range(3)], axis=1)
    table = flat[0:8] + flat[8:16]
    for k in range(3):
        keep1[2048 + 8 * k : 2056 + 8 * k] = table[:, 128 * k : 128 * k + 128]
        send1[2048 + 8 * k : 2056 + 8 * k] = table[:, 128 * k : 128 * k + 128]

    core = lax.axis_index("gz") & 1

    def put(grad, block):
        keep, send = (keep1, send1) if block < 8 else (keep2, send2)
        for half in range(2):
            cols = slice(128 * half, 128 * half + 128)
            for k in range(16):
                at = 128 * k + 16 * (block % 8 + half)
                keep[at : at + 16] = grad[16 * k : 16 * k + 16, cols]
                send[at : at + 16] = grad[256 + 16 * k : 272 + 16 * k, cols]

    reorder(core, tokw, t_s)
    for n in range(6):
        put(dot(t_s[...], dqkv_s[:, 256 * n : 256 * n + 256]), 2 * n)
    reorder(core, att_s, t_s)
    for n in range(2):
        put(dot(t_s[...], cotw[:, 256 * n : 256 * n + 256]), 12 + 2 * n)


def place():
    gx, gz = lax.axis_index("gx"), lax.axis_index("gz")
    return gx & 3, ((gx >> 2) << 1) + (gz >> 1)


def block(index, size):
    return pl.ds(pl.multiple_of(index * size, size), size)


def by_offset(refs):
    return [[refs[2 * OFFSETS.index(k) + half] for k in range(4)] for half in range(2)]


def sum_core_x(keep, got, *outs):
    x, _ = place()
    for out, k in zip(outs, OFFSETS):
        for other in range(4):
            at = block(4 * other + ((x + k) & 3), 128)
            out[128 * other : 128 * other + 128] = keep[at] + got[at]
        out[512:536] = keep[2048:2072] + got[2048:2072]


def sum_core_y(keep, got, *outs):
    _, y = place()
    for out, k in zip(outs, OFFSETS):
        for other in range(4):
            at = block(4 * ((y + k) & 3) + other, 128)
            out[128 * other : 128 * other + 128] = keep[at] + got[at]


def four(refs, rows):
    return (refs[0][rows] + refs[2][rows]) + (refs[1][rows] + refs[3][rows])


def sum_first(*refs):
    (a, b), (one, two) = by_offset(refs[0:8]), by_offset(refs[8:16])
    x, y = place()
    table = four(a, slice(512, 536))
    for k in range(4):
        one[k][0:128] = four(a, block((y + k) & 3, 128))
        one[k][128:152] = table
        two[k][...] = four(b, block((x + k) & 3, 128))


def sum_second(*refs):
    (a, b), out = by_offset(refs[0:8]), refs[8]
    for n in range(16):
        rows = slice(16 * (n % 8), 16 * (n % 8) + 16)
        part = four(a if n < 8 else b, rows)
        for z in range(8):
            out[z, 2 * n : 2 * n + 2] = part[2 * z : 2 * z + 2]
    table = four(a, slice(128, 152))
    for z in range(8):
        out[z, 32:56] = table


def finish(got, mq, mp, mt, oq, op, ot):
    total = got[0]
    for k in range(1, 8):
        total = total + got[k]
    total = total * (1.0 / 4096)
    for e in range(2):
        for c in range(12):
            row = 2 * c + e
            r = slice(12 * e + c, 12 * e + c + 1)
            oq[r] = 0.9 * mq[r] + total[row : row + 1]
        for c in range(4):
            row = 2 * (12 + c) + e
            r = slice(4 * e + c, 4 * e + c + 1)
            op[r] = 0.9 * mp[r] + total[row : row + 1]
    table = jnp.concatenate([total[32:40], total[40:48], total[48:56]], axis=1)
    for h in range(HEADS):
        at = (h % 2) * EPAD
        ot[h : h + 1] = 0.9 * mt[h : h + 1] + table[h // 2 : h // 2 + 1, at : at + ENT]


def shapes(*dims):
    return tuple(jax.ShapeDtypeStruct(d, F32) for d in dims)


def local_grads(tok, cot, regions, rel_index, w_qkv, w_proj, table, interpret=False):
    return pl.pallas_call(
        local_kernel,
        out_shape=shapes((2072, 128), (2048, 128), (2072, 128), (2048, 128)),
        in_specs=[pl.BlockSpec(memory_space=pltpu.HBM)] * 7,
        scratch_shapes=[
            pltpu.VMEM((ROWS, D), BF16),
            pltpu.VMEM((ROWS, D), BF16),
            pltpu.VMEM((WIN, TOK), jnp.int32),
            pltpu.VMEM((TOK, TOK), jnp.int32),
            pltpu.VMEM((D, 3 * D), BF16),
            pltpu.VMEM((D, D), BF16),
            pltpu.VMEM((HEADS, ENT), F32),
            pltpu.SemaphoreType.DMA((7,)),
            pltpu.VMEM((PROWS, D), BF16),
            pltpu.VMEM((PROWS, D), BF16),
            pltpu.VMEM((PROWS, 3 * D), BF16),
            pltpu.VMEM((PROWS, D), BF16),
            pltpu.VMEM((PROWS, D), BF16),
            pltpu.VMEM((PROWS, 3 * D), BF16),
            pltpu.VMEM((8 * PAD, 128), F32),
            pltpu.VMEM((WIN * PAD, 128), F32),
            pltpu.VMEM((8 * PAD, 128), F32),
            pltpu.VMEM((128, 128), F32),
            pltpu.VMEM((D, PROWS), BF16),
        ],
        name="local_grads",
        compiler_params=pltpu.CompilerParams(vmem_limit_bytes=40 << 20),
        interpret=interpret,
    )(*(pltpu.with_memory_space_constraint(v, pltpu.HBM) for v in (tok, cot, regions, rel_index, w_qkv, w_proj, table)))


def small(kernel, out_shape, *args):
    return pl.pallas_call(
        kernel, out_shape=out_shape, compiler_params=pltpu.CompilerParams(vmem_limit_bytes=3 << 20)
    )(*args)


def spread_out(m, one, two):
    out = list(m)
    for n in range(6):
        out[n] = shift(m[n], **{(one, two)[n % 2]: OFFSETS[n // 2]})
    return out


def body(
    tokens, cotangent, regions, rel_index, w_qkv, w_proj, bias_table, mom_qkv, mom_proj, mom_table
):
    tok = jnp.transpose(tokens, (1, 0, 2)).reshape(ROWS, D)
    cot = jnp.transpose(cotangent, (1, 0, 2)).reshape(ROWS, D)
    keep1, keep2, send1, send2 = local_grads(tok, cot, regions, rel_index, w_qkv, w_proj, bias_table.T)
    got1 = shift(send1, dc=1)
    got2 = shift(send2, dc=1)
    xs = small(sum_core_x, shapes(*[(536, 128)] * 4), keep1, got1)
    ys = small(sum_core_y, shapes(*[(512, 128)] * 4), keep2, got2)
    m = [v for pair in zip(xs, ys) for v in pair]
    m = spread_out(m, "dx", "dy")
    m = small(sum_first, shapes(*[(152, 128), (128, 128)] * 4), *m)
    m = spread_out(m, "dy", "dx")
    line = small(sum_second, jax.ShapeDtypeStruct((8, 56, 128), F32), *m)
    line = lax.all_to_all(line, "gy", 0, 0, tiled=True)
    new_q, new_p, new_t = small(
        finish,
        shapes((24, 128), (8, 128), (HEADS, ENT)),
        line,
        mom_qkv.reshape(24, 128),
        mom_proj.reshape(8, 128),
        mom_table.T,
    )
    return new_q.reshape(-1), new_p.reshape(-1), new_t.T


def solution(mesh):
    return jax.shard_map(
        body,
        mesh=mesh,
        in_specs=(
            P(AXES, None, None),
            P(AXES, None, None),
            P(AXES, None),
            P(),
            P(),
            P(),
            P(),
            P(AXES),
            P(AXES),
            P(),
        ),
        out_specs=(P(AXES), P(AXES), P()),
        check_vma=False,
    )
```

```python
import jax
import jax.numpy as jnp
from jax import lax
from jax.experimental import pallas as pl
from jax.experimental.pallas import tpu as pltpu
from jax.sharding import PartitionSpec as P


AXES = ("gx", "gy", "gz")
WIN = 16
TOK = 49
PAD = 64
D = 512
HEADS = 16
HD = 32
ENT = 169
EPAD = 176
UNROLL = 8
OFFSETS = (2, 1, 3, 0)
AHEAD = 2
ROWS = TOK * WIN
PROWS = PAD * WIN
F32 = jnp.float32
BF16 = jnp.bfloat16
NT = (((1,), (1,)), ((), ()))
NN = (((1,), (0,)), ((), ()))


def dot(a, b, dims=NN):
    return lax.dot_general(a, b, dims, preferred_element_type=F32)


def decode(flat):
    gx, gy, gz = flat // 32, (flat // 4) % 8, flat % 4
    return gx % 4, (gx // 4) * 2 + gz // 2, gy, gz % 2


def encode(x, y, z, c):
    x, y, z = x % 4, y % 4, z % 8
    return ((y // 2) * 4 + x) * 32 + z * 4 + (y % 2) * 2 + c


def shift(value, dx=0, dy=0, dz=0, dc=0):
    pairs = []
    for d in range(256):
        x, y, z, c = decode(d)
        pairs.append((d, encode(x + dx, y + dy, z + dz, c ^ dc)))
    return lax.ppermute(value, AXES, pairs)


def reorder(core, src, dst):
    r = lax.broadcasted_iota(jnp.int32, (128, 128), 0)
    col = lax.broadcasted_iota(jnp.int32, (128, 128), 1)
    e = r & 1
    z = (r >> 1) & 7
    x = (r >> 4) & 3
    y0 = (r >> 6) & 1
    for rc in range(2):
        c = (rc + core) & 1
        orig = ((x * 32 + z * 4 + y0 * 2 + c) << 1) + e
        hot = jnp.concatenate([jnp.where(orig == col + 128 * k, 1.0, 0.0) for k in range(2)], axis=1).astype(BF16)
        for y1 in range(2):
            at = 256 * rc + 128 * y1
            dst[at : at + 128] = dot(hot, src[:, 256 * y1 : 256 * y1 + 256], NT).astype(BF16)


def local_kernel(
    tok_h, cot_h, reg_h, rel_h, wqkv_h, wproj_h, tab_h, keep1, keep2, send1, send2,
    tok, cot, reg, rel, wqkv, wproj, tab, sems, tokw, cotw, qkv_s, da_s, att_s, dqkv_s, bias_s, mask_s, acc_s, sq_s, t_s, u_s,
):
    moves = [
        pltpu.make_async_copy(src, dst, sems.at[n])
        for n, (src, dst) in enumerate(
            zip((rel_h, reg_h, tab_h, tok_h, wqkv_h, cot_h, wproj_h), (rel, reg, tab, tok, wqkv, cot, wproj))
        )
    ]
    for move in moves:
        move.start()
    factor = 1.4426950408889634
    scale = HD**-0.5

    line = lax.broadcasted_iota(jnp.int32, (256, 128), 0)
    lanes = lax.broadcasted_iota(jnp.int32, (256, 128), 1)
    source = (line & 15) * WIN + (line >> 4)
    pick = jnp.concatenate([jnp.where(source == lanes + 128 * k, 1.0, 0.0) for k in range(2)], axis=1).astype(BF16)
    alone = jnp.where(((line & 15) == 0) & ((line >> 4) == lanes), 1.0, 0.0).astype(BF16)[:, 0:WIN]

    def regroup(src, dst):
        for b in range(4):
            if b < 3:
                moved = dot(pick, src[256 * b : 256 * b + 256]).astype(BF16)
            else:
                moved = dot(alone, src[768:784]).astype(BF16)
            for w in range(WIN):
                dst[w * PAD + 16 * b : w * PAD + 16 * b + 16] = moved[16 * w : 16 * w + 16]

    for move in moves[0:4]:
        move.wait()
    core = lax.axis_index("gz") & 1
    regroup(tok, tokw)
    reorder(core, tokw, t_s)

    sq_s[...] = jnp.zeros((128, 128), F32)
    sq_s[0:TOK, 0:TOK] = rel[...].astype(F32)
    sq_s[PAD : PAD + TOK, 0:TOK] = rel[...].astype(F32)
    relt = jnp.transpose(sq_s[...])[0:PAD].astype(jnp.int32)
    lane = lax.broadcasted_iota(jnp.int32, (PAD, 128), 1)
    sub = lax.broadcasted_iota(jnp.int32, (PAD, 128), 0)
    live = ((lane & 63) < TOK) & (sub < TOK)
    relt = jnp.where(live, relt, -1)
    safe = jnp.where(live, relt, 0)
    low_i = jnp.where(safe < 128, safe, 0)
    high_i = jnp.where(safe < 128, 0, safe - 128)
    is_low = safe < 128
    first = lane < 64
    for hp in range(HEADS // 2):
        looked = []
        for par in range(2):
            h = 2 * hp + par
            low = jnp.broadcast_to(tab[h : h + 1, 0:128], (8, 128))
            high = jnp.concatenate([tab[h : h + 1, 128:ENT], jnp.zeros((1, 256 - ENT), F32)], axis=1)
            high = jnp.broadcast_to(high, (8, 128))
            rows = []
            for b in range(PAD // 8):
                s = slice(8 * b, 8 * b + 8)
                a0 = jnp.take_along_axis(low, low_i[s], axis=1, mode="promise_in_bounds")
                a1 = jnp.take_along_axis(high, high_i[s], axis=1, mode="promise_in_bounds")
                rows.append(jnp.where(is_low[s], a0, a1))
            looked.append(jnp.concatenate(rows, axis=0))
        both = jnp.where(first, looked[0], looked[1])
        bias_s[hp * PAD : (hp + 1) * PAD] = jnp.where(sub < TOK, both * factor, -1e30)

    sq_s[...] = jnp.zeros((128, 128), F32)
    sq_s[0:WIN, 0:TOK] = reg[...].astype(F32)
    base = sq_s[...]
    cols = jnp.transpose(base)
    for w in range(WIN):
        row = jnp.concatenate([base[w : w + 1, 0:64], base[w : w + 1, 0:64]], axis=1)
        mask_s[w * PAD : (w + 1) * PAD] = jnp.where(cols[0:PAD, w : w + 1] == row, 0.0, -100.0 * factor)

    acc_s[...] = jnp.zeros(acc_s.shape, F32)

    moves[4].wait()
    for n in range(6):
        cols = slice(256 * n, 256 * n + 256)
        qkv_s[:, cols] = dot(tokw[...], wqkv[:, cols]).astype(BF16)
    for move in moves[5:7]:
        move.wait()
    regroup(cot, cotw)
    for n in range(2):
        cols = slice(256 * n, 256 * n + 256)
        da_s[:, cols] = dot(cotw[...], wproj[cols], NT).astype(BF16)

    chan = lax.broadcasted_iota(jnp.int32, (PAD, 128), 1) // HD
    none = jnp.zeros((PAD, 128), BF16)

    def spread(v):
        return jnp.concatenate([jnp.where(chan == h, v, none) for h in range(4)], axis=0)

    def fold(full):
        total = full[0:PAD]
        for h in range(1, 4):
            total = jnp.where(chan == h, full[h * PAD : (h + 1) * PAD], total)
        return total.astype(BF16)

    def scores(rows, mask, g):
        cq = slice(g * 128, g * 128 + 128)
        k = qkv_s[rows, D + g * 128 : D + g * 128 + 128]
        v = qkv_s[rows, 2 * D + g * 128 : 2 * D + g * 128 + 128]
        qd = spread(qkv_s[rows, cq])
        dd = spread(da_s[rows, cq])
        return dict(rows=rows, mask=mask, g=g, k=k, v=v, qd=qd, dd=dd, s=dot(k, qd, NT), dp=dot(v, dd, NT))

    def softmax(it):
        g, mask = it["g"], it["mask"]
        bias = jnp.concatenate(
            [bias_s[2 * g * PAD : (2 * g + 1) * PAD] + mask, bias_s[(2 * g + 1) * PAD : (2 * g + 2) * PAD] + mask], axis=1
        )
        s = it["s"] * (scale * factor) + bias
        p = jnp.exp2(s - jnp.max(s, axis=0, keepdims=True))
        p = p * (1.0 / jnp.sum(p, axis=0, keepdims=True))
        dp = it["dp"].astype(BF16).astype(F32)
        ds = p * (dp - jnp.sum(dp * p, axis=0, keepdims=True))
        it["pb"] = p.astype(BF16)
        it["dsb"] = (ds * scale).astype(BF16)
        it["pt"] = jnp.transpose(it["pb"])
        it["dst"] = jnp.transpose(it["dsb"])
        return ds

    def results(it):
        rows, g = it["rows"], it["g"]
        cq = slice(g * 128, g * 128 + 128)
        dqkv_s[rows, 2 * D + g * 128 : 2 * D + g * 128 + 128] = dot(it["pb"], it["dd"]).astype(BF16)
        att_s[rows, cq] = fold(dot(it["pt"], it["v"]))
        dqkv_s[rows, D + g * 128 : D + g * 128 + 128] = dot(it["dsb"], it["qd"]).astype(BF16)
        dqkv_s[rows, cq] = fold(dot(it["dst"], it["k"]))

    def windows(step, carry):
        chains = []
        for g in range(4):
            for i in range(UNROLL):
                rows = pl.ds(pl.multiple_of((step * UNROLL + i) * PAD, PAD), PAD)
                chains.append((rows, i, g))
        masks = [mask_s[pl.ds(pl.multiple_of((step * UNROLL + i) * PAD, PAD), PAD), :] for i in range(UNROLL)]
        sums = [None] * 4
        items = []
        for c in range(len(chains) + 1 + AHEAD):
            if c < len(chains):
                rows, i, g = chains[c]
                items.append(scores(rows, masks[i], g))
            if 0 <= c - AHEAD < len(chains):
                it = items[c - AHEAD]
                ds = softmax(it)
                g = it["g"]
                sums[g] = ds if sums[g] is None else sums[g] + ds
                if c - AHEAD == UNROLL * g + UNROLL - 1:
                    acc_s[2 * g * PAD : (2 * g + 1) * PAD] += sums[g][:, 0:128]
                    acc_s[(2 * g + 1) * PAD : (2 * g + 2) * PAD] += sums[g][:, 128:256]
            if c - AHEAD - 1 >= 0:
                results(items[c - AHEAD - 1])
        return carry

    lax.fori_loop(0, WIN // UNROLL, windows, 0)

    ent = lax.broadcasted_iota(jnp.int32, (EPAD, 128), 0)
    sums = jnp.zeros((EPAD, 32), F32)
    left = lax.broadcasted_iota(jnp.int32, (8, 128), 1) < 64
    for j7 in range(7):
        hots, parts = [], []
        for j in range(7 * j7, 7 * j7 + 7):
            part = acc_s[pl.ds(j, 8, stride=PAD), :]
            top = part.astype(BF16).astype(F32)
            rest = part - top
            split = [jnp.where(left, top, 0.0), jnp.where(left, rest, 0.0), jnp.where(left, 0.0, top), jnp.where(left, 0.0, rest)]
            parts.append(jnp.concatenate(split, axis=0).astype(BF16))
            hots.append(jnp.where(ent == relt[j : j + 1], 1.0, 0.0).astype(BF16))
        sums = sums + dot(jnp.concatenate(hots, axis=1), jnp.concatenate(parts, axis=1), NT)
    sums = jnp.concatenate([sums, jnp.zeros((EPAD, 96), F32)], axis=1)
    sums = jnp.concatenate([sums, pltpu.roll(sums, 112, 1), jnp.zeros((384 - 2 * EPAD, 128), F32)], axis=0)
    flat = jnp.concatenate([jnp.transpose(sums[128 * k : 128 * k + 128])[0:16] for k in range(3)], axis=1)
    table = flat[0:8] + flat[8:16]
    for k in range(3):
        keep1[2048 + 8 * k : 2056 + 8 * k] = table[:, 128 * k : 128 * k + 128]
        send1[2048 + 8 * k : 2056 + 8 * k] = table[:, 128 * k : 128 * k + 128]


    def put(grad, block):
        keep, send = (keep1, send1) if block < 8 else (keep2, send2)
        for half in range(2):
            cols = slice(128 * half, 128 * half + 128)
            for k in range(16):
                at = 128 * k + 16 * (block % 8 + half)
                keep[at : at + 16] = grad[16 * k : 16 * k + 16, cols]
                send[at : at + 16] = grad[256 + 16 * k : 272 + 16 * k, cols]

    for n in range(6):
        put(dot(t_s[...], dqkv_s[:, 256 * n : 256 * n + 256]), 2 * n)
    reorder(core, att_s, u_s)
    for n in range(2):
        put(dot(u_s[...], cotw[:, 256 * n : 256 * n + 256]), 12 + 2 * n)


def place():
    gx, gz = lax.axis_index("gx"), lax.axis_index("gz")
    return gx & 3, ((gx >> 2) << 1) + (gz >> 1)


def block(index, size):
    return pl.ds(pl.multiple_of(index * size, size), size)


def by_offset(refs):
    return [[refs[2 * OFFSETS.index(k) + half] for k in range(4)] for half in range(2)]


def sum_core_x(keep, got, *outs):
    x, _ = place()
    for out, k in zip(outs, OFFSETS):
        for other in range(4):
            at = block(4 * other + ((x + k) & 3), 128)
            out[128 * other : 128 * other + 128] = keep[at] + got[at]
        out[512:536] = keep[2048:2072] + got[2048:2072]


def sum_core_y(keep, got, *outs):
    _, y = place()
    for out, k in zip(outs, OFFSETS):
        for other in range(4):
            at = block(4 * ((y + k) & 3) + other, 128)
            out[128 * other : 128 * other + 128] = keep[at] + got[at]


def four(refs, rows):
    return (refs[0][rows] + refs[2][rows]) + (refs[1][rows] + refs[3][rows])


def sum_first(*refs):
    (a, b), (one, two) = by_offset(refs[0:8]), by_offset(refs[8:16])
    x, y = place()
    table = four(a, slice(512, 536))
    for k in range(4):
        one[k][0:128] = four(a, block((y + k) & 3, 128))
        one[k][128:152] = table
        two[k][...] = four(b, block((x + k) & 3, 128))


def sum_second(*refs):
    (a, b), out = by_offset(refs[0:8]), refs[8]
    for n in range(16):
        rows = slice(16 * (n % 8), 16 * (n % 8) + 16)
        part = four(a if n < 8 else b, rows)
        for z in range(8):
            out[z, 2 * n : 2 * n + 2] = part[2 * z : 2 * z + 2]
    table = four(a, slice(128, 152))
    for z in range(8):
        out[z, 32:56] = table


def finish(got, mq, mp, mt, oq, op, ot):
    total = got[0]
    for k in range(1, 8):
        total = total + got[k]
    total = total * (1.0 / 4096)
    for e in range(2):
        for c in range(12):
            row = 2 * c + e
            r = slice(12 * e + c, 12 * e + c + 1)
            oq[r] = 0.9 * mq[r] + total[row : row + 1]
        for c in range(4):
            row = 2 * (12 + c) + e
            r = slice(4 * e + c, 4 * e + c + 1)
            op[r] = 0.9 * mp[r] + total[row : row + 1]
    table = jnp.concatenate([total[32:40], total[40:48], total[48:56]], axis=1)
    for h in range(HEADS):
        at = (h % 2) * EPAD
        ot[h : h + 1] = 0.9 * mt[h : h + 1] + table[h // 2 : h // 2 + 1, at : at + ENT]


def shapes(*dims):
    return tuple(jax.ShapeDtypeStruct(d, F32) for d in dims)


def local_grads(tok, cot, regions, rel_index, w_qkv, w_proj, table, interpret=False):
    return pl.pallas_call(
        local_kernel,
        out_shape=shapes((2072, 128), (2048, 128), (2072, 128), (2048, 128)),
        in_specs=[pl.BlockSpec(memory_space=pltpu.HBM)] * 7,
        scratch_shapes=[
            pltpu.VMEM((ROWS, D), BF16),
            pltpu.VMEM((ROWS, D), BF16),
            pltpu.VMEM((WIN, TOK), jnp.int32),
            pltpu.VMEM((TOK, TOK), jnp.int32),
            pltpu.VMEM((D, 3 * D), BF16),
            pltpu.VMEM((D, D), BF16),
            pltpu.VMEM((HEADS, ENT), F32),
            pltpu.SemaphoreType.DMA((7,)),
            pltpu.VMEM((PROWS, D), BF16),
            pltpu.VMEM((PROWS, D), BF16),
            pltpu.VMEM((PROWS, 3 * D), BF16),
            pltpu.VMEM((PROWS, D), BF16),
            pltpu.VMEM((PROWS, D), BF16),
            pltpu.VMEM((PROWS, 3 * D), BF16),
            pltpu.VMEM((8 * PAD, 128), F32),
            pltpu.VMEM((WIN * PAD, 128), F32),
            pltpu.VMEM((8 * PAD, 128), F32),
            pltpu.VMEM((128, 128), F32),
            pltpu.VMEM((D, PROWS), BF16),
            pltpu.VMEM((D, PROWS), BF16),
        ],
        name="local_grads",
        compiler_params=pltpu.CompilerParams(vmem_limit_bytes=40 << 20),
        interpret=interpret,
    )(*(pltpu.with_memory_space_constraint(v, pltpu.HBM) for v in (tok, cot, regions, rel_index, w_qkv, w_proj, table)))


def small(kernel, out_shape, *args):
    return pl.pallas_call(
        kernel, out_shape=out_shape, compiler_params=pltpu.CompilerParams(vmem_limit_bytes=3 << 20)
    )(*args)


def spread_out(m, one, two):
    out = list(m)
    for n in range(6):
        out[n] = shift(m[n], **{(one, two)[n % 2]: OFFSETS[n // 2]})
    return out


def body(
    tokens, cotangent, regions, rel_index, w_qkv, w_proj, bias_table, mom_qkv, mom_proj, mom_table
):
    tok = jnp.transpose(tokens, (1, 0, 2)).reshape(ROWS, D)
    cot = jnp.transpose(cotangent, (1, 0, 2)).reshape(ROWS, D)
    keep1, keep2, send1, send2 = local_grads(tok, cot, regions, rel_index, w_qkv, w_proj, bias_table.T)
    got1 = shift(send1, dc=1)
    got2 = shift(send2, dc=1)
    xs = small(sum_core_x, shapes(*[(536, 128)] * 4), keep1, got1)
    ys = small(sum_core_y, shapes(*[(512, 128)] * 4), keep2, got2)
    m = [v for pair in zip(xs, ys) for v in pair]
    m = spread_out(m, "dx", "dy")
    m = small(sum_first, shapes(*[(152, 128), (128, 128)] * 4), *m)
    m = spread_out(m, "dy", "dx")
    line = small(sum_second, jax.ShapeDtypeStruct((8, 56, 128), F32), *m)
    line = lax.all_to_all(line, "gy", 0, 0, tiled=True)
    new_q, new_p, new_t = small(
        finish,
        shapes((24, 128), (8, 128), (HEADS, ENT)),
        line,
        mom_qkv.reshape(24, 128),
        mom_proj.reshape(8, 128),
        mom_table.T,
    )
    return new_q.reshape(-1), new_p.reshape(-1), new_t.T


def solution(mesh):
    return jax.shard_map(
        body,
        mesh=mesh,
        in_specs=(
            P(AXES, None, None),
            P(AXES, None, None),
            P(AXES, None),
            P(),
            P(),
            P(),
            P(),
            P(AXES),
            P(AXES),
            P(),
        ),
        out_specs=(P(AXES), P(AXES), P()),
        check_vma=False,
    )
```
